32 devices in a mesh: win: 4 (over z), step: 8 (over y, x, core).
Axes of the slice: x: 2, y: 2, z: 4, core: 2. Of those that a mesh axis runs over, the one named last changes fastest.
Arguments:
- initial_state: float32 [32, 32, 128], replicated, may hold values from -6 to 6
- source: float32 [4, 8, 32, 32, 128], P('win', 'step'), may hold values from -6 to 6
- absorption: float32 [32, 32, 128], replicated, may hold values from 0.01 to 0.2
Outputs:
- state: float32 [4, 8, 32, 32, 128], P('win', 'step')
The draws below stay inside these ranges and needn't reach their ends.
All inputs are finite; a program needn't handle non-finite values.
Results may differ from the reference program's by a relative error of at most 0.00026.
Values sent between devices are 32-bit elements; how exact they have to be, the bound alone decides.
A program may use at most 64 MiB of HBM per device.

```python
import math
import jax
import jax.numpy as jnp

NX = 32
NY = 32
NZ = 128
ITERS = 2
SWEEPS = 8
STEPS = 8
WINDOWS = 4


def block_scale(rng, dims, split, low, largest):
    def one(dim, blocks):
        heights = jax.random.uniform(jax.random.fold_in(jax.random.fold_in(rng, 6), dim), (blocks,), jnp.float32, low / len(split), largest / len(split))
        return jnp.repeat(jnp.exp(heights), dims[dim] // blocks).reshape((-1,) + (1,) * (len(dims) - dim - 1))

    loudness = one(*split[0])
    for cut in split[1:]:
        loudness = loudness * one(*cut)
    return loudness


def centred(own_key, extent, spread, most, shards=(), kind=jnp.bfloat16):
    factor_of = block_scale(own_key, extent, shards, -0.22, 0.18) if shards else 1.0
    values = jax.random.normal(own_key, extent, jnp.float32) * spread * factor_of
    return jnp.minimum(jnp.maximum(values, -most), most).astype(kind)


def setup_inputs(seed: int = 0) -> dict:
    keys = jax.random.split(jax.random.key(seed), 4)
    initial_state = centred(keys[0], (NX, NY, NZ), 1.0, 6.0, (), jnp.float32)
    source = centred(keys[1], (WINDOWS, STEPS, NX, NY, NZ), 1.0, 6.0, ((0, 4), (1, 8)), jnp.float32)
    absorption = jnp.clip(jnp.exp(jax.random.uniform(keys[2], (NX, NY, NZ), jnp.float32, math.log(0.01), math.log(0.2))), 0.01, 0.2)
    return dict(initial_state=initial_state, source=source, absorption=absorption)


alpha_corner = 0.1
coupling = 0.05


def pad_cube(field):
    widths = [(0, 0)] * (field.ndim - 3) + [(1, 1)] * 3
    return jnp.pad(field, widths)


def neighbours(field):
    padded = pad_cube(field)
    total = padded[..., 2:, 1:-1, 1:-1] + padded[..., :-2, 1:-1, 1:-1]
    total = total + padded[..., 1:-1, 2:, 1:-1] + padded[..., 1:-1, :-2, 1:-1]
    total = total + padded[..., 1:-1, 1:-1, 2:] + padded[..., 1:-1, 1:-1, :-2]
    return total


def complex_times(first, second):
    return jnp.stack([first[0] * second[0] - first[1] * second[1], first[0] * second[1] + first[1] * second[0]])


def relax(spectrum, inverse):
    field = complex_times(inverse, spectrum)
    for repeat in range(SWEEPS - 1):
        field = complex_times(inverse, spectrum + coupling * neighbours(field))
    return field


def inverse_diagonal(angle, absorption, gamma):
    real_part = 1.0 - gamma * jnp.cos(angle) + absorption + 6.0 * coupling
    imag_part = jnp.broadcast_to(gamma * jnp.sin(angle), real_part.shape)
    magnitude = real_part * real_part + imag_part * imag_part
    return jnp.stack([real_part / magnitude, -imag_part / magnitude])


def reference(initial_state, source, absorption):
    gamma = alpha_corner ** (1.0 / STEPS)
    moments = jnp.arange(STEPS, dtype=jnp.float32)
    scale = (gamma ** moments)[None, :, None, None, None]
    angle = (moments * (2.0 * math.pi / STEPS))[:, None, None, None]
    inverse = inverse_diagonal(angle, absorption, gamma)[:, None]
    state = jnp.zeros_like(source)
    for repeat in range(ITERS):
        ends = state[:, -1]
        before = jnp.concatenate([initial_state[None], ends[:-1]], axis=0)
        forcing = source.at[:, 0].add(before - alpha_corner * ends)
        spectrum_full = jnp.fft.fft(forcing * scale, axis=1)
        field = relax(jnp.stack([spectrum_full.real, spectrum_full.imag]), inverse)
        state = jnp.fft.ifft(field[0] + 1j * field[1], axis=1).real / scale
    return state
```

```python
import functools
import math

import jax
import jax.numpy as jnp
from jax import lax
from jax.experimental import pallas as pl
from jax.experimental.pallas import tpu as pltpu
from jax.sharding import PartitionSpec as P

ITERS = 2
SWEEPS = 8


alpha_corner = 0.1
coupling = 0.05


def from_behind(block, axis, distance):
    devices = range(lax.axis_size(axis))
    route = [(i - distance, i) for i in devices if i - distance in devices]
    return lax.ppermute(block, axis, route)


def pad_cube(field):
    widths = [(0, 0)] * (field.ndim - 3) + [(1, 1)] * 3
    return jnp.pad(field, widths)


def neighbours(field):
    padded = pad_cube(field)
    total = padded[..., 2:, 1:-1, 1:-1] + padded[..., :-2, 1:-1, 1:-1]
    total = total + padded[..., 1:-1, 2:, 1:-1] + padded[..., 1:-1, :-2, 1:-1]
    total = total + padded[..., 1:-1, 1:-1, 2:] + padded[..., 1:-1, 1:-1, :-2]
    return total


def complex_times(first, second):
    return jnp.stack(
        [first[0] * second[0] - first[1] * second[1], first[0] * second[1] + first[1] * second[0]]
    )


def relax(spectrum, inverse):
    field = complex_times(inverse, spectrum)
    for repeat in range(SWEEPS - 1):
        field = complex_times(inverse, spectrum + coupling * neighbours(field))
    return field


def inverse_diagonal(angle, absorption, gamma):
    real_part = 1.0 - gamma * jnp.cos(angle) + absorption + 6.0 * coupling
    imag_part = jnp.broadcast_to(gamma * jnp.sin(angle), real_part.shape)
    magnitude = real_part * real_part + imag_part * imag_part
    return jnp.stack([real_part / magnitude, -imag_part / magnitude])


def dft_tables(window_len):
    index = jnp.arange(window_len, dtype=jnp.int32)
    product = index[:, None] * index[None, :] % window_len
    angle = product.astype(jnp.float32) * (2.0 * math.pi / window_len)
    return (jnp.cos(angle), jnp.sin(angle))


def transform_exchange(scaled, window_len):
    pencil = lax.all_to_all(scaled[None], "step", split_axis=1, concat_axis=0, tiled=True)
    cosine, sine = dft_tables(window_len)
    flat = pencil.reshape(window_len, -1)
    real_part = jnp.dot(cosine, flat, precision=lax.Precision.HIGHEST)
    imag_part = -jnp.dot(sine, flat, precision=lax.Precision.HIGHEST)
    shaped = pencil.shape
    spectrum = (
        lax.all_to_all(real_part.reshape(shaped), "step", split_axis=0, concat_axis=1, tiled=True),
        lax.all_to_all(imag_part.reshape(shaped), "step", split_axis=0, concat_axis=1, tiled=True),
    )
    return jnp.stack([spectrum[0][0], spectrum[1][0]])


def untransform_exchange(field, window_len):
    pencil = (
        lax.all_to_all(field[0][None], "step", split_axis=1, concat_axis=0, tiled=True),
        lax.all_to_all(field[1][None], "step", split_axis=1, concat_axis=0, tiled=True),
    )
    cosine, sine = dft_tables(window_len)
    shaped = pencil[0].shape
    values = jnp.dot(cosine, pencil[0].reshape(window_len, -1), precision=lax.Precision.HIGHEST)
    values = values - jnp.dot(
        sine, pencil[1].reshape(window_len, -1), precision=lax.Precision.HIGHEST
    )
    values = values / window_len
    result = lax.all_to_all(values.reshape(shaped), "step", split_axis=0, concat_axis=1, tiled=True)
    return result[0]


def per_device(initial_state, source, absorption):
    window_len = lax.axis_size("step")
    moment = lax.axis_index("step")
    window_index = lax.axis_index("win")
    gamma = alpha_corner ** (1.0 / window_len)
    scale = gamma ** moment.astype(jnp.float32)
    forcing_base = source[0, 0]
    is_first = moment == 0
    state = jnp.zeros_like(forcing_base)
    angle = moment.astype(jnp.float32) * (2.0 * math.pi / window_len)
    inverse = inverse_diagonal(angle, absorption, gamma)
    for repeat in range(ITERS):
        if repeat == 0:
            correction = jnp.where(window_index == 0, initial_state, 0.0)
        else:
            ends = from_behind(state, "step", 1 - window_len)
            before = from_behind(ends, "win", 1)
            before = jnp.where(window_index == 0, initial_state, before)
            correction = before - alpha_corner * ends
        forcing = forcing_base + jnp.where(is_first, correction, 0.0)
        scaled = forcing * scale
        spectrum = transform_exchange(scaled, window_len)
        field = relax(spectrum, inverse)
        values = untransform_exchange(field, window_len)
        state = values / scale
    return state[None, None]


LANES = 128
TILE = 8
GROUP = 8


def tables(length):
    gamma = alpha_corner ** (1.0 / length)
    into, back, angles = [], [], []
    for core in range(2):
        rows_in, rows_back = [], []
        for time in range(length):
            scale = gamma**time
            row_in, row_back = [], []
            for p in range(length // 4):
                j = 2 * p + core
                if j == 0:
                    pair, weight = (1.0, (-1.0) ** time), 1.0 / length
                else:
                    turn = 2.0 * math.pi * (j * time % length) / length
                    pair, weight = (math.cos(turn), -math.sin(turn)), 2.0 / length
                row_in += [value * scale / coupling for value in pair]
                row_back += [value * weight / scale for value in pair]
            rows_in.append(row_in)
            rows_back.append(row_back)
        into.append(rows_in)
        back.append(rows_back)
        angles.append([2.0 * math.pi * (2 * p + core) / length for p in range(length // 4)])
    return into, back, angles


def kernel(
    length, windows, nx, ny, ext, ey,
    source, initial, absorb, out,
    raw, first, absv, coef, base, again, fa, fb, corr,
    psend, pgot, ends, zgot, csend, qsend, qgot, obuf,
    lsem, asend, brecv, fsend, esem, zsem, csem_s, csem_r, qsem_s, qsem_r, osem_s, osem_r,
):
    half = length // 2
    gx, gy = half // 2, 2
    bs, bsy = nx // gx, ny // gy
    reach = SWEEPS - 1
    pairs = length // 4
    units = 2 * pairs
    gamma = alpha_corner ** (1.0 / length)
    into, back, angles = tables(length)
    me = lax.axis_index("step")
    w = lax.axis_index("win")
    core, m = me % 2, me // 2
    partner = m * 2 + (1 - core)
    bx, by = m % gx, m // gx

    def xlo(b):
        if gx == 2:
            return b * (nx - ext)
        return jnp.minimum(jnp.maximum(b * bs - reach, 0), nx - ext)

    def ylo(b):
        return pl.multiple_of(b * (ny - ey), TILE)

    def pick(a, b):
        return jnp.where(core == 0, jnp.float32(a), jnp.float32(b))

    def region(ref, b_x, b_y):
        return ref.at[pl.ds(xlo(b_x), ext), pl.ds(ylo(b_y), ey), :]

    ox = bx * bs - xlo(bx)
    oy = pl.multiple_of(by * bsy - ylo(by), TILE)

    loads = [
        pltpu.make_async_copy(region(absorb, bx, by), absv, lsem.at[0]),
        pltpu.make_async_copy(region(source, bx, by), raw.at[me], lsem.at[1]),
        pltpu.make_async_copy(region(initial, bx, by), first, lsem.at[2]),
    ]
    for load in loads:
        load.start()
    zero_row = jnp.zeros((ey, LANES), jnp.float32)
    for u in range(units):
        for ref in (fa, fb):
            ref[u, 0, pl.ds(TILE, ey)] = zero_row
            ref[u, ext + 1, pl.ds(TILE, ey)] = zero_row
            for r in range(1, ext + 1):
                ref[u, r, pl.ds(0, TILE)] = zero_row[:TILE]
                ref[u, r, pl.ds(TILE + ey, TILE)] = zero_row[:TILE]
    if gx > 2:
        corr[...] = jnp.zeros_like(corr)

    barrier = pltpu.get_barrier_semaphore()
    for d in range(1, length):
        pl.semaphore_signal(
            barrier, inc=1, device_id={"step": (me + d) % length}, device_id_type=pl.DeviceIdType.MESH
        )

    @pl.when(w > 0)
    def _():
        pl.semaphore_signal(barrier, inc=1, device_id={"win": w - 1}, device_id_type=pl.DeviceIdType.MESH)

    @pl.when(w < windows - 1)
    def _():
        pl.semaphore_signal(barrier, inc=1, device_id={"win": w + 1}, device_id_type=pl.DeviceIdType.MESH)

    nearby = jnp.where(w > 0, 1, 0) + jnp.where(w < windows - 1, 1, 0)
    pl.semaphore_wait(barrier, length - 1 + nearby)

    def remote(src, dst, send, recv, **where):
        return pltpu.make_async_remote_copy(
            src_ref=src, dst_ref=dst, send_sem=send, recv_sem=recv,
            device_id=where, device_id_type=pl.DeviceIdType.MESH,
        )

    outgoing = []
    for d in range(1, half):
        to = (m + d) % half
        copy = remote(
            region(source, to % gx, to // gx), raw.at[me], asend.at[d], brecv.at[me], step=to * 2 + core
        )
        copy.start()
        outgoing.append(copy)
    copy = remote(region(source, bx, by), raw.at[me], asend.at[0], brecv.at[me], step=partner)
    copy.start()
    outgoing.append(copy)

    def grouped(begin, count, work, most=GROUP):
        size = -(-count // max(1, count // most))

        def body(g, carry):
            work(begin + g * size, size)
            return carry

        lax.fori_loop(0, count // size, body, 0)
        if count % size:
            work(begin + count - size, size)

    def each(one):
        def work(start, rows):
            for n in range(rows):
                one(start + n)

        return work

    loads[0].wait()

    def coefficients(i):
        for p in range(pairs):
            rows = absv[i]
            cosine = pick(math.cos(angles[0][p]), math.cos(angles[1][p]))
            imag = pick(gamma * math.sin(angles[0][p]), gamma * math.sin(angles[1][p]))
            real = 1.0 - gamma * cosine + rows + 6.0 * coupling
            over = coupling / (real * real + imag * imag)
            coef[3 * p, i] = real * over
            coef[3 * p + 1, i] = -imag * over
            if p == 0:
                other = pick(-1.0, math.cos(angles[1][p]))
                real = 1.0 - gamma * other + rows + 6.0 * coupling
                over = coupling / (real * real + imag * imag)
                coef[3 * p + 2, i] = real * over

    grouped(0, ext, each(coefficients))

    def weights(p, i):
        straight = coef[3 * p, i]
        return straight, (coef[3 * p + 2, i] if p == 0 else straight), coef[3 * p + 1, i]

    def arrival(t):
        return remote(raw.at[t], raw.at[t], asend.at[0], brecv.at[t], step=partner)

    for d in range(1, half):
        t = ((m + half - d) % half) * 2 + core
        arrival(t).wait_recv()
        copy = remote(raw.at[t], raw.at[t], fsend.at[d], brecv.at[t], step=partner)
        copy.start()
        outgoing.append(copy)
    for d in range(half):
        arrival(((m + half - d) % half) * 2 + (1 - core)).wait_recv()
    loads[1].wait()
    loads[2].wait()
    is_first = jnp.where(w == 0, jnp.float32(1.0 / coupling), jnp.float32(0.0))

    def second_weight(p, weight):
        return weight[2] + (pick(1.0, 0.0) * weight[1] if p == 0 else 0.0)

    def transform(i):
        begin = first[i] * is_first
        fields = [raw[t, i] for t in range(length)]
        for p in range(pairs):
            weight = weights(p, i)
            s0, s1 = begin, begin * pick(1.0, 0.0) if p == 0 else None
            for t in range(length):
                s0 = s0 + pick(into[0][t][2 * p], into[1][t][2 * p]) * fields[t]
                term = pick(into[0][t][2 * p + 1], into[1][t][2 * p + 1]) * fields[t]
                s1 = term if s1 is None else s1 + term
            b0 = weight[0] * s0 - weight[2] * s1
            b1 = weight[1] * s1 + weight[2] * s0
            base[2 * p, i] = b0
            base[2 * p + 1, i] = b1
            fa[2 * p, i + 1, pl.ds(TILE, ey)] = b0
            fa[2 * p + 1, i + 1, pl.ds(TILE, ey)] = b1

    grouped(0, ext, each(transform), GROUP // 2)

    lane = lax.broadcasted_iota(jnp.int32, (ey, LANES), 1)

    def around(ref, u, r):
        v = ref[u, r, pl.ds(TILE, ey)]
        total = jnp.where(lane == 0, 0.0, pltpu.roll(v, 1, 1))
        total = total + jnp.where(lane == LANES - 1, 0.0, pltpu.roll(v, LANES - 1, 1))
        beside = ref[u, r - 1, pl.ds(TILE, ey)] + ref[u, r + 1, pl.ds(TILE, ey)]
        return total + (beside + (ref[u, r, pl.ds(TILE - 1, ey)] + ref[u, r, pl.ds(TILE + 1, ey)]))

    def sweep_rows(base, here, there, start, rows):
        for n in range(rows):
            i = start + n
            for p in range(pairs):
                weight = weights(p, i)
                n0 = around(here, 2 * p, i + 1)
                n1 = around(here, 2 * p + 1, i + 1)
                there[2 * p, i + 1, pl.ds(TILE, ey)] = base[2 * p, i] + (weight[0] * n0 - weight[2] * n1)
                there[2 * p + 1, i + 1, pl.ds(TILE, ey)] = base[2 * p + 1, i] + (
                    weight[1] * n1 + weight[2] * n0
                )

    def sweeps(base):
        here, there = fa, fb
        for k in range(1, SWEEPS):
            begin, count = (bx * k, ext - k) if gx == 2 else (0, ext)
            grouped(begin, count, functools.partial(sweep_rows, base, here, there))
            here, there = there, here
        return here

    final = sweeps(base)

    def part(t, y0, rows):
        total = None
        for u in range(units):
            factor = pick(back[0][t[0]][u], back[1][t[1]][u])
            term = factor * final[u, pl.ds(ox + 1, bs), pl.ds(y0 + TILE, rows), :]
            total = term if total is None else total + term
        return total

    last = (length - 1, length - 1)
    psend[...] = part(last, pl.multiple_of(oy + TILE * (1 - core), TILE), TILE)
    swap = remote(psend, pgot, esem.at[0], esem.at[1], step=partner)
    swap.start()
    mine = part(last, pl.multiple_of(oy + TILE * core, TILE), TILE)
    swap.wait_recv()
    mine = mine + pgot[...]
    ends[...] = mine
    outgoing.append(swap)

    onward = remote(ends, zgot, zsem.at[0], zsem.at[1], win=(w + 1) % windows)

    @pl.when(w < windows - 1)
    def _():
        onward.start()

    @pl.when(w == 0)
    def _():
        zgot[...] = jnp.zeros_like(zgot)

    @pl.when(w > 0)
    def _():
        onward.wait_recv()

    change = zgot[...] - alpha_corner * ends[...]
    csend[...] = change
    corr[pl.ds(ox, bs), pl.ds(pl.multiple_of(oy + TILE * core, TILE), TILE), :] = change

    def spread(ex, ey_, send):
        rows, skip = (bs, 0) if ex == 0 else (reach, bs - reach if ex == 1 else 0)
        tx, ty = (bx + ex, by + ey_) if send else (bx, by)
        fx, fy = (bx, by) if send else (bx - ex, by - ey_)
        ax, ay = (tx, ty) if send else (fx, fy)
        inside = (ax >= 0) & (ax < gx) & (ay >= 0) & (ay < gy)
        slot = ((ex + 1) * 3 + (ey_ + 1)) * 2
        for c in range(2):
            near = c == (1 if ey_ == 1 else 0)
            if send:
                okay = inside if ey_ == 0 else inside & (core == (1 if ey_ == 1 else 0))
                if ex == 0 and ey_ == 0:
                    okay = core != c
                fc, tc = core, c
            else:
                if ey_ != 0 and not near:
                    continue
                okay = inside
                if ex == 0 and ey_ == 0:
                    okay = core != c
                fc, tc = c, core

            @pl.when(okay)
            def _(c=c, fc=fc, tc=tc):
                copy = remote(
                    csend.at[pl.ds(skip, rows)],
                    corr.at[
                        pl.ds(fx * bs + skip - xlo(tx), rows),
                        pl.ds(pl.multiple_of(fy * bsy + TILE * fc - ylo(ty), TILE), TILE),
                        :,
                    ],
                    csem_s.at[slot + c],
                    csem_r.at[slot + fc],
                    step=(ty * gx + tx) * 2 + tc if send == 1 else partner,
                )
                if send == 1:
                    copy.start()
                elif send == 2:
                    copy.wait_send()
                else:
                    copy.wait_recv()

    offsets = [(ex, e) for ex in (-1, 0, 1) for e in (-1, 0, 1)]
    for ex, e in offsets:
        spread(ex, e, 1)
    for ex, e in offsets:
        spread(ex, e, 0)

    def correct(i):
        x = corr[i] * (1.0 / coupling)
        for p in range(pairs):
            weight = weights(p, i)
            b0 = base[2 * p, i] + weight[0] * x
            b1 = base[2 * p + 1, i] + second_weight(p, weight) * x
            again[2 * p, i] = b0
            again[2 * p + 1, i] = b1
            fa[2 * p, i + 1, pl.ds(TILE, ey)] = b0
            fa[2 * p + 1, i + 1, pl.ds(TILE, ey)] = b1

    grouped(0, ext, each(correct))
    final = sweeps(again)

    for k in range(half):
        qsend[k] = part((2 * k + 1, 2 * k), oy, bsy)
        copy = remote(qsend.at[k], qgot.at[k], qsem_s.at[k], qsem_r.at[k], step=partner)
        copy.start()
        outgoing.append(copy)
    for k in range(half):
        obuf[k] = part((2 * k, 2 * k + 1), oy, bsy)

    def place(b_x, b_y):
        return out.at[pl.ds(b_x * bs, bs), pl.ds(pl.multiple_of(b_y * bsy, TILE), bsy), :]

    for k in range(half):
        remote(qsend.at[k], qgot.at[k], qsem_s.at[k], qsem_r.at[k], step=partner).wait_recv()
        obuf[k] = obuf[k] + qgot[k]

        @pl.when(m == k)
        def _(k=k):
            pltpu.make_async_copy(obuf.at[k], place(bx, by), lsem.at[3]).start()

        @pl.when(m != k)
        def _(k=k):
            remote(obuf.at[k], place(bx, by), osem_s.at[k], osem_r.at[m], step=2 * k + core).start()

    for copy in outgoing:
        copy.wait_send()
    for ex, e in offsets:
        spread(ex, e, 2)

    @pl.when(w < windows - 1)
    def _():
        onward.wait_send()

    for k in range(half):

        @pl.when(m == k)
        def _(k=k):
            pltpu.make_async_copy(obuf.at[k], place(bx, by), lsem.at[3]).wait()

        @pl.when(m != k)
        def _(k=k):
            done = remote(obuf.at[k], place(k % gx, k // gx), osem_s.at[k], osem_r.at[k], step=partner)
            done.wait_send()
            done.wait_recv()


def blocks(initial_state, source, absorption):
    length = lax.axis_size("step")
    windows = lax.axis_size("win")
    nx, ny, nz = initial_state.shape
    half = length // 2
    gx, reach = half // 2, SWEEPS - 1
    bs, bsy = nx // gx, ny // 2
    ext = min(nx, bs + reach * (1 if gx == 2 else 2))
    ey = bsy + -(-reach // TILE) * TILE
    units = length // 2
    f32 = jnp.float32
    dma = pltpu.SemaphoreType.DMA
    return pl.pallas_call(
        functools.partial(kernel, length, windows, nx, ny, ext, ey),
        out_shape=jax.ShapeDtypeStruct((nx, ny, nz), f32),
        in_specs=[pl.BlockSpec(memory_space=pl.ANY)] * 3,
        out_specs=pl.BlockSpec(memory_space=pl.ANY),
        scratch_shapes=[
            pltpu.VMEM((length, ext, ey, nz), f32),
            pltpu.VMEM((ext, ey, nz), f32),
            pltpu.VMEM((ext, ey, nz), f32),
            pltpu.VMEM((3 * length // 4, ext, ey, nz), f32),
            pltpu.VMEM((units, ext, ey, nz), f32),
            pltpu.VMEM((units, ext, ey, nz), f32),
            pltpu.VMEM((units, ext + 2, ey + 2 * TILE, nz), f32),
            pltpu.VMEM((units, ext + 2, ey + 2 * TILE, nz), f32),
            pltpu.VMEM((ext, ey, nz), f32),
            pltpu.VMEM((bs, TILE, nz), f32),
            pltpu.VMEM((bs, TILE, nz), f32),
            pltpu.VMEM((bs, TILE, nz), f32),
            pltpu.VMEM((bs, TILE, nz), f32),
            pltpu.VMEM((bs, TILE, nz), f32),
            pltpu.VMEM((half, bs, bsy, nz), f32),
            pltpu.VMEM((half, bs, bsy, nz), f32),
            pltpu.VMEM((half, bs, bsy, nz), f32),
            dma((4,)),
            dma((half,)),
            dma((length,)),
            dma((half,)),
            dma((2,)),
            dma((2,)),
            dma((18,)),
            dma((18,)),
            dma((half,)),
            dma((half,)),
            dma((half,)),
            dma((half,)),
        ],
        compiler_params=pltpu.CompilerParams(
            collective_id=0, has_side_effects=True, vmem_limit_bytes=28 * 1024 * 1024
        ),
    )(source[0, 0], initial_state, absorption)[None, None]


def spans(ext, bs, reach):
    bounds = [0, *range(reach + 5, ext, 4), ext]
    arrive = list(zip(bounds[:-1], bounds[1:]))
    final = [(max(0, a - reach), b - reach) for a, b in arrive]
    second = [(a, b, "own", e) for e, (a, b) in enumerate(final)]
    for e in reversed(range(len(final))):
        a, b = final[e]
        if b > bs - reach:
            a = max(a, bs - reach)
            second.append((2 * bs - b, 2 * bs - a, "beyond", e))
    leave = [(max(0, a - reach), b - reach) for a, b, _, _ in second if b > reach]
    return arrive, final, second, leave


def wave_kernel(
    length, windows, nx, ny, ext, ey, plan,
    source, initial, absorb, out,
    srcv, raw, first, absv, coef, level, fin, corr,
    emine, esend, egot, zgot, zother, csend, xsend, xgot, obuf,
    lsem, asend, brecv, fsend, esem_s, esem_r, zsem_s, zsem_r, csem_s, csem_r, xsem_s, xsem_r, osem_s, osem_r, hsem,
):
    arrive, final, second, leave = plan
    half = length // 2
    bs, bsy = nx // 2, ny // 2
    reach = SWEEPS - 1
    pairs = length // 4
    units = 2 * pairs
    kept = half // 2
    gamma = alpha_corner ** (1.0 / length)
    into, back, angles = tables(length)
    me = lax.axis_index("step")
    w = lax.axis_index("win")
    core, m = me % 2, me // 2
    partner = m * 2 + (1 - core)
    bx, by = m % 2, m // 2
    near = core == 1 - by

    def chip(b_x, b_y):
        return b_y * 2 + b_x

    def xlo(b):
        return b * (nx - ext)

    def ylo(b):
        return pl.multiple_of(b * (ny - ey), TILE)

    def rows_of(lo, hi, b=bx):
        return lo + b * (ext - lo - hi)

    def own_of(lo, hi, b=bx):
        return lo + b * (bs - lo - hi)

    def pick(a, b):
        if a == b:
            return jnp.float32(a)
        return jnp.where(core == 0, jnp.float32(a), jnp.float32(b))

    def region(ref, b_x, b_y, lo, hi):
        rows = pl.ds(xlo(b_x) + rows_of(lo, hi, b_x), hi - lo)
        return ref.at[rows, pl.ds(ylo(b_y), ey), :]

    ox = bx * bs - xlo(bx)
    oy = pl.multiple_of(by * bsy - ylo(by), TILE)

    loads = [
        pltpu.make_async_copy(source, srcv, lsem.at[0]),
        pltpu.make_async_copy(region(absorb, bx, by, 0, ext), absv, lsem.at[1]),
        pltpu.make_async_copy(region(source, bx, by, 0, ext), raw.at[me], lsem.at[2]),
        pltpu.make_async_copy(region(initial, bx, by, 0, ext), first, lsem.at[3]),
    ]
    for load in loads:
        load.start()

    barrier = pltpu.get_barrier_semaphore()

    def greet(**where):
        pl.semaphore_signal(barrier, inc=1, device_id=where, device_id_type=pl.DeviceIdType.MESH)

    for d in range(1, length):
        greet(step=(me + d) % length)

    @pl.when(w > 0)
    def _():
        greet(win=w - 1, step=me)
        greet(win=w - 1, step=partner)

    @pl.when(w < windows - 1)
    def _():
        greet(win=w + 1, step=me)
        greet(win=w + 1, step=partner)

    @pl.when(w == 0)
    def _():
        zgot[...] = jnp.zeros_like(zgot)
        zother[...] = jnp.zeros_like(zother)

    nearby = jnp.where(w > 0, 2, 0) + jnp.where(w < windows - 1, 2, 0)
    loads[0].wait()
    pl.semaphore_wait(barrier, length - 1 + nearby)

    def remote(src, dst, send, recv, **where):
        return pltpu.make_async_remote_copy(
            src_ref=src, dst_ref=dst, send_sem=send, recv_sem=recv,
            device_id=where, device_id_type=pl.DeviceIdType.MESH,
        )

    outgoing = []

    def launch(copy):
        copy.start()
        outgoing.append(copy)

    others = [(1, 1), (1, 0), (0, 1)]

    def beside(ex, e_y):
        return (bx + ex) % 2, (by + e_y) % 2

    for c, (lo, hi) in enumerate(arrive):
        for d, (ex, e_y) in enumerate(others):
            tx, ty = beside(ex, e_y)
            launch(
                remote(
                    region(srcv, tx, ty, lo, hi),
                    raw.at[me, pl.ds(rows_of(lo, hi, tx), hi - lo)],
                    asend.at[d, c], brecv.at[me, c], step=chip(tx, ty) * 2 + core,
                )
            )
        here = pl.ds(rows_of(lo, hi), hi - lo)
        launch(
            remote(
                region(srcv, bx, by, lo, hi), raw.at[me, here],
                asend.at[len(others), c], brecv.at[me, c], step=partner,
            )
        )

    zero_row = jnp.zeros((ey, LANES), jnp.float32)

    def rim(g, carry):
        k, u = g // units, g % units
        for r in (0, ext + 1):
            level[k, u, r, pl.ds(TILE, ey)] = zero_row
        for r in range(1, ext + 1):
            level[k, u, r, pl.ds(0, TILE)] = zero_row[:TILE]
            level[k, u, r, pl.ds(TILE + ey, TILE)] = zero_row[:TILE]
        return carry

    lax.fori_loop(0, reach * units, rim, 0)

    def grouped(begin, count, work, most):
        groups = -(-count // most)
        size = -(-count // groups)
        if groups == 1:
            work(begin, count)
            return

        def body(g, carry):
            work(begin + g * size, size)
            return carry

        lax.fori_loop(0, count // size, body, 0)
        if count % size:
            work(begin + count - count % size, count % size)

    loads[1].wait()

    def coefficients(start, rows):
        for n in range(rows):
            i = start + n
            for p in range(pairs):
                here = absv[i]
                cosine = pick(math.cos(angles[0][p]), math.cos(angles[1][p]))
                imag = pick(gamma * math.sin(angles[0][p]), gamma * math.sin(angles[1][p]))
                real = 1.0 - gamma * cosine + here + 6.0 * coupling
                over = coupling / (real * real + imag * imag)
                coef[3 * p, i] = real * over
                coef[3 * p + 1, i] = -imag * over
                if p == 0:
                    other = pick(-1.0, math.cos(angles[1][p]))
                    real = 1.0 - gamma * other + here + 6.0 * coupling
                    over = coupling / (real * real + imag * imag)
                    coef[3 * p + 2, i] = real * over

    grouped(0, ext, coefficients, 4)

    def weights(p, i, y0=0, rows=ey):
        part = pl.ds(y0, rows)
        straight = coef[3 * p, i, part]
        return straight, (coef[3 * p + 2, i, part] if p == 0 else straight), coef[3 * p + 1, i, part]

    is_first = jnp.where(w == 0, jnp.float32(1.0 / coupling), jnp.float32(0.0))

    def combine(pair, values):
        total = None
        for (a, b), value in zip(pair, values):
            if a == 0 and b == 0:
                continue
            term = value if a == 1 and b == 1 else pick(a, b) * value
            total = term if total is None else total + term
        return total

    def spectrum(start, rows):
        for n in range(rows):
            i = start + n
            folded = []
            for t in range(half):
                early, late = gamma**t / coupling, gamma ** (t + half) / coupling
                folded.append(early * raw[t, i] + pick(late, -late) * raw[t + half, i])
            folded[0] = folded[0] + first[i] * is_first
            for p in range(pairs):
                weight = weights(p, i)
                turn = [
                    [
                        tuple(into[c][t][2 * p + q] * coupling / gamma**t for c in range(2))
                        for t in range(half)
                    ]
                    for q in range(2)
                ]
                turn = [[tuple(round(v, 15) for v in pair) for pair in row] for row in turn]
                s0 = combine(turn[0], folded)
                s1 = combine(turn[1], folded)
                level[0, 2 * p, i + 1, pl.ds(TILE, ey)] = weight[0] * s0 - weight[2] * s1
                level[0, 2 * p + 1, i + 1, pl.ds(TILE, ey)] = weight[1] * s1 + weight[2] * s0

    def stencil(k, u, start, rows, y0, depth):
        lane = lax.broadcasted_iota(jnp.int32, (depth, LANES), 1)
        at = pl.multiple_of(y0 + TILE, TILE)
        line = [level[k, u, start + n, pl.ds(at, depth)] for n in range(rows + 2)]
        sums = []
        for n in range(1, rows + 1):
            v = line[n]
            around = level.at[k, u, start + n, pl.ds(y0, depth + 2 * TILE), :]
            total = jnp.where(lane == 0, 0.0, pltpu.roll(v, 1, 1))
            total = total + jnp.where(lane == LANES - 1, 0.0, pltpu.roll(v, LANES - 1, 1))
            across = around[pl.ds(TILE - 1, depth)] + around[pl.ds(TILE + 1, depth)]
            sums.append(total + ((line[n - 1] + line[n + 1]) + across))
        return sums

    def sweep_rows(k, start, rows):
        last = k == reach
        y0, depth = (oy, bsy) if last else (0, ey)
        at = pl.multiple_of(y0 + TILE, TILE)
        for p in range(pairs):
            s0 = stencil(k - 1, 2 * p, start, rows, y0, depth)
            s1 = stencil(k - 1, 2 * p + 1, start, rows, y0, depth)
            for n in range(rows):
                i = start + n
                weight = weights(p, i, y0, depth)
                b0 = level[0, 2 * p, i + 1, pl.ds(at, depth)]
                b1 = level[0, 2 * p + 1, i + 1, pl.ds(at, depth)]
                v0 = b0 + (weight[0] * s0[n] - weight[2] * s1[n])
                v1 = b1 + (weight[1] * s1[n] + weight[2] * s0[n])
                if last:
                    fin[2 * p, i - ox] = v0
                    fin[2 * p + 1, i - ox] = v1
                else:
                    level[k, 2 * p, i + 1, pl.ds(TILE, ey)] = v0
                    level[k, 2 * p + 1, i + 1, pl.ds(TILE, ey)] = v1

    def sweeps(a, b):
        for k in range(1, SWEEPS):
            lo, hi = max(0, a - k), b - k
            if hi > lo:
                grouped(rows_of(lo, hi), hi - lo, functools.partial(sweep_rows, k), 6)

    def part(t, start, rows, y0, depth):
        total = None
        for u in range(units):
            factor = pick(back[0][t[0]][u], back[1][t[1]][u])
            term = factor * fin[u, pl.ds(start, rows), pl.ds(y0, depth), :]
            total = term if total is None else total + term
        return total

    def strip(ref, lo, hi):
        return ref.at[pl.ds(own_of(lo, hi), hi - lo)]

    def swap(e):
        lo, hi = final[e]
        return remote(strip(esend, lo, hi), strip(egot, lo, hi), esem_s.at[e], esem_r.at[e], step=partner)

    def onward(e):
        lo, hi = final[e]
        after = (w + 1) % windows
        return [
            remote(
                strip(emine, lo, hi), strip(zgot, lo, hi),
                zsem_s.at[0, e], zsem_r.at[0, e], win=after, step=me,
            ),
            remote(
                strip(esend, lo, hi), strip(zother, lo, hi),
                zsem_s.at[1, e], zsem_r.at[1, e], win=after, step=partner,
            ),
        ]

    def finish(e):
        lo, hi = final[e]
        last = (length - 1, length - 1)
        start, rows = own_of(lo, hi), hi - lo
        esend[pl.ds(start, rows)] = part(last, start, rows, pl.multiple_of(TILE * (1 - core), TILE), TILE)
        emine[pl.ds(start, rows)] = part(last, start, rows, pl.multiple_of(TILE * core, TILE), TILE)
        launch(swap(e))

        @pl.when(w < windows - 1)
        def _():
            for copy in onward(e):
                copy.start()

    def landing(f_x, f_y, f_c, t_x, t_y, lo, hi):
        rows = pl.ds(f_x * bs + own_of(lo, hi, f_x) - xlo(t_x), hi - lo)
        depth = pl.ds(pl.multiple_of(f_y * bsy + TILE * f_c - ylo(t_y), TILE), TILE)
        return corr.at[rows, depth, :]

    def edge(e):
        lo, hi = final[e]
        return max(lo, bs - reach), hi

    def spread(e, act):
        lo, hi = final[e]

        def one(slot, where, to_core, lo, hi, recv):
            tx, ty = beside(*where)
            act(
                remote(
                    strip(csend, lo, hi), landing(bx, by, core, tx, ty, lo, hi),
                    csem_s.at[slot, e], csem_r.at[recv, e], step=chip(tx, ty) * 2 + to_core,
                )
            )

        lo2, hi2 = edge(e)
        if hi2 > lo2:

            @pl.when(near)
            def _():
                for c in range(2):
                    one(1 + c, (1, 1), c, lo2, hi2, 4)

            for c in range(2):
                one(3 + c, (1, 0), c, lo2, hi2, 2 + core)

        @pl.when(near)
        def _():
            for c in range(2):
                one(5 + c, (0, 1), c, lo, hi, 1)

        one(0, (0, 0), 1 - core, lo, hi, 0)

    def gather(e, kind):
        lo, hi = final[e]
        if kind == "own":
            sources = [(0, (0, 0), 1 - core), (1, (0, 1), by)]
        else:
            lo, hi = edge(e)
            sources = [(2, (1, 0), 0), (3, (1, 0), 1), (4, (1, 1), by)]
        for slot, where, f_c in sources:
            fx, fy = beside(*where)
            remote(
                strip(csend, lo, hi), landing(fx, fy, f_c, bx, by, lo, hi),
                csem_s.at[0, e], csem_r.at[slot, e], step=partner,
            ).wait_recv()

    def change(e):
        lo, hi = final[e]
        swap(e).wait_recv()

        @pl.when(w > 0)
        def _():
            for copy in onward(e):
                copy.wait_recv()

        mine = pl.ds(own_of(lo, hi), hi - lo)
        value = (zgot[mine] + zother[mine]) - alpha_corner * (emine[mine] + egot[mine])
        csend[mine] = value
        corr[pl.ds(ox + own_of(lo, hi), hi - lo), pl.ds(pl.multiple_of(oy + TILE * core, TILE), TILE), :] = value
        spread(e, lambda copy: copy.start())

    def arrival(t, c):
        lo, hi = arrive[c]
        return raw.at[t, pl.ds(rows_of(lo, hi), hi - lo)]

    for c, (a, b) in enumerate(arrive):
        for d, (ex, e_y) in enumerate(others):
            t = chip(*beside(ex, e_y)) * 2 + core
            block = arrival(t, c)
            copy = remote(block, block, fsend.at[d, c], brecv.at[t, c], step=partner)
            copy.wait_recv()
            launch(copy)
        if c == 0:
            loads[2].wait()
            loads[3].wait()
        for ex, e_y in [(0, 0), *others]:
            t = chip(*beside(ex, e_y)) * 2 + (1 - core)
            block = arrival(t, c)
            remote(block, block, fsend.at[0, c], brecv.at[t, c], step=partner).wait_recv()
        grouped(rows_of(a, b), b - a, spectrum, 3)
        sweeps(a, b)
        finish(c)
        if c:
            change(c - 1)

    def second_weight(p, weight):
        return weight[2] + (pick(1.0, 0.0) * weight[1] if p == 0 else 0.0)

    def correct(start, rows):
        for n in range(rows):
            i = start + n
            x = corr[i] * (1.0 / coupling)
            for p in range(pairs):
                weight = weights(p, i)
                spot = pl.ds(TILE, ey)
                level[0, 2 * p, i + 1, spot] = level[0, 2 * p, i + 1, spot] + weight[0] * x
                level[0, 2 * p + 1, i + 1, spot] = (
                    level[0, 2 * p + 1, i + 1, spot] + second_weight(p, weight) * x
                )

    def trade(i, o):
        lo, hi = leave[o]
        mine = pl.ds(own_of(lo, hi), hi - lo)
        return remote(xsend.at[i, mine], xgot.at[i, mine], xsem_s.at[i, o], xsem_r.at[i, o], step=partner)

    def emit(o):
        lo, hi = leave[o]
        start, rows = own_of(lo, hi), hi - lo
        for i in range(kept):
            xsend[i, pl.ds(start, rows)] = part((2 * i + 1, 2 * i), start, rows, 0, bsy)
            launch(trade(i, o))
        for i in range(kept):
            obuf[i, pl.ds(start, rows)] = part((2 * i, 2 * i + 1), start, rows, 0, bsy)

    def place(b_x, b_y, lo, hi):
        rows = pl.ds(b_x * bs + own_of(lo, hi, b_x), hi - lo)
        return out.at[rows, pl.ds(pl.multiple_of(b_y * bsy, TILE), bsy), :]

    def stay(k, o):
        lo, hi = leave[o]
        return pltpu.make_async_copy(strip(obuf.at[k], lo, hi), place(bx, by, lo, hi), hsem.at[o])

    def deliver(k, o, b_x, b_y, slot):
        lo, hi = leave[o]
        return remote(
            strip(obuf.at[k], lo, hi), place(b_x, b_y, lo, hi),
            osem_s.at[k, o], osem_r.at[slot, o], step=2 * k + core,
        )

    ratio = gamma ** (-half)

    def settle(o):
        lo, hi = leave[o]
        mine = pl.ds(own_of(lo, hi), hi - lo)
        for i in range(kept):
            trade(i, o).wait_recv()
            ours, theirs = obuf[i, mine], xgot[i, mine]
            obuf[i, mine] = ours + theirs
            obuf[i + kept, mine] = pick(ratio, -ratio) * (ours - theirs)
            for k in (i, i + kept):

                @pl.when(m == k)
                def _(k=k):
                    stay(k, o).start()

                @pl.when(m != k)
                def _(k=k):
                    deliver(k, o, bx, by, m).start()

    pending = len(final) - 1
    o = -1
    for g, (a, b, kind, e) in enumerate(second):
        if kind == "own" and e == pending - 1:
            change(pending)
        gather(e, kind)
        grouped(rows_of(a, b), b - a, correct, 5)
        sweeps(a, b)
        if b > reach:
            o += 1
            emit(o)
            if o:
                settle(o - 1)
    settle(o)

    for copy in outgoing:
        copy.wait_send()
    for e in range(len(final)):
        spread(e, lambda copy: copy.wait_send())

    @pl.when(w < windows - 1)
    def _():
        for e in range(len(final)):
            for copy in onward(e):
                copy.wait_send()

    for k in range(half):
        for o in range(len(leave)):

            @pl.when(m == k)
            def _(k=k, o=o):
                stay(k, o).wait()

            @pl.when(m != k)
            def _(k=k, o=o):
                done = deliver(k, o, k % 2, k // 2, k)
                done.wait_send()
                done.wait_recv()


def waves(initial_state, source, absorption):
    length = lax.axis_size("step")
    windows = lax.axis_size("win")
    nx, ny, nz = initial_state.shape
    half = length // 2
    reach = SWEEPS - 1
    bs, bsy = nx // 2, ny // 2
    ext = bs + reach
    ey = bsy + TILE
    units = length // 2
    plan = spans(ext, bs, reach)
    arrive, final, second, leave = (len(group) for group in plan)
    f32 = jnp.float32
    dma = pltpu.SemaphoreType.DMA
    edge = pltpu.VMEM((bs, TILE, nz), f32)
    return pl.pallas_call(
        functools.partial(wave_kernel, length, windows, nx, ny, ext, ey, plan),
        out_shape=jax.ShapeDtypeStruct((nx, ny, nz), f32),
        in_specs=[pl.BlockSpec(memory_space=pltpu.HBM)] * 3,
        out_specs=pl.BlockSpec(memory_space=pl.ANY),
        scratch_shapes=[
            pltpu.VMEM((nx, ny, nz), f32),
            pltpu.VMEM((length, ext, ey, nz), f32),
            pltpu.VMEM((ext, ey, nz), f32),
            pltpu.VMEM((ext, ey, nz), f32),
            pltpu.VMEM((3 * length // 4, ext, ey, nz), f32),
            pltpu.VMEM((reach, units, ext + 2, ey + 2 * TILE, nz), f32),
            pltpu.VMEM((units, bs, bsy, nz), f32),
            pltpu.VMEM((ext, ey, nz), f32),
            edge, edge, edge, edge, edge, edge,
            pltpu.VMEM((half // 2, bs, bsy, nz), f32),
            pltpu.VMEM((half // 2, bs, bsy, nz), f32),
            pltpu.VMEM((half, bs, bsy, nz), f32),
            dma((4,)),
            dma((half, arrive)),
            dma((length, arrive)),
            dma((half, arrive)),
            dma((final,)),
            dma((final,)),
            dma((2, final)),
            dma((2, final)),
            dma((7, final)),
            dma((5, final)),
            dma((half // 2, leave)),
            dma((half // 2, leave)),
            dma((half, leave)),
            dma((half, leave)),
            dma((leave,)),
        ],
        compiler_params=pltpu.CompilerParams(
            collective_id=0, has_side_effects=True, vmem_limit_bytes=40 * 1024 * 1024
        ),
    )(source[0, 0], initial_state, absorption)[None, None]


def fits(mesh, shape):
    length = mesh.shape["step"]
    if length % 8 or shape[2] != LANES or shape[1] != 4 * TILE:
        return False
    gx = length // 4
    return shape[0] % gx == 0 and shape[0] // gx >= SWEEPS - 1


def pairs_up(mesh, shape):
    return mesh.shape["step"] == 8 and shape[0] // 2 >= 2 * SWEEPS


def solution(mesh):
    def body(initial_state, source, absorption):
        plan = per_device
        if fits(mesh, initial_state.shape):
            plan = waves if pairs_up(mesh, initial_state.shape) else blocks
        return plan(initial_state, source, absorption)

    return jax.shard_map(
        body,
        mesh=mesh,
        in_specs=(P(), P("win", "step", None, None, None), P()),
        out_specs=P("win", "step", None, None, None),
        check_vma=False,
    )
```

```python
import functools
import math

import jax
import jax.numpy as jnp
from jax import lax
from jax.experimental import pallas as pl
from jax.experimental.pallas import tpu as pltpu
from jax.sharding import PartitionSpec as P

ITERS = 2
SWEEPS = 8


alpha_corner = 0.1
coupling = 0.05


def from_behind(block, axis, distance):
    devices = range(lax.axis_size(axis))
    route = [(i - distance, i) for i in devices if i - distance in devices]
    return lax.ppermute(block, axis, route)


def pad_cube(field):
    widths = [(0, 0)] * (field.ndim - 3) + [(1, 1)] * 3
    return jnp.pad(field, widths)


def neighbours(field):
    padded = pad_cube(field)
    total = padded[..., 2:, 1:-1, 1:-1] + padded[..., :-2, 1:-1, 1:-1]
    total = total + padded[..., 1:-1, 2:, 1:-1] + padded[..., 1:-1, :-2, 1:-1]
    total = total + padded[..., 1:-1, 1:-1, 2:] + padded[..., 1:-1, 1:-1, :-2]
    return total


def complex_times(first, second):
    return jnp.stack(
        [first[0] * second[0] - first[1] * second[1], first[0] * second[1] + first[1] * second[0]]
    )


def relax(spectrum, inverse):
    field = complex_times(inverse, spectrum)
    for repeat in range(SWEEPS - 1):
        field = complex_times(inverse, spectrum + coupling * neighbours(field))
    return field


def inverse_diagonal(angle, absorption, gamma):
    real_part = 1.0 - gamma * jnp.cos(angle) + absorption + 6.0 * coupling
    imag_part = jnp.broadcast_to(gamma * jnp.sin(angle), real_part.shape)
    magnitude = real_part * real_part + imag_part * imag_part
    return jnp.stack([real_part / magnitude, -imag_part / magnitude])


def dft_tables(window_len):
    index = jnp.arange(window_len, dtype=jnp.int32)
    product = index[:, None] * index[None, :] % window_len
    angle = product.astype(jnp.float32) * (2.0 * math.pi / window_len)
    return (jnp.cos(angle), jnp.sin(angle))


def transform_exchange(scaled, window_len):
    pencil = lax.all_to_all(scaled[None], "step", split_axis=1, concat_axis=0, tiled=True)
    cosine, sine = dft_tables(window_len)
    flat = pencil.reshape(window_len, -1)
    real_part = jnp.dot(cosine, flat, precision=lax.Precision.HIGHEST)
    imag_part = -jnp.dot(sine, flat, precision=lax.Precision.HIGHEST)
    shaped = pencil.shape
    spectrum = (
        lax.all_to_all(real_part.reshape(shaped), "step", split_axis=0, concat_axis=1, tiled=True),
        lax.all_to_all(imag_part.reshape(shaped), "step", split_axis=0, concat_axis=1, tiled=True),
    )
    return jnp.stack([spectrum[0][0], spectrum[1][0]])


def untransform_exchange(field, window_len):
    pencil = (
        lax.all_to_all(field[0][None], "step", split_axis=1, concat_axis=0, tiled=True),
        lax.all_to_all(field[1][None], "step", split_axis=1, concat_axis=0, tiled=True),
    )
    cosine, sine = dft_tables(window_len)
    shaped = pencil[0].shape
    values = jnp.dot(cosine, pencil[0].reshape(window_len, -1), precision=lax.Precision.HIGHEST)
    values = values - jnp.dot(
        sine, pencil[1].reshape(window_len, -1), precision=lax.Precision.HIGHEST
    )
    values = values / window_len
    result = lax.all_to_all(values.reshape(shaped), "step", split_axis=0, concat_axis=1, tiled=True)
    return result[0]


def per_device(initial_state, source, absorption):
    window_len = lax.axis_size("step")
    moment = lax.axis_index("step")
    window_index = lax.axis_index("win")
    gamma = alpha_corner ** (1.0 / window_len)
    scale = gamma ** moment.astype(jnp.float32)
    forcing_base = source[0, 0]
    is_first = moment == 0
    state = jnp.zeros_like(forcing_base)
    angle = moment.astype(jnp.float32) * (2.0 * math.pi / window_len)
    inverse = inverse_diagonal(angle, absorption, gamma)
    for repeat in range(ITERS):
        if repeat == 0:
            correction = jnp.where(window_index == 0, initial_state, 0.0)
        else:
            ends = from_behind(state, "step", 1 - window_len)
            before = from_behind(ends, "win", 1)
            before = jnp.where(window_index == 0, initial_state, before)
            correction = before - alpha_corner * ends
        forcing = forcing_base + jnp.where(is_first, correction, 0.0)
        scaled = forcing * scale
        spectrum = transform_exchange(scaled, window_len)
        field = relax(spectrum, inverse)
        values = untransform_exchange(field, window_len)
        state = values / scale
    return state[None, None]


LANES = 128
TILE = 8
GROUP = 8


def tables(length):
    gamma = alpha_corner ** (1.0 / length)
    into, back, angles = [], [], []
    for core in range(2):
        rows_in, rows_back = [], []
        for time in range(length):
            scale = gamma**time
            row_in, row_back = [], []
            for p in range(length // 4):
                j = 2 * p + core
                if j == 0:
                    pair, weight = (1.0, (-1.0) ** time), 1.0 / length
                else:
                    turn = 2.0 * math.pi * (j * time % length) / length
                    pair, weight = (math.cos(turn), -math.sin(turn)), 2.0 / length
                row_in += [value * scale / coupling for value in pair]
                row_back += [value * weight / scale for value in pair]
            rows_in.append(row_in)
            rows_back.append(row_back)
        into.append(rows_in)
        back.append(rows_back)
        angles.append([2.0 * math.pi * (2 * p + core) / length for p in range(length // 4)])
    return into, back, angles


def kernel(
    length, windows, nx, ny, ext, ey,
    source, initial, absorb, out,
    raw, first, absv, coef, base, again, fa, fb, corr,
    psend, pgot, ends, zgot, csend, qsend, qgot, obuf,
    lsem, asend, brecv, fsend, esem, zsem, csem_s, csem_r, qsem_s, qsem_r, osem_s, osem_r,
):
    half = length // 2
    gx, gy = half // 2, 2
    bs, bsy = nx // gx, ny // gy
    reach = SWEEPS - 1
    pairs = length // 4
    units = 2 * pairs
    gamma = alpha_corner ** (1.0 / length)
    into, back, angles = tables(length)
    me = lax.axis_index("step")
    w = lax.axis_index("win")
    core, m = me % 2, me // 2
    partner = m * 2 + (1 - core)
    bx, by = m % gx, m // gx

    def xlo(b):
        if gx == 2:
            return b * (nx - ext)
        return jnp.minimum(jnp.maximum(b * bs - reach, 0), nx - ext)

    def ylo(b):
        return pl.multiple_of(b * (ny - ey), TILE)

    def pick(a, b):
        return jnp.where(core == 0, jnp.float32(a), jnp.float32(b))

    def region(ref, b_x, b_y):
        return ref.at[pl.ds(xlo(b_x), ext), pl.ds(ylo(b_y), ey), :]

    ox = bx * bs - xlo(bx)
    oy = pl.multiple_of(by * bsy - ylo(by), TILE)

    loads = [
        pltpu.make_async_copy(region(absorb, bx, by), absv, lsem.at[0]),
        pltpu.make_async_copy(region(source, bx, by), raw.at[me], lsem.at[1]),
        pltpu.make_async_copy(region(initial, bx, by), first, lsem.at[2]),
    ]
    for load in loads:
        load.start()
    zero_row = jnp.zeros((ey, LANES), jnp.float32)
    for u in range(units):
        for ref in (fa, fb):
            ref[u, 0, pl.ds(TILE, ey)] = zero_row
            ref[u, ext + 1, pl.ds(TILE, ey)] = zero_row
            for r in range(1, ext + 1):
                ref[u, r, pl.ds(0, TILE)] = zero_row[:TILE]
                ref[u, r, pl.ds(TILE + ey, TILE)] = zero_row[:TILE]
    if gx > 2:
        corr[...] = jnp.zeros_like(corr)

    barrier = pltpu.get_barrier_semaphore()
    for d in range(1, length):
        pl.semaphore_signal(
            barrier, inc=1, device_id={"step": (me + d) % length}, device_id_type=pl.DeviceIdType.MESH
        )

    @pl.when(w > 0)
    def _():
        pl.semaphore_signal(barrier, inc=1, device_id={"win": w - 1}, device_id_type=pl.DeviceIdType.MESH)

    @pl.when(w < windows - 1)
    def _():
        pl.semaphore_signal(barrier, inc=1, device_id={"win": w + 1}, device_id_type=pl.DeviceIdType.MESH)

    nearby = jnp.where(w > 0, 1, 0) + jnp.where(w < windows - 1, 1, 0)
    pl.semaphore_wait(barrier, length - 1 + nearby)

    def remote(src, dst, send, recv, **where):
        return pltpu.make_async_remote_copy(
            src_ref=src, dst_ref=dst, send_sem=send, recv_sem=recv,
            device_id=where, device_id_type=pl.DeviceIdType.MESH,
        )

    outgoing = []
    for d in range(1, half):
        to = (m + d) % half
        copy = remote(
            region(source, to % gx, to // gx), raw.at[me], asend.at[d], brecv.at[me], step=to * 2 + core
        )
        copy.start()
        outgoing.append(copy)
    copy = remote(region(source, bx, by), raw.at[me], asend.at[0], brecv.at[me], step=partner)
    copy.start()
    outgoing.append(copy)

    def grouped(begin, count, work, most=GROUP):
        size = -(-count // max(1, count // most))

        def body(g, carry):
            work(begin + g * size, size)
            return carry

        lax.fori_loop(0, count // size, body, 0)
        if count % size:
            work(begin + count - size, size)

    def each(one):
        def work(start, rows):
            for n in range(rows):
                one(start + n)

        return work

    loads[0].wait()

    def coefficients(i):
        for p in range(pairs):
            rows = absv[i]
            cosine = pick(math.cos(angles[0][p]), math.cos(angles[1][p]))
            imag = pick(gamma * math.sin(angles[0][p]), gamma * math.sin(angles[1][p]))
            real = 1.0 - gamma * cosine + rows + 6.0 * coupling
            over = coupling / (real * real + imag * imag)
            coef[3 * p, i] = real * over
            coef[3 * p + 1, i] = -imag * over
            if p == 0:
                other = pick(-1.0, math.cos(angles[1][p]))
                real = 1.0 - gamma * other + rows + 6.0 * coupling
                over = coupling / (real * real + imag * imag)
                coef[3 * p + 2, i] = real * over

    grouped(0, ext, each(coefficients))

    def weights(p, i):
        straight = coef[3 * p, i]
        return straight, (coef[3 * p + 2, i] if p == 0 else straight), coef[3 * p + 1, i]

    def arrival(t):
        return remote(raw.at[t], raw.at[t], asend.at[0], brecv.at[t], step=partner)

    for d in range(1, half):
        t = ((m + half - d) % half) * 2 + core
        arrival(t).wait_recv()
        copy = remote(raw.at[t], raw.at[t], fsend.at[d], brecv.at[t], step=partner)
        copy.start()
        outgoing.append(copy)
    for d in range(half):
        arrival(((m + half - d) % half) * 2 + (1 - core)).wait_recv()
    loads[1].wait()
    loads[2].wait()
    is_first = jnp.where(w == 0, jnp.float32(1.0 / coupling), jnp.float32(0.0))

    def second_weight(p, weight):
        return weight[2] + (pick(1.0, 0.0) * weight[1] if p == 0 else 0.0)

    def transform(i):
        begin = first[i] * is_first
        fields = [raw[t, i] for t in range(length)]
        for p in range(pairs):
            weight = weights(p, i)
            s0, s1 = begin, begin * pick(1.0, 0.0) if p == 0 else None
            for t in range(length):
                s0 = s0 + pick(into[0][t][2 * p], into[1][t][2 * p]) * fields[t]
                term = pick(into[0][t][2 * p + 1], into[1][t][2 * p + 1]) * fields[t]
                s1 = term if s1 is None else s1 + term
            b0 = weight[0] * s0 - weight[2] * s1
            b1 = weight[1] * s1 + weight[2] * s0
            base[2 * p, i] = b0
            base[2 * p + 1, i] = b1
            fa[2 * p, i + 1, pl.ds(TILE, ey)] = b0
            fa[2 * p + 1, i + 1, pl.ds(TILE, ey)] = b1

    grouped(0, ext, each(transform), GROUP // 2)

    lane = lax.broadcasted_iota(jnp.int32, (ey, LANES), 1)

    def around(ref, u, r):
        v = ref[u, r, pl.ds(TILE, ey)]
        total = jnp.where(lane == 0, 0.0, pltpu.roll(v, 1, 1))
        total = total + jnp.where(lane == LANES - 1, 0.0, pltpu.roll(v, LANES - 1, 1))
        beside = ref[u, r - 1, pl.ds(TILE, ey)] + ref[u, r + 1, pl.ds(TILE, ey)]
        return total + (beside + (ref[u, r, pl.ds(TILE - 1, ey)] + ref[u, r, pl.ds(TILE + 1, ey)]))

    def sweep_rows(base, here, there, start, rows):
        for n in range(rows):
            i = start + n
            for p in range(pairs):
                weight = weights(p, i)
                n0 = around(here, 2 * p, i + 1)
                n1 = around(here, 2 * p + 1, i + 1)
                there[2 * p, i + 1, pl.ds(TILE, ey)] = base[2 * p, i] + (weight[0] * n0 - weight[2] * n1)
                there[2 * p + 1, i + 1, pl.ds(TILE, ey)] = base[2 * p + 1, i] + (
                    weight[1] * n1 + weight[2] * n0
                )

    def sweeps(base):
        here, there = fa, fb
        for k in range(1, SWEEPS):
            begin, count = (bx * k, ext - k) if gx == 2 else (0, ext)
            grouped(begin, count, functools.partial(sweep_rows, base, here, there))
            here, there = there, here
        return here

    final = sweeps(base)

    def part(t, y0, rows):
        total = None
        for u in range(units):
            factor = pick(back[0][t[0]][u], back[1][t[1]][u])
            term = factor * final[u, pl.ds(ox + 1, bs), pl.ds(y0 + TILE, rows), :]
            total = term if total is None else total + term
        return total

    last = (length - 1, length - 1)
    psend[...] = part(last, pl.multiple_of(oy + TILE * (1 - core), TILE), TILE)
    swap = remote(psend, pgot, esem.at[0], esem.at[1], step=partner)
    swap.start()
    mine = part(last, pl.multiple_of(oy + TILE * core, TILE), TILE)
    swap.wait_recv()
    mine = mine + pgot[...]
    ends[...] = mine
    outgoing.append(swap)

    onward = remote(ends, zgot, zsem.at[0], zsem.at[1], win=(w + 1) % windows)

    @pl.when(w < windows - 1)
    def _():
        onward.start()

    @pl.when(w == 0)
    def _():
        zgot[...] = jnp.zeros_like(zgot)

    @pl.when(w > 0)
    def _():
        onward.wait_recv()

    change = zgot[...] - alpha_corner * ends[...]
    csend[...] = change
    corr[pl.ds(ox, bs), pl.ds(pl.multiple_of(oy + TILE * core, TILE), TILE), :] = change

    def spread(ex, ey_, send):
        rows, skip = (bs, 0) if ex == 0 else (reach, bs - reach if ex == 1 else 0)
        tx, ty = (bx + ex, by + ey_) if send else (bx, by)
        fx, fy = (bx, by) if send else (bx - ex, by - ey_)
        ax, ay = (tx, ty) if send else (fx, fy)
        inside = (ax >= 0) & (ax < gx) & (ay >= 0) & (ay < gy)
        slot = ((ex + 1) * 3 + (ey_ + 1)) * 2
        for c in range(2):
            near = c == (1 if ey_ == 1 else 0)
            if send:
                okay = inside if ey_ == 0 else inside & (core == (1 if ey_ == 1 else 0))
                if ex == 0 and ey_ == 0:
                    okay = core != c
                fc, tc = core, c
            else:
                if ey_ != 0 and not near:
                    continue
                okay = inside
                if ex == 0 and ey_ == 0:
                    okay = core != c
                fc, tc = c, core

            @pl.when(okay)
            def _(c=c, fc=fc, tc=tc):
                copy = remote(
                    csend.at[pl.ds(skip, rows)],
                    corr.at[
                        pl.ds(fx * bs + skip - xlo(tx), rows),
                        pl.ds(pl.multiple_of(fy * bsy + TILE * fc - ylo(ty), TILE), TILE),
                        :,
                    ],
                    csem_s.at[slot + c],
                    csem_r.at[slot + fc],
                    step=(ty * gx + tx) * 2 + tc if send == 1 else partner,
                )
                if send == 1:
                    copy.start()
                elif send == 2:
                    copy.wait_send()
                else:
                    copy.wait_recv()

    offsets = [(ex, e) for ex in (-1, 0, 1) for e in (-1, 0, 1)]
    for ex, e in offsets:
        spread(ex, e, 1)
    for ex, e in offsets:
        spread(ex, e, 0)

    def correct(i):
        x = corr[i] * (1.0 / coupling)
        for p in range(pairs):
            weight = weights(p, i)
            b0 = base[2 * p, i] + weight[0] * x
            b1 = base[2 * p + 1, i] + second_weight(p, weight) * x
            again[2 * p, i] = b0
            again[2 * p + 1, i] = b1
            fa[2 * p, i + 1, pl.ds(TILE, ey)] = b0
            fa[2 * p + 1, i + 1, pl.ds(TILE, ey)] = b1

    grouped(0, ext, each(correct))
    final = sweeps(again)

    for k in range(half):
        qsend[k] = part((2 * k + 1, 2 * k), oy, bsy)
        copy = remote(qsend.at[k], qgot.at[k], qsem_s.at[k], qsem_r.at[k], step=partner)
        copy.start()
        outgoing.append(copy)
    for k in range(half):
        obuf[k] = part((2 * k, 2 * k + 1), oy, bsy)

    def place(b_x, b_y):
        return out.at[pl.ds(b_x * bs, bs), pl.ds(pl.multiple_of(b_y * bsy, TILE), bsy), :]

    for k in range(half):
        remote(qsend.at[k], qgot.at[k], qsem_s.at[k], qsem_r.at[k], step=partner).wait_recv()
        obuf[k] = obuf[k] + qgot[k]

        @pl.when(m == k)
        def _(k=k):
            pltpu.make_async_copy(obuf.at[k], place(bx, by), lsem.at[3]).start()

        @pl.when(m != k)
        def _(k=k):
            remote(obuf.at[k], place(bx, by), osem_s.at[k], osem_r.at[m], step=2 * k + core).start()

    for copy in outgoing:
        copy.wait_send()
    for ex, e in offsets:
        spread(ex, e, 2)

    @pl.when(w < windows - 1)
    def _():
        onward.wait_send()

    for k in range(half):

        @pl.when(m == k)
        def _(k=k):
            pltpu.make_async_copy(obuf.at[k], place(bx, by), lsem.at[3]).wait()

        @pl.when(m != k)
        def _(k=k):
            done = remote(obuf.at[k], place(k % gx, k // gx), osem_s.at[k], osem_r.at[k], step=partner)
            done.wait_send()
            done.wait_recv()


def blocks(initial_state, source, absorption):
    length = lax.axis_size("step")
    windows = lax.axis_size("win")
    nx, ny, nz = initial_state.shape
    half = length // 2
    gx, reach = half // 2, SWEEPS - 1
    bs, bsy = nx // gx, ny // 2
    ext = min(nx, bs + reach * (1 if gx == 2 else 2))
    ey = bsy + -(-reach // TILE) * TILE
    units = length // 2
    f32 = jnp.float32
    dma = pltpu.SemaphoreType.DMA
    return pl.pallas_call(
        functools.partial(kernel, length, windows, nx, ny, ext, ey),
        out_shape=jax.ShapeDtypeStruct((nx, ny, nz), f32),
        in_specs=[pl.BlockSpec(memory_space=pl.ANY)] * 3,
        out_specs=pl.BlockSpec(memory_space=pl.ANY),
        scratch_shapes=[
            pltpu.VMEM((length, ext, ey, nz), f32),
            pltpu.VMEM((ext, ey, nz), f32),
            pltpu.VMEM((ext, ey, nz), f32),
            pltpu.VMEM((3 * length // 4, ext, ey, nz), f32),
            pltpu.VMEM((units, ext, ey, nz), f32),
            pltpu.VMEM((units, ext, ey, nz), f32),
            pltpu.VMEM((units, ext + 2, ey + 2 * TILE, nz), f32),
            pltpu.VMEM((units, ext + 2, ey + 2 * TILE, nz), f32),
            pltpu.VMEM((ext, ey, nz), f32),
            pltpu.VMEM((bs, TILE, nz), f32),
            pltpu.VMEM((bs, TILE, nz), f32),
            pltpu.VMEM((bs, TILE, nz), f32),
            pltpu.VMEM((bs, TILE, nz), f32),
            pltpu.VMEM((bs, TILE, nz), f32),
            pltpu.VMEM((half, bs, bsy, nz), f32),
            pltpu.VMEM((half, bs, bsy, nz), f32),
            pltpu.VMEM((half, bs, bsy, nz), f32),
            dma((4,)),
            dma((half,)),
            dma((length,)),
            dma((half,)),
            dma((2,)),
            dma((2,)),
            dma((18,)),
            dma((18,)),
            dma((half,)),
            dma((half,)),
            dma((half,)),
            dma((half,)),
        ],
        compiler_params=pltpu.CompilerParams(
            collective_id=0, has_side_effects=True, vmem_limit_bytes=28 * 1024 * 1024
        ),
    )(source[0, 0], initial_state, absorption)[None, None]


ARRIVE = (8, 4, 3, 3, 3)
SECOND = (5, 3, 3, 3, 3, 3)
LEAST = 3


def cuts(sizes, extent):
    bounds = [0]
    for size in sizes:
        if bounds[-1] + size < extent:
            bounds.append(bounds[-1] + size)
    bounds.append(extent)
    return list(zip(bounds[:-1], bounds[1:]))


def spans(ext, bs, reach):
    arrive = cuts(ARRIVE, ext)
    final = [(max(0, a - reach), b - reach) for a, b in arrive if b > reach]
    sources = [(a, b, "own", e) for e, (a, b) in enumerate(final)]
    for e, (a, b) in enumerate(final):
        if b > bs - reach:
            sources.append((2 * bs - b, 2 * bs - max(a, bs - reach), "beyond", e))
    second, leave, after, sent = [], [], {}, 0
    groups = cuts(SECOND, ext)
    for g, (a, b) in enumerate(groups):
        needs = [(kind, e) for lo, hi, kind, e in sources if a <= lo < b or (lo < a and g == 0)]
        second.append((a, b, needs))
        if b - reach - sent >= LEAST or g == len(groups) - 1:
            after[g] = len(leave)
            leave.append((sent, b - reach))
            sent = b - reach
    return arrive, final, second, leave, after


def wave_kernel(
    length, windows, nx, ny, ext, ey, plan,
    source, initial, absorb, out,
    srcv, raw, first, absv, coef, levels, fin, corr,
    emine, esend, egot, zgot, csend, xsend, xgot, obuf,
    lsem, asem, isem, fsem, dsem, esem_s, esem_r, zsem_s, zsem_r, csem_s, csem_r, bsem_r, xsem_s, xsem_r, osem, hsem,
):
    arrive, final, second, leave, after = plan
    half = length // 2
    bs, bsy = nx // 2, ny // 2
    reach = SWEEPS - 1
    pairs = length // 4
    units = 2 * pairs
    kept = half // 2
    gamma = alpha_corner ** (1.0 / length)
    into, back, angles = tables(length)
    me = lax.axis_index("step")
    w = lax.axis_index("win")
    core, m = me % 2, me // 2
    partner = m * 2 + (1 - core)
    bx, by = m % 2, m // 2
    near = core == 1 - by

    def chip(b_x, b_y):
        return b_y * 2 + b_x

    def xlo(b):
        return b * (nx - ext)

    def ylo(b):
        return pl.multiple_of(b * (ny - ey), TILE)

    def rows_of(lo, hi, b=bx):
        return lo + b * (ext - lo - hi)

    def own_of(lo, hi, b=bx):
        return lo + b * (bs - lo - hi)

    def pick(a, b):
        if a == b:
            return jnp.float32(a)
        return jnp.where(core == 0, jnp.float32(a), jnp.float32(b))

    def region(ref, b_x, b_y, lo, hi):
        rows = pl.ds(xlo(b_x) + rows_of(lo, hi, b_x), hi - lo)
        return ref.at[rows, pl.ds(ylo(b_y), ey), :]

    ox = bx * bs - xlo(bx)
    oy = pl.multiple_of(by * bsy - ylo(by), TILE)

    loads = [
        pltpu.make_async_copy(source, srcv, lsem.at[0]),
        pltpu.make_async_copy(region(absorb, bx, by, 0, ext), absv, lsem.at[1]),
        pltpu.make_async_copy(region(source, bx, by, 0, ext), raw.at[core, m], lsem.at[2]),
        pltpu.make_async_copy(region(initial, bx, by, 0, ext), first, lsem.at[3]),
    ]
    for load in loads:
        load.start()

    barrier = pltpu.get_barrier_semaphore()

    def greet(**where):
        pl.semaphore_signal(barrier, inc=1, device_id=where, device_id_type=pl.DeviceIdType.MESH)

    for d in range(1, length):
        greet(step=(me + d) % length)

    @pl.when(w > 0)
    def _():
        greet(win=w - 1, step=me)
        greet(win=w - 1, step=partner)

    @pl.when(w < windows - 1)
    def _():
        greet(win=w + 1, step=me)
        greet(win=w + 1, step=partner)

    @pl.when(w == 0)
    def _():
        zgot[...] = jnp.zeros_like(zgot)

    nearby = jnp.where(w > 0, 2, 0) + jnp.where(w < windows - 1, 2, 0)
    loads[0].wait()
    pl.semaphore_wait(barrier, length - 1 + nearby)

    def remote(src, dst, send, recv, **where):
        return pltpu.make_async_remote_copy(
            src_ref=src, dst_ref=dst, send_sem=send, recv_sem=recv,
            device_id=where, device_id_type=pl.DeviceIdType.MESH,
        )

    def taken(block, sem):
        return remote(block, block, sem, sem, step=partner)

    others = [(1, 1), (1, 0), (0, 1)]

    def beside(ex, e_y):
        return (bx + ex) % 2, (by + e_y) % 2

    for c, (lo, hi) in enumerate(arrive):
        for where in others:
            tx, ty = beside(*where)
            remote(
                region(srcv, tx, ty, lo, hi),
                raw.at[core, m, pl.ds(rows_of(lo, hi, tx), hi - lo)],
                asem, isem.at[c], step=chip(tx, ty) * 2 + core,
            ).start()

    zero_row = jnp.zeros((ey, LANES), jnp.float32)

    def rim(r, carry):
        for refs in levels:
            for ref in refs:
                for q in range(2):
                    ref[q, r, pl.ds(0, TILE)] = zero_row[:TILE]
                    ref[q, r, pl.ds(TILE + ey, TILE)] = zero_row[:TILE]
        return carry

    for refs in levels:
        for ref in refs:
            for q in range(2):
                for r in (0, ext + 1):
                    ref[q, r, pl.ds(TILE, ey)] = zero_row
    lax.fori_loop(1, ext + 1, rim, 0)

    def grouped(begin, count, work, most):
        groups = -(-count // most)
        size = -(-count // groups)
        if groups == 1:
            work(begin, count)
            return

        def body(g, carry):
            work(begin + g * size, size)
            return carry

        lax.fori_loop(0, count // size, body, 0)
        if count % size:
            work(begin + count - count % size, count % size)

    loads[1].wait()

    def coefficients(start, rows):
        for n in range(rows):
            i = start + n
            for p in range(pairs):
                here = absv[i]
                cosine = pick(math.cos(angles[0][p]), math.cos(angles[1][p]))
                imag = pick(gamma * math.sin(angles[0][p]), gamma * math.sin(angles[1][p]))
                real = 1.0 - gamma * cosine + here + 6.0 * coupling
                over = coupling / (real * real + imag * imag)
                coef[3 * p, i] = real * over
                coef[3 * p + 1, i] = -imag * over
                if p == 0:
                    other = pick(-1.0, math.cos(angles[1][p]))
                    real = 1.0 - gamma * other + here + 6.0 * coupling
                    over = coupling / (real * real + imag * imag)
                    coef[3 * p + 2, i] = real * over

    grouped(0, ext, coefficients, 4)

    def weights(p, i, y0=0, rows=ey):
        part = pl.ds(y0, rows)
        straight = coef[3 * p, i, part]
        return straight, (coef[3 * p + 2, i, part] if p == 0 else straight), coef[3 * p + 1, i, part]

    is_first = jnp.where(w == 0, jnp.float32(1.0 / coupling), jnp.float32(0.0))

    def combine(pair, values):
        total = None
        for (a, b), value in zip(pair, values):
            if a == 0 and b == 0:
                continue
            term = value if a == 1 and b == 1 else pick(a, b) * value
            total = term if total is None else total + term
        return total

    def spectrum(start, rows):
        for n in range(rows):
            i = start + n
            folded = []
            for t in range(half):
                early, late = gamma**t / coupling, gamma ** (t + half) / coupling
                now, then = raw[t % 2, t // 2, i], raw[t % 2, (t + half) // 2, i]
                folded.append(early * now + pick(late, -late) * then)
            folded[0] = folded[0] + first[i] * is_first
            for p in range(pairs):
                weight = weights(p, i)
                turn = [
                    [
                        tuple(into[c][t][2 * p + q] * coupling / gamma**t for c in range(2))
                        for t in range(half)
                    ]
                    for q in range(2)
                ]
                turn = [[tuple(round(v, 15) for v in pair) for pair in row] for row in turn]
                s0 = combine(turn[0], folded)
                s1 = combine(turn[1], folded)
                levels[0][p][0, i + 1, pl.ds(TILE, ey)] = weight[0] * s0 - weight[2] * s1
                levels[0][p][1, i + 1, pl.ds(TILE, ey)] = weight[1] * s1 + weight[2] * s0

    def stencil(ref, q, start, rows, y0, depth):
        lane = lax.broadcasted_iota(jnp.int32, (depth, LANES), 1)
        at = pl.multiple_of(y0 + TILE, TILE)
        line = [ref[q, start + n, pl.ds(at, depth)] for n in range(rows + 2)]
        sums = []
        for n in range(1, rows + 1):
            v = line[n]
            around = ref.at[q, start + n, pl.ds(y0, depth + 2 * TILE), :]
            total = jnp.where(lane == 0, 0.0, pltpu.roll(v, 1, 1))
            total = total + jnp.where(lane == LANES - 1, 0.0, pltpu.roll(v, LANES - 1, 1))
            across = around[pl.ds(TILE - 1, depth)] + around[pl.ds(TILE + 1, depth)]
            sums.append(total + ((line[n - 1] + line[n + 1]) + across))
        return sums

    def sweep_rows(k, start, rows):
        last = k == reach
        y0, depth = (oy, bsy) if last else (0, ey)
        at = pl.multiple_of(y0 + TILE, TILE)
        for p in range(pairs):
            s0 = stencil(levels[k - 1][p], 0, start, rows, y0, depth)
            s1 = stencil(levels[k - 1][p], 1, start, rows, y0, depth)
            for n in range(rows):
                i = start + n
                weight = weights(p, i, y0, depth)
                b0 = levels[0][p][0, i + 1, pl.ds(at, depth)]
                b1 = levels[0][p][1, i + 1, pl.ds(at, depth)]
                v0 = b0 + (weight[0] * s0[n] - weight[2] * s1[n])
                v1 = b1 + (weight[1] * s1[n] + weight[2] * s0[n])
                if last:
                    fin[p][0, i - ox] = v0
                    fin[p][1, i - ox] = v1
                else:
                    levels[k][p][0, i + 1, pl.ds(TILE, ey)] = v0
                    levels[k][p][1, i + 1, pl.ds(TILE, ey)] = v1

    def sweeps(a, b):
        for k in range(1, SWEEPS):
            lo, hi = max(0, a - k), b - k
            if hi > lo:
                grouped(rows_of(lo, hi), hi - lo, functools.partial(sweep_rows, k), 6)

    def part(t, start, rows, y0, depth):
        total = None
        for u in range(units):
            factor = pick(back[0][t[0]][u], back[1][t[1]][u])
            term = factor * fin[u // 2][u % 2, pl.ds(start, rows), pl.ds(y0, depth), :]
            total = term if total is None else total + term
        return total

    def strip(ref, lo, hi):
        return ref.at[pl.ds(own_of(lo, hi), hi - lo)]

    def swap(e):
        lo, hi = final[e]
        return remote(strip(esend, lo, hi), strip(egot, lo, hi), esem_s, esem_r.at[e], step=partner)

    def onward(e):
        lo, hi = final[e]
        after_w = (w + 1) % windows
        return [
            remote(strip(emine, lo, hi), strip(zgot.at[0], lo, hi), zsem_s, zsem_r.at[e], win=after_w, step=me),
            remote(strip(esend, lo, hi), strip(zgot.at[1], lo, hi), zsem_s, zsem_r.at[e], win=after_w, step=partner),
        ]

    def finish(e):
        lo, hi = final[e]
        last = (length - 1, length - 1)
        start, rows = own_of(lo, hi), hi - lo
        esend[pl.ds(start, rows)] = part(last, start, rows, pl.multiple_of(TILE * (1 - core), TILE), TILE)
        emine[pl.ds(start, rows)] = part(last, start, rows, pl.multiple_of(TILE * core, TILE), TILE)

        @pl.when(w < windows - 1)
        def _():
            for copy in onward(e):
                copy.start()

        swap(e).start()

    def landing(f_x, f_y, f_c, t_x, t_y, lo, hi):
        rows = pl.ds(f_x * bs + own_of(lo, hi, f_x) - xlo(t_x), hi - lo)
        depth = pl.ds(pl.multiple_of(f_y * bsy + TILE * f_c - ylo(t_y), TILE), TILE)
        return corr.at[rows, depth, :]

    def edge(e):
        lo, hi = final[e]
        return max(lo, bs - reach), hi

    def spread(e):
        lo, hi = final[e]

        def one(where, to_core, lo, hi, send, recv):
            tx, ty = beside(*where)
            remote(
                strip(csend, lo, hi), landing(bx, by, core, tx, ty, lo, hi),
                send, recv, step=chip(tx, ty) * 2 + to_core,
            ).start()

        lo2, hi2 = edge(e)
        if hi2 > lo2:

            @pl.when(near)
            def _():
                for c in range(2):
                    one((1, 1), c, lo2, hi2, csem_s.at[2], bsem_r.at[e])

            for c in range(2):
                one((1, 0), c, lo2, hi2, csem_s.at[0], bsem_r.at[e])

        @pl.when(near)
        def _():
            for c in range(2):
                one((0, 1), c, lo, hi, csem_s.at[1], csem_r.at[e])

        one((0, 0), 1 - core, lo, hi, csem_s.at[0], csem_r.at[e])

    def spread_done():
        taken(srcv.at[pl.ds(0, bs + 2 * reach), pl.ds(0, TILE), :], csem_s.at[0]).wait_send()

        @pl.when(near)
        def _():
            taken(srcv.at[pl.ds(0, 2 * bs), pl.ds(0, TILE), :], csem_s.at[1]).wait_send()
            taken(srcv.at[pl.ds(0, 2 * reach), pl.ds(0, TILE), :], csem_s.at[2]).wait_send()

    def gather(e, kind):
        lo, hi = final[e]
        if kind == "own":
            taken(corr.at[pl.ds(0, hi - lo), pl.ds(0, 2 * TILE), :], csem_r.at[e]).wait_recv()
        else:
            lo, hi = edge(e)
            taken(corr.at[pl.ds(0, hi - lo)], bsem_r.at[e]).wait_recv()

    def change(e):
        lo, hi = final[e]
        swap(e).wait_recv()

        @pl.when(w > 0)
        def _():
            taken(zgot.at[:, pl.ds(0, hi - lo)], zsem_r.at[e]).wait_recv()

        mine = pl.ds(own_of(lo, hi), hi - lo)
        value = (zgot[0, mine] + zgot[1, mine]) - alpha_corner * (emine[mine] + egot[mine])
        csend[mine] = value
        corr[pl.ds(ox + own_of(lo, hi), hi - lo), pl.ds(pl.multiple_of(oy + TILE * core, TILE), TILE), :] = value
        spread(e)

    def second_weight(p, weight):
        return weight[2] + (pick(1.0, 0.0) * weight[1] if p == 0 else 0.0)

    def correct(start, rows):
        for n in range(rows):
            i = start + n
            x = corr[i] * (1.0 / coupling)
            for p in range(pairs):
                weight = weights(p, i)
                spot = pl.ds(TILE, ey)
                ref = levels[0][p]
                ref[0, i + 1, spot] = ref[0, i + 1, spot] + weight[0] * x
                ref[1, i + 1, spot] = ref[1, i + 1, spot] + second_weight(p, weight) * x

    def trade(i, o):
        lo, hi = leave[o]
        mine = pl.ds(own_of(lo, hi), hi - lo)
        return remote(xsend.at[i, mine], xgot.at[i, mine], xsem_s, xsem_r.at[o], step=partner)

    def emit(o):
        lo, hi = leave[o]
        start, rows = own_of(lo, hi), hi - lo
        for i in range(kept):
            xsend[i, pl.ds(start, rows)] = part((2 * i + 1, 2 * i), start, rows, 0, bsy)
            trade(i, o).start()
        for i in range(kept):
            obuf[i, pl.ds(start, rows)] = part((2 * i, 2 * i + 1), start, rows, 0, bsy)

    def place(b_x, b_y, lo, hi):
        rows = pl.ds(b_x * bs + own_of(lo, hi, b_x), hi - lo)
        return out.at[rows, pl.ds(pl.multiple_of(b_y * bsy, TILE), bsy), :]

    def settle(o):
        lo, hi = leave[o]
        mine = pl.ds(own_of(lo, hi), hi - lo)
        ratio = gamma ** (-half)
        taken(xgot.at[:, pl.ds(0, hi - lo)], xsem_r.at[o]).wait_recv()
        for i in range(kept):
            ours, theirs = obuf[i, mine], xgot[i, mine]
            obuf[i, mine] = ours + theirs
            obuf[i + kept, mine] = pick(ratio, -ratio) * (ours - theirs)
        for where in others:
            k = chip(*beside(*where))
            remote(
                strip(obuf.at[k], lo, hi), place(bx, by, lo, hi), osem.at[0], osem.at[1], step=2 * k + core
            ).start()
        pltpu.make_async_copy(strip(obuf.at[m], lo, hi), place(bx, by, lo, hi), hsem).start()

    def receive(c):
        lo, hi = arrive[c]
        taken(raw.at[0, pl.ds(0, len(others)), pl.ds(0, hi - lo)], isem.at[c]).wait_recv()
        block = raw.at[core, :, pl.ds(rows_of(lo, hi), hi - lo)]
        remote(block, block, fsem, dsem.at[c], step=partner).start()

    def advance(c):
        a, b = arrive[c]
        taken(raw.at[0, :, pl.ds(0, b - a)], dsem.at[c]).wait_recv()
        grouped(rows_of(a, b), b - a, spectrum, 3)
        sweeps(a, b)

    waiting = []

    def again(g):
        a, b, needs = second[g]
        for kind, e in needs:
            gather(e, kind)
        if waiting and ("own", ends - 2) in needs:
            settle(waiting.pop())
        grouped(rows_of(a, b), b - a, correct, 5)
        sweeps(a, b)
        if g in after:
            emit(after[g])
            if waiting:
                settle(waiting.pop())
            waiting.append(after[g])

    chunks, ends = len(arrive), len(final)

    def step(c):
        advance(c)
        e = c - (chunks - ends)
        if e >= 0:
            finish(e)
            if 1 <= e < ends - 1:
                change(e - 1)

    loads[2].wait()
    loads[3].wait()
    for c in range(chunks):
        receive(c)
        if c:
            step(c - 1)
    step(chunks - 1)
    late = [ends - 2, ends - 1]
    for g in range(len(second)):
        while any(kind == "own" and e in late for kind, e in second[g][2]):
            change(late.pop(0))
        again(g)
        if late:
            change(late.pop(0))
    settle(waiting.pop())

    taken(raw.at[0, pl.ds(0, len(others))], asem).wait_send()
    taken(raw.at[0], fsem).wait_send()
    taken(esend, esem_s).wait_send()
    spread_done()

    @pl.when(w < windows - 1)
    def _():
        taken(zgot, zsem_s).wait_send()

    taken(xsend, xsem_s).wait_send()
    taken(obuf.at[pl.ds(0, len(others))], osem.at[0]).wait_send()
    taken(obuf.at[pl.ds(0, len(others))], osem.at[1]).wait_recv()
    pltpu.make_async_copy(obuf.at[0], obuf.at[0], hsem).wait()


def waves(initial_state, source, absorption):
    length = lax.axis_size("step")
    windows = lax.axis_size("win")
    nx, ny, nz = initial_state.shape
    half = length // 2
    reach = SWEEPS - 1
    bs, bsy = nx // 2, ny // 2
    ext = bs + reach
    ey = bsy + TILE
    units = length // 2
    plan = spans(ext, bs, reach)
    arrive, final, _, leave, _ = (len(group) for group in plan)
    f32 = jnp.float32
    dma = pltpu.SemaphoreType.DMA
    edge = pltpu.VMEM((bs, TILE, nz), f32)
    return pl.pallas_call(
        functools.partial(wave_kernel, length, windows, nx, ny, ext, ey, plan),
        out_shape=jax.ShapeDtypeStruct((nx, ny, nz), f32),
        in_specs=[pl.BlockSpec(memory_space=pltpu.HBM)] * 3,
        out_specs=pl.BlockSpec(memory_space=pl.ANY),
        scratch_shapes=[
            pltpu.VMEM((nx, ny, nz), f32),
            pltpu.VMEM((2, half, ext, ey, nz), f32),
            pltpu.VMEM((ext, ey, nz), f32),
            pltpu.VMEM((ext, ey, nz), f32),
            pltpu.VMEM((3 * length // 4, ext, ey, nz), f32),
            [[pltpu.VMEM((2, ext + 2, ey + 2 * TILE, nz), f32)] * (units // 2)] * reach,
            [pltpu.VMEM((2, bs, bsy, nz), f32)] * (units // 2),
            pltpu.VMEM((ext, ey, nz), f32),
            edge, edge, edge,
            pltpu.VMEM((2, bs, TILE, nz), f32),
            edge,
            pltpu.VMEM((half // 2, bs, bsy, nz), f32),
            pltpu.VMEM((half // 2, bs, bsy, nz), f32),
            pltpu.VMEM((half, bs, bsy, nz), f32),
            dma((4,)),
            dma,
            dma((arrive,)),
            dma,
            dma((arrive,)),
            dma,
            dma((final,)),
            dma,
            dma((final,)),
            dma((3,)),
            dma((final,)),
            dma((final,)),
            dma,
            dma((leave,)),
            dma((2,)),
            dma,
        ],
        compiler_params=pltpu.CompilerParams(
            collective_id=0, has_side_effects=True, vmem_limit_bytes=40 * 1024 * 1024
        ),
    )(*(pltpu.with_memory_space_constraint(x, pltpu.HBM) for x in (source[0, 0], initial_state, absorption)))[None, None]


def fits(mesh, shape):
    length = mesh.shape["step"]
    if length % 8 or shape[2] != LANES or shape[1] != 4 * TILE:
        return False
    gx = length // 4
    return shape[0] % gx == 0 and shape[0] // gx >= SWEEPS - 1


def pairs_up(mesh, shape):
    return mesh.shape["step"] == 8 and shape[0] // 2 >= 2 * SWEEPS


def solution(mesh):
    def body(initial_state, source, absorption):
        plan = per_device
        if fits(mesh, initial_state.shape):
            plan = waves if pairs_up(mesh, initial_state.shape) else blocks
        return plan(initial_state, source, absorption)

    return jax.shard_map(
        body,
        mesh=mesh,
        in_specs=(P(), P("win", "step", None, None, None), P()),
        out_specs=P("win", "step", None, None, None),
        check_vma=False,
    )
```

```python
import functools
import math

import jax
import jax.numpy as jnp
from jax import lax
from jax.experimental import pallas as pl
from jax.experimental.pallas import tpu as pltpu
from jax.sharding import PartitionSpec as P

ITERS = 2
SWEEPS = 8


alpha_corner = 0.1
coupling = 0.05


def from_behind(block, axis, distance):
    devices = range(lax.axis_size(axis))
    route = [(i - distance, i) for i in devices if i - distance in devices]
    return lax.ppermute(block, axis, route)


def pad_cube(field):
    widths = [(0, 0)] * (field.ndim - 3) + [(1, 1)] * 3
    return jnp.pad(field, widths)


def neighbours(field):
    padded = pad_cube(field)
    total = padded[..., 2:, 1:-1, 1:-1] + padded[..., :-2, 1:-1, 1:-1]
    total = total + padded[..., 1:-1, 2:, 1:-1] + padded[..., 1:-1, :-2, 1:-1]
    total = total + padded[..., 1:-1, 1:-1, 2:] + padded[..., 1:-1, 1:-1, :-2]
    return total


def complex_times(first, second):
    return jnp.stack(
        [first[0] * second[0] - first[1] * second[1], first[0] * second[1] + first[1] * second[0]]
    )


def relax(spectrum, inverse):
    field = complex_times(inverse, spectrum)
    for repeat in range(SWEEPS - 1):
        field = complex_times(inverse, spectrum + coupling * neighbours(field))
    return field


def inverse_diagonal(angle, absorption, gamma):
    real_part = 1.0 - gamma * jnp.cos(angle) + absorption + 6.0 * coupling
    imag_part = jnp.broadcast_to(gamma * jnp.sin(angle), real_part.shape)
    magnitude = real_part * real_part + imag_part * imag_part
    return jnp.stack([real_part / magnitude, -imag_part / magnitude])


def dft_tables(window_len):
    index = jnp.arange(window_len, dtype=jnp.int32)
    product = index[:, None] * index[None, :] % window_len
    angle = product.astype(jnp.float32) * (2.0 * math.pi / window_len)
    return (jnp.cos(angle), jnp.sin(angle))


def transform_exchange(scaled, window_len):
    pencil = lax.all_to_all(scaled[None], "step", split_axis=1, concat_axis=0, tiled=True)
    cosine, sine = dft_tables(window_len)
    flat = pencil.reshape(window_len, -1)
    real_part = jnp.dot(cosine, flat, precision=lax.Precision.HIGHEST)
    imag_part = -jnp.dot(sine, flat, precision=lax.Precision.HIGHEST)
    shaped = pencil.shape
    spectrum = (
        lax.all_to_all(real_part.reshape(shaped), "step", split_axis=0, concat_axis=1, tiled=True),
        lax.all_to_all(imag_part.reshape(shaped), "step", split_axis=0, concat_axis=1, tiled=True),
    )
    return jnp.stack([spectrum[0][0], spectrum[1][0]])


def untransform_exchange(field, window_len):
    pencil = (
        lax.all_to_all(field[0][None], "step", split_axis=1, concat_axis=0, tiled=True),
        lax.all_to_all(field[1][None], "step", split_axis=1, concat_axis=0, tiled=True),
    )
    cosine, sine = dft_tables(window_len)
    shaped = pencil[0].shape
    values = jnp.dot(cosine, pencil[0].reshape(window_len, -1), precision=lax.Precision.HIGHEST)
    values = values - jnp.dot(
        sine, pencil[1].reshape(window_len, -1), precision=lax.Precision.HIGHEST
    )
    values = values / window_len
    result = lax.all_to_all(values.reshape(shaped), "step", split_axis=0, concat_axis=1, tiled=True)
    return result[0]


def per_device(initial_state, source, absorption):
    window_len = lax.axis_size("step")
    moment = lax.axis_index("step")
    window_index = lax.axis_index("win")
    gamma = alpha_corner ** (1.0 / window_len)
    scale = gamma ** moment.astype(jnp.float32)
    forcing_base = source[0, 0]
    is_first = moment == 0
    state = jnp.zeros_like(forcing_base)
    angle = moment.astype(jnp.float32) * (2.0 * math.pi / window_len)
    inverse = inverse_diagonal(angle, absorption, gamma)
    for repeat in range(ITERS):
        if repeat == 0:
            correction = jnp.where(window_index == 0, initial_state, 0.0)
        else:
            ends = from_behind(state, "step", 1 - window_len)
            before = from_behind(ends, "win", 1)
            before = jnp.where(window_index == 0, initial_state, before)
            correction = before - alpha_corner * ends
        forcing = forcing_base + jnp.where(is_first, correction, 0.0)
        scaled = forcing * scale
        spectrum = transform_exchange(scaled, window_len)
        field = relax(spectrum, inverse)
        values = untransform_exchange(field, window_len)
        state = values / scale
    return state[None, None]


LANES = 128
TILE = 8
GROUP = 8


def tables(length):
    gamma = alpha_corner ** (1.0 / length)
    into, back, angles = [], [], []
    for core in range(2):
        rows_in, rows_back = [], []
        for time in range(length):
            scale = gamma**time
            row_in, row_back = [], []
            for p in range(length // 4):
                j = 2 * p + core
                if j == 0:
                    pair, weight = (1.0, (-1.0) ** time), 1.0 / length
                else:
                    turn = 2.0 * math.pi * (j * time % length) / length
                    pair, weight = (math.cos(turn), -math.sin(turn)), 2.0 / length
                row_in += [value * scale / coupling for value in pair]
                row_back += [value * weight / scale for value in pair]
            rows_in.append(row_in)
            rows_back.append(row_back)
        into.append(rows_in)
        back.append(rows_back)
        angles.append([2.0 * math.pi * (2 * p + core) / length for p in range(length // 4)])
    return into, back, angles


def kernel(
    length, windows, nx, ny, ext, ey,
    source, initial, absorb, out,
    raw, first, absv, coef, base, again, fa, fb, corr,
    psend, pgot, ends, zgot, csend, qsend, qgot, obuf,
    lsem, asend, brecv, fsend, esem, zsem, csem_s, csem_r, qsem_s, qsem_r, osem_s, osem_r,
):
    half = length // 2
    gx, gy = half // 2, 2
    bs, bsy = nx // gx, ny // gy
    reach = SWEEPS - 1
    pairs = length // 4
    units = 2 * pairs
    gamma = alpha_corner ** (1.0 / length)
    into, back, angles = tables(length)
    me = lax.axis_index("step")
    w = lax.axis_index("win")
    core, m = me % 2, me // 2
    partner = m * 2 + (1 - core)
    bx, by = m % gx, m // gx

    def xlo(b):
        if gx == 2:
            return b * (nx - ext)
        return jnp.minimum(jnp.maximum(b * bs - reach, 0), nx - ext)

    def ylo(b):
        return pl.multiple_of(b * (ny - ey), TILE)

    def pick(a, b):
        return jnp.where(core == 0, jnp.float32(a), jnp.float32(b))

    def region(ref, b_x, b_y):
        return ref.at[pl.ds(xlo(b_x), ext), pl.ds(ylo(b_y), ey), :]

    ox = bx * bs - xlo(bx)
    oy = pl.multiple_of(by * bsy - ylo(by), TILE)

    loads = [
        pltpu.make_async_copy(region(absorb, bx, by), absv, lsem.at[0]),
        pltpu.make_async_copy(region(source, bx, by), raw.at[me], lsem.at[1]),
        pltpu.make_async_copy(region(initial, bx, by), first, lsem.at[2]),
    ]
    for load in loads:
        load.start()
    zero_row = jnp.zeros((ey, LANES), jnp.float32)
    for u in range(units):
        for ref in (fa, fb):
            ref[u, 0, pl.ds(TILE, ey)] = zero_row
            ref[u, ext + 1, pl.ds(TILE, ey)] = zero_row
            for r in range(1, ext + 1):
                ref[u, r, pl.ds(0, TILE)] = zero_row[:TILE]
                ref[u, r, pl.ds(TILE + ey, TILE)] = zero_row[:TILE]
    if gx > 2:
        corr[...] = jnp.zeros_like(corr)

    barrier = pltpu.get_barrier_semaphore()
    for d in range(1, length):
        pl.semaphore_signal(
            barrier, inc=1, device_id={"step": (me + d) % length}, device_id_type=pl.DeviceIdType.MESH
        )

    @pl.when(w > 0)
    def _():
        pl.semaphore_signal(barrier, inc=1, device_id={"win": w - 1}, device_id_type=pl.DeviceIdType.MESH)

    @pl.when(w < windows - 1)
    def _():
        pl.semaphore_signal(barrier, inc=1, device_id={"win": w + 1}, device_id_type=pl.DeviceIdType.MESH)

    nearby = jnp.where(w > 0, 1, 0) + jnp.where(w < windows - 1, 1, 0)
    pl.semaphore_wait(barrier, length - 1 + nearby)

    def remote(src, dst, send, recv, **where):
        return pltpu.make_async_remote_copy(
            src_ref=src, dst_ref=dst, send_sem=send, recv_sem=recv,
            device_id=where, device_id_type=pl.DeviceIdType.MESH,
        )

    outgoing = []
    for d in range(1, half):
        to = (m + d) % half
        copy = remote(
            region(source, to % gx, to // gx), raw.at[me], asend.at[d], brecv.at[me], step=to * 2 + core
        )
        copy.start()
        outgoing.append(copy)
    copy = remote(region(source, bx, by), raw.at[me], asend.at[0], brecv.at[me], step=partner)
    copy.start()
    outgoing.append(copy)

    def grouped(begin, count, work, most=GROUP):
        size = -(-count // max(1, count // most))

        def body(g, carry):
            work(begin + g * size, size)
            return carry

        lax.fori_loop(0, count // size, body, 0)
        if count % size:
            work(begin + count - size, size)

    def each(one):
        def work(start, rows):
            for n in range(rows):
                one(start + n)

        return work

    loads[0].wait()

    def coefficients(i):
        for p in range(pairs):
            rows = absv[i]
            cosine = pick(math.cos(angles[0][p]), math.cos(angles[1][p]))
            imag = pick(gamma * math.sin(angles[0][p]), gamma * math.sin(angles[1][p]))
            real = 1.0 - gamma * cosine + rows + 6.0 * coupling
            over = coupling / (real * real + imag * imag)
            coef[3 * p, i] = real * over
            coef[3 * p + 1, i] = -imag * over
            if p == 0:
                other = pick(-1.0, math.cos(angles[1][p]))
                real = 1.0 - gamma * other + rows + 6.0 * coupling
                over = coupling / (real * real + imag * imag)
                coef[3 * p + 2, i] = real * over

    grouped(0, ext, each(coefficients))

    def weights(p, i):
        straight = coef[3 * p, i]
        return straight, (coef[3 * p + 2, i] if p == 0 else straight), coef[3 * p + 1, i]

    def arrival(t):
        return remote(raw.at[t], raw.at[t], asend.at[0], brecv.at[t], step=partner)

    for d in range(1, half):
        t = ((m + half - d) % half) * 2 + core
        arrival(t).wait_recv()
        copy = remote(raw.at[t], raw.at[t], fsend.at[d], brecv.at[t], step=partner)
        copy.start()
        outgoing.append(copy)
    for d in range(half):
        arrival(((m + half - d) % half) * 2 + (1 - core)).wait_recv()
    loads[1].wait()
    loads[2].wait()
    is_first = jnp.where(w == 0, jnp.float32(1.0 / coupling), jnp.float32(0.0))

    def second_weight(p, weight):
        return weight[2] + (pick(1.0, 0.0) * weight[1] if p == 0 else 0.0)

    def transform(i):
        begin = first[i] * is_first
        fields = [raw[t, i] for t in range(length)]
        for p in range(pairs):
            weight = weights(p, i)
            s0, s1 = begin, begin * pick(1.0, 0.0) if p == 0 else None
            for t in range(length):
                s0 = s0 + pick(into[0][t][2 * p], into[1][t][2 * p]) * fields[t]
                term = pick(into[0][t][2 * p + 1], into[1][t][2 * p + 1]) * fields[t]
                s1 = term if s1 is None else s1 + term
            b0 = weight[0] * s0 - weight[2] * s1
            b1 = weight[1] * s1 + weight[2] * s0
            base[2 * p, i] = b0
            base[2 * p + 1, i] = b1
            fa[2 * p, i + 1, pl.ds(TILE, ey)] = b0
            fa[2 * p + 1, i + 1, pl.ds(TILE, ey)] = b1

    grouped(0, ext, each(transform), GROUP // 2)

    lane = lax.broadcasted_iota(jnp.int32, (ey, LANES), 1)

    def around(ref, u, r):
        v = ref[u, r, pl.ds(TILE, ey)]
        total = jnp.where(lane == 0, 0.0, pltpu.roll(v, 1, 1))
        total = total + jnp.where(lane == LANES - 1, 0.0, pltpu.roll(v, LANES - 1, 1))
        beside = ref[u, r - 1, pl.ds(TILE, ey)] + ref[u, r + 1, pl.ds(TILE, ey)]
        return total + (beside + (ref[u, r, pl.ds(TILE - 1, ey)] + ref[u, r, pl.ds(TILE + 1, ey)]))

    def sweep_rows(base, here, there, start, rows):
        for n in range(rows):
            i = start + n
            for p in range(pairs):
                weight = weights(p, i)
                n0 = around(here, 2 * p, i + 1)
                n1 = around(here, 2 * p + 1, i + 1)
                there[2 * p, i + 1, pl.ds(TILE, ey)] = base[2 * p, i] + (weight[0] * n0 - weight[2] * n1)
                there[2 * p + 1, i + 1, pl.ds(TILE, ey)] = base[2 * p + 1, i] + (
                    weight[1] * n1 + weight[2] * n0
                )

    def sweeps(base):
        here, there = fa, fb
        for k in range(1, SWEEPS):
            begin, count = (bx * k, ext - k) if gx == 2 else (0, ext)
            grouped(begin, count, functools.partial(sweep_rows, base, here, there))
            here, there = there, here
        return here

    final = sweeps(base)

    def part(t, y0, rows):
        total = None
        for u in range(units):
            factor = pick(back[0][t[0]][u], back[1][t[1]][u])
            term = factor * final[u, pl.ds(ox + 1, bs), pl.ds(y0 + TILE, rows), :]
            total = term if total is None else total + term
        return total

    last = (length - 1, length - 1)
    psend[...] = part(last, pl.multiple_of(oy + TILE * (1 - core), TILE), TILE)
    swap = remote(psend, pgot, esem.at[0], esem.at[1], step=partner)
    swap.start()
    mine = part(last, pl.multiple_of(oy + TILE * core, TILE), TILE)
    swap.wait_recv()
    mine = mine + pgot[...]
    ends[...] = mine
    outgoing.append(swap)

    onward = remote(ends, zgot, zsem.at[0], zsem.at[1], win=(w + 1) % windows)

    @pl.when(w < windows - 1)
    def _():
        onward.start()

    @pl.when(w == 0)
    def _():
        zgot[...] = jnp.zeros_like(zgot)

    @pl.when(w > 0)
    def _():
        onward.wait_recv()

    change = zgot[...] - alpha_corner * ends[...]
    csend[...] = change
    corr[pl.ds(ox, bs), pl.ds(pl.multiple_of(oy + TILE * core, TILE), TILE), :] = change

    def spread(ex, ey_, send):
        rows, skip = (bs, 0) if ex == 0 else (reach, bs - reach if ex == 1 else 0)
        tx, ty = (bx + ex, by + ey_) if send else (bx, by)
        fx, fy = (bx, by) if send else (bx - ex, by - ey_)
        ax, ay = (tx, ty) if send else (fx, fy)
        inside = (ax >= 0) & (ax < gx) & (ay >= 0) & (ay < gy)
        slot = ((ex + 1) * 3 + (ey_ + 1)) * 2
        for c in range(2):
            near = c == (1 if ey_ == 1 else 0)
            if send:
                okay = inside if ey_ == 0 else inside & (core == (1 if ey_ == 1 else 0))
                if ex == 0 and ey_ == 0:
                    okay = core != c
                fc, tc = core, c
            else:
                if ey_ != 0 and not near:
                    continue
                okay = inside
                if ex == 0 and ey_ == 0:
                    okay = core != c
                fc, tc = c, core

            @pl.when(okay)
            def _(c=c, fc=fc, tc=tc):
                copy = remote(
                    csend.at[pl.ds(skip, rows)],
                    corr.at[
                        pl.ds(fx * bs + skip - xlo(tx), rows),
                        pl.ds(pl.multiple_of(fy * bsy + TILE * fc - ylo(ty), TILE), TILE),
                        :,
                    ],
                    csem_s.at[slot + c],
                    csem_r.at[slot + fc],
                    step=(ty * gx + tx) * 2 + tc if send == 1 else partner,
                )
                if send == 1:
                    copy.start()
                elif send == 2:
                    copy.wait_send()
                else:
                    copy.wait_recv()

    offsets = [(ex, e) for ex in (-1, 0, 1) for e in (-1, 0, 1)]
    for ex, e in offsets:
        spread(ex, e, 1)
    for ex, e in offsets:
        spread(ex, e, 0)

    def correct(i):
        x = corr[i] * (1.0 / coupling)
        for p in range(pairs):
            weight = weights(p, i)
            b0 = base[2 * p, i] + weight[0] * x
            b1 = base[2 * p + 1, i] + second_weight(p, weight) * x
            again[2 * p, i] = b0
            again[2 * p + 1, i] = b1
            fa[2 * p, i + 1, pl.ds(TILE, ey)] = b0
            fa[2 * p + 1, i + 1, pl.ds(TILE, ey)] = b1

    grouped(0, ext, each(correct))
    final = sweeps(again)

    for k in range(half):
        qsend[k] = part((2 * k + 1, 2 * k), oy, bsy)
        copy = remote(qsend.at[k], qgot.at[k], qsem_s.at[k], qsem_r.at[k], step=partner)
        copy.start()
        outgoing.append(copy)
    for k in range(half):
        obuf[k] = part((2 * k, 2 * k + 1), oy, bsy)

    def place(b_x, b_y):
        return out.at[pl.ds(b_x * bs, bs), pl.ds(pl.multiple_of(b_y * bsy, TILE), bsy), :]

    for k in range(half):
        remote(qsend.at[k], qgot.at[k], qsem_s.at[k], qsem_r.at[k], step=partner).wait_recv()
        obuf[k] = obuf[k] + qgot[k]

        @pl.when(m == k)
        def _(k=k):
            pltpu.make_async_copy(obuf.at[k], place(bx, by), lsem.at[3]).start()

        @pl.when(m != k)
        def _(k=k):
            remote(obuf.at[k], place(bx, by), osem_s.at[k], osem_r.at[m], step=2 * k + core).start()

    for copy in outgoing:
        copy.wait_send()
    for ex, e in offsets:
        spread(ex, e, 2)

    @pl.when(w < windows - 1)
    def _():
        onward.wait_send()

    for k in range(half):

        @pl.when(m == k)
        def _(k=k):
            pltpu.make_async_copy(obuf.at[k], place(bx, by), lsem.at[3]).wait()

        @pl.when(m != k)
        def _(k=k):
            done = remote(obuf.at[k], place(k % gx, k // gx), osem_s.at[k], osem_r.at[k], step=partner)
            done.wait_send()
            done.wait_recv()


def blocks(initial_state, source, absorption):
    length = lax.axis_size("step")
    windows = lax.axis_size("win")
    nx, ny, nz = initial_state.shape
    half = length // 2
    gx, reach = half // 2, SWEEPS - 1
    bs, bsy = nx // gx, ny // 2
    ext = min(nx, bs + reach * (1 if gx == 2 else 2))
    ey = bsy + -(-reach // TILE) * TILE
    units = length // 2
    f32 = jnp.float32
    dma = pltpu.SemaphoreType.DMA
    return pl.pallas_call(
        functools.partial(kernel, length, windows, nx, ny, ext, ey),
        out_shape=jax.ShapeDtypeStruct((nx, ny, nz), f32),
        in_specs=[pl.BlockSpec(memory_space=pl.ANY)] * 3,
        out_specs=pl.BlockSpec(memory_space=pl.ANY),
        scratch_shapes=[
            pltpu.VMEM((length, ext, ey, nz), f32),
            pltpu.VMEM((ext, ey, nz), f32),
            pltpu.VMEM((ext, ey, nz), f32),
            pltpu.VMEM((3 * length // 4, ext, ey, nz), f32),
            pltpu.VMEM((units, ext, ey, nz), f32),
            pltpu.VMEM((units, ext, ey, nz), f32),
            pltpu.VMEM((units, ext + 2, ey + 2 * TILE, nz), f32),
            pltpu.VMEM((units, ext + 2, ey + 2 * TILE, nz), f32),
            pltpu.VMEM((ext, ey, nz), f32),
            pltpu.VMEM((bs, TILE, nz), f32),
            pltpu.VMEM((bs, TILE, nz), f32),
            pltpu.VMEM((bs, TILE, nz), f32),
            pltpu.VMEM((bs, TILE, nz), f32),
            pltpu.VMEM((bs, TILE, nz), f32),
            pltpu.VMEM((half, bs, bsy, nz), f32),
            pltpu.VMEM((half, bs, bsy, nz), f32),
            pltpu.VMEM((half, bs, bsy, nz), f32),
            dma((4,)),
            dma((half,)),
            dma((length,)),
            dma((half,)),
            dma((2,)),
            dma((2,)),
            dma((18,)),
            dma((18,)),
            dma((half,)),
            dma((half,)),
            dma((half,)),
            dma((half,)),
        ],
        compiler_params=pltpu.CompilerParams(
            collective_id=0, has_side_effects=True, vmem_limit_bytes=28 * 1024 * 1024
        ),
    )(source[0, 0], initial_state, absorption)[None, None]


ARRIVE = (8, 4, 3, 3, 3)
SECOND = (5, 3, 3, 3, 3, 3)
LEAST = 3


def cuts(sizes, extent):
    bounds = [0]
    for size in sizes:
        if bounds[-1] + size < extent:
            bounds.append(bounds[-1] + size)
    bounds.append(extent)
    return list(zip(bounds[:-1], bounds[1:]))


def spans(ext, bs, reach):
    arrive = cuts(ARRIVE, ext)
    final = [(max(0, a - reach), b - reach) for a, b in arrive if b > reach]
    sources = [(a, b, "own", e) for e, (a, b) in enumerate(final)]
    for e, (a, b) in enumerate(final):
        if b > bs - reach:
            sources.append((2 * bs - b, 2 * bs - max(a, bs - reach), "beyond", e))
    second, leave, after, sent = [], [], {}, 0
    groups = cuts(SECOND, ext)
    for g, (a, b) in enumerate(groups):
        needs = [(kind, e) for lo, hi, kind, e in sources if a <= lo < b or (lo < a and g == 0)]
        second.append((a, b, needs))
        if b - reach - sent >= LEAST or g == len(groups) - 1:
            after[g] = len(leave)
            leave.append((sent, b - reach))
            sent = b - reach
    return arrive, final, second, leave, after


def wave_kernel(
    length, windows, nx, ny, ext, ey, plan,
    source, initial, absorb, out,
    srcv, raw, first, absv, coef, levels, fin, corr,
    emine, esend, egot, zgot, csend, xsend, xgot, obuf,
    lsem, asem, isem, fsem, dsem, esem_s, esem_r, zsem_s, zsem_r, csem_s, csem_r, bsem_r, xsem_s, xsem_r, osem, hsem,
):
    arrive, final, second, leave, after = plan
    half = length // 2
    bs, bsy = nx // 2, ny // 2
    reach = SWEEPS - 1
    pairs = length // 4
    units = 2 * pairs
    kept = half // 2
    gamma = alpha_corner ** (1.0 / length)
    into, back, angles = tables(length)
    me = lax.axis_index("step")
    w = lax.axis_index("win")
    core, m = me % 2, me // 2
    partner = m * 2 + (1 - core)
    bx, by = m % 2, m // 2
    near = core == 1 - by

    def chip(b_x, b_y):
        return b_y * 2 + b_x

    def xlo(b):
        return b * (nx - ext)

    def ylo(b):
        return pl.multiple_of(b * (ny - ey), TILE)

    def rows_of(lo, hi, b=bx):
        return lo + b * (ext - lo - hi)

    def own_of(lo, hi, b=bx):
        return lo + b * (bs - lo - hi)

    def held(i):
        return i + bx * (ext - 1 - 2 * i)

    def own(i):
        return i + bx * (bs - 1 - 2 * i)

    def pick(a, b):
        if a == b:
            return jnp.float32(a)
        return jnp.where(core == 0, jnp.float32(a), jnp.float32(b))

    def region(ref, b_x, b_y, lo, hi):
        rows = pl.ds(xlo(b_x) + rows_of(lo, hi, b_x), hi - lo)
        return ref.at[rows, pl.ds(ylo(b_y), ey), :]

    ox = bx * bs - xlo(bx)
    oy = pl.multiple_of(by * bsy - ylo(by), TILE)

    loads = [
        pltpu.make_async_copy(source, srcv, lsem.at[0]),
        pltpu.make_async_copy(region(absorb, bx, by, 0, ext), absv, lsem.at[1]),
        pltpu.make_async_copy(region(source, bx, by, 0, ext), raw.at[core, m], lsem.at[2]),
        pltpu.make_async_copy(region(initial, bx, by, 0, ext), first, lsem.at[3]),
    ]
    for load in loads:
        load.start()

    barrier = pltpu.get_barrier_semaphore()

    def greet(**where):
        pl.semaphore_signal(barrier, inc=1, device_id=where, device_id_type=pl.DeviceIdType.MESH)

    for d in range(1, length):
        greet(step=(me + d) % length)

    @pl.when(w > 0)
    def _():
        greet(win=w - 1, step=me)
        greet(win=w - 1, step=partner)

    @pl.when(w < windows - 1)
    def _():
        greet(win=w + 1, step=me)
        greet(win=w + 1, step=partner)

    @pl.when(w == 0)
    def _():
        zgot[...] = jnp.zeros_like(zgot)

    nearby = jnp.where(w > 0, 2, 0) + jnp.where(w < windows - 1, 2, 0)
    loads[0].wait()
    pl.semaphore_wait(barrier, length - 1 + nearby)

    def remote(src, dst, send, recv, **where):
        return pltpu.make_async_remote_copy(
            src_ref=src, dst_ref=dst, send_sem=send, recv_sem=recv,
            device_id=where, device_id_type=pl.DeviceIdType.MESH,
        )

    def taken(block, sem):
        return remote(block, block, sem, sem, step=partner)

    others = [(1, 1), (1, 0), (0, 1)]

    def beside(ex, e_y):
        return (bx + ex) % 2, (by + e_y) % 2

    for c, (lo, hi) in enumerate(arrive):
        for where in others:
            tx, ty = beside(*where)
            remote(
                region(srcv, tx, ty, lo, hi),
                raw.at[core, m, pl.ds(rows_of(lo, hi, tx), hi - lo)],
                asem, isem.at[c], step=chip(tx, ty) * 2 + core,
            ).start()

    zero_row = jnp.zeros((ey, LANES), jnp.float32)

    def rim(r, carry):
        for refs in levels:
            for ref in refs:
                for q in range(2):
                    ref[q, r, pl.ds(0, TILE)] = zero_row[:TILE]
                    ref[q, r, pl.ds(TILE + ey, TILE)] = zero_row[:TILE]
        return carry

    for refs in levels:
        for ref in refs:
            for q in range(2):
                for r in (0, ext + 1):
                    ref[q, r, pl.ds(TILE, ey)] = zero_row
    lax.fori_loop(1, ext + 1, rim, 0)

    def grouped(begin, count, work, most):
        groups = -(-count // most)
        size = -(-count // groups)
        if groups == 1:
            work(begin, count)
            return

        def body(g, carry):
            work(begin + g * size, size)
            return carry

        lax.fori_loop(0, count // size, body, 0)
        if count % size:
            work(begin + count - count % size, count % size)

    loads[1].wait()

    def coefficients(start, rows):
        for n in range(rows):
            i = start + n
            for p in range(pairs):
                here = absv[held(i)]
                cosine = pick(math.cos(angles[0][p]), math.cos(angles[1][p]))
                imag = pick(gamma * math.sin(angles[0][p]), gamma * math.sin(angles[1][p]))
                real = 1.0 - gamma * cosine + here + 6.0 * coupling
                over = coupling / (real * real + imag * imag)
                coef[3 * p, i] = real * over
                coef[3 * p + 1, i] = -imag * over
                if p == 0:
                    other = pick(-1.0, math.cos(angles[1][p]))
                    real = 1.0 - gamma * other + here + 6.0 * coupling
                    over = coupling / (real * real + imag * imag)
                    coef[3 * p + 2, i] = real * over

    grouped(0, ext, coefficients, 4)

    def weights(p, i, y0=0, rows=ey):
        part = pl.ds(y0, rows)
        straight = coef[3 * p, i, part]
        return straight, (coef[3 * p + 2, i, part] if p == 0 else straight), coef[3 * p + 1, i, part]

    is_first = jnp.where(w == 0, jnp.float32(1.0 / coupling), jnp.float32(0.0))

    def combine(pair, values):
        total = None
        for (a, b), value in zip(pair, values):
            if a == 0 and b == 0:
                continue
            term = value if a == 1 and b == 1 else pick(a, b) * value
            total = term if total is None else total + term
        return total

    def spectrum(start, rows):
        for n in range(rows):
            i = start + n
            folded = []
            for t in range(half):
                early, late = gamma**t / coupling, gamma ** (t + half) / coupling
                now, then = raw[t % 2, t // 2, held(i)], raw[t % 2, (t + half) // 2, held(i)]
                folded.append(early * now + pick(late, -late) * then)
            folded[0] = folded[0] + first[held(i)] * is_first
            for p in range(pairs):
                weight = weights(p, i)
                turn = [
                    [
                        tuple(into[c][t][2 * p + q] * coupling / gamma**t for c in range(2))
                        for t in range(half)
                    ]
                    for q in range(2)
                ]
                turn = [[tuple(round(v, 15) for v in pair) for pair in row] for row in turn]
                s0 = combine(turn[0], folded)
                s1 = combine(turn[1], folded)
                levels[0][p][0, i + 1, pl.ds(TILE, ey)] = weight[0] * s0 - weight[2] * s1
                levels[0][p][1, i + 1, pl.ds(TILE, ey)] = weight[1] * s1 + weight[2] * s0

    def stencil(ref, q, start, rows, y0, depth):
        lane = lax.broadcasted_iota(jnp.int32, (depth, LANES), 1)
        at = pl.multiple_of(y0 + TILE, TILE)
        line = [ref[q, start + n, pl.ds(at, depth)] for n in range(rows + 2)]
        sums = []
        for n in range(1, rows + 1):
            v = line[n]
            around = ref.at[q, start + n, pl.ds(y0, depth + 2 * TILE), :]
            total = jnp.where(lane == 0, 0.0, pltpu.roll(v, 1, 1))
            total = total + jnp.where(lane == LANES - 1, 0.0, pltpu.roll(v, LANES - 1, 1))
            across = around[pl.ds(TILE - 1, depth)] + around[pl.ds(TILE + 1, depth)]
            sums.append(total + ((line[n - 1] + line[n + 1]) + across))
        return sums

    def sweep_rows(k, start, rows):
        last = k == reach
        y0, depth = (oy, bsy) if last else (0, ey)
        at = pl.multiple_of(y0 + TILE, TILE)
        for p in range(pairs):
            s0 = stencil(levels[k - 1][p], 0, start, rows, y0, depth)
            s1 = stencil(levels[k - 1][p], 1, start, rows, y0, depth)
            for n in range(rows):
                i = start + n
                weight = weights(p, i, y0, depth)
                b0 = levels[0][p][0, i + 1, pl.ds(at, depth)]
                b1 = levels[0][p][1, i + 1, pl.ds(at, depth)]
                v0 = b0 + (weight[0] * s0[n] - weight[2] * s1[n])
                v1 = b1 + (weight[1] * s1[n] + weight[2] * s0[n])
                if last:
                    fin[p][0, i] = v0
                    fin[p][1, i] = v1
                else:
                    levels[k][p][0, i + 1, pl.ds(TILE, ey)] = v0
                    levels[k][p][1, i + 1, pl.ds(TILE, ey)] = v1

    def sweeps(a, b):
        for k in range(1, SWEEPS):
            lo, hi = max(0, a - k), b - k
            if hi > lo:
                grouped(lo, hi - lo, functools.partial(sweep_rows, k), 6)

    def part(ref, t, lo, hi, y0, depth):
        factors = [pick(back[0][t[0]][u], back[1][t[1]][u]) for u in range(units)]
        for i in range(lo, hi):
            total = None
            for u, factor in enumerate(factors):
                term = factor * fin[u // 2][u % 2, i, pl.ds(y0, depth)]
                total = term if total is None else total + term
            ref[own(i)] = total

    def strip(ref, lo, hi):
        return ref.at[pl.ds(own_of(lo, hi), hi - lo)]

    def swap(e):
        lo, hi = final[e]
        return remote(strip(esend, lo, hi), strip(egot, lo, hi), esem_s, esem_r.at[e], step=partner)

    def onward(e):
        lo, hi = final[e]
        after_w = (w + 1) % windows
        return [
            remote(strip(emine, lo, hi), strip(zgot.at[0], lo, hi), zsem_s, zsem_r.at[e], win=after_w, step=me),
            remote(strip(esend, lo, hi), strip(zgot.at[1], lo, hi), zsem_s, zsem_r.at[e], win=after_w, step=partner),
        ]

    def finish(e):
        lo, hi = final[e]
        last = (length - 1, length - 1)
        part(esend, last, lo, hi, pl.multiple_of(TILE * (1 - core), TILE), TILE)
        part(emine, last, lo, hi, pl.multiple_of(TILE * core, TILE), TILE)

        @pl.when(w < windows - 1)
        def _():
            for copy in onward(e):
                copy.start()

        swap(e).start()

    def landing(f_x, f_y, f_c, t_x, t_y, lo, hi):
        rows = pl.ds(f_x * bs + own_of(lo, hi, f_x) - xlo(t_x), hi - lo)
        depth = pl.ds(pl.multiple_of(f_y * bsy + TILE * f_c - ylo(t_y), TILE), TILE)
        return corr.at[rows, depth, :]

    def edge(e):
        lo, hi = final[e]
        return max(lo, bs - reach), hi

    def spread(e):
        lo, hi = final[e]

        def one(where, to_core, lo, hi, send, recv):
            tx, ty = beside(*where)
            remote(
                strip(csend, lo, hi), landing(bx, by, core, tx, ty, lo, hi),
                send, recv, step=chip(tx, ty) * 2 + to_core,
            ).start()

        lo2, hi2 = edge(e)
        if hi2 > lo2:

            @pl.when(near)
            def _():
                for c in range(2):
                    one((1, 1), c, lo2, hi2, csem_s.at[2], bsem_r.at[e])

            for c in range(2):
                one((1, 0), c, lo2, hi2, csem_s.at[0], bsem_r.at[e])

        @pl.when(near)
        def _():
            for c in range(2):
                one((0, 1), c, lo, hi, csem_s.at[1], csem_r.at[e])

        one((0, 0), 1 - core, lo, hi, csem_s.at[0], csem_r.at[e])

    def spread_done():
        taken(srcv.at[pl.ds(0, bs + 2 * reach), pl.ds(0, TILE), :], csem_s.at[0]).wait_send()

        @pl.when(near)
        def _():
            taken(srcv.at[pl.ds(0, 2 * bs), pl.ds(0, TILE), :], csem_s.at[1]).wait_send()
            taken(srcv.at[pl.ds(0, 2 * reach), pl.ds(0, TILE), :], csem_s.at[2]).wait_send()

    def gather(e, kind):
        lo, hi = final[e]
        if kind == "own":
            taken(corr.at[pl.ds(0, hi - lo), pl.ds(0, 2 * TILE), :], csem_r.at[e]).wait_recv()
        else:
            lo, hi = edge(e)
            taken(corr.at[pl.ds(0, hi - lo)], bsem_r.at[e]).wait_recv()

    def change(e):
        lo, hi = final[e]
        swap(e).wait_recv()

        @pl.when(w > 0)
        def _():
            taken(zgot.at[:, pl.ds(0, hi - lo)], zsem_r.at[e]).wait_recv()

        mine = pl.ds(own_of(lo, hi), hi - lo)
        value = (zgot[0, mine] + zgot[1, mine]) - alpha_corner * (emine[mine] + egot[mine])
        csend[mine] = value
        corr[pl.ds(ox + own_of(lo, hi), hi - lo), pl.ds(pl.multiple_of(oy + TILE * core, TILE), TILE), :] = value
        spread(e)

    def second_weight(p, weight):
        return weight[2] + (pick(1.0, 0.0) * weight[1] if p == 0 else 0.0)

    def correct(start, rows):
        for n in range(rows):
            i = start + n
            x = corr[held(i)] * (1.0 / coupling)
            for p in range(pairs):
                weight = weights(p, i)
                spot = pl.ds(TILE, ey)
                ref = levels[0][p]
                ref[0, i + 1, spot] = ref[0, i + 1, spot] + weight[0] * x
                ref[1, i + 1, spot] = ref[1, i + 1, spot] + second_weight(p, weight) * x

    def trade(i, o):
        lo, hi = leave[o]
        mine = pl.ds(own_of(lo, hi), hi - lo)
        return remote(xsend.at[i, mine], xgot.at[i, mine], xsem_s, xsem_r.at[o], step=partner)

    def emit(o):
        lo, hi = leave[o]
        for i in range(kept):
            part(xsend.at[i], (2 * i + 1, 2 * i), lo, hi, 0, bsy)
            trade(i, o).start()
        for i in range(kept):
            part(obuf.at[i], (2 * i, 2 * i + 1), lo, hi, 0, bsy)

    def place(b_x, b_y, lo, hi):
        rows = pl.ds(b_x * bs + own_of(lo, hi, b_x), hi - lo)
        return out.at[rows, pl.ds(pl.multiple_of(b_y * bsy, TILE), bsy), :]

    def settle(o):
        lo, hi = leave[o]
        mine = pl.ds(own_of(lo, hi), hi - lo)
        ratio = gamma ** (-half)
        taken(xgot.at[:, pl.ds(0, hi - lo)], xsem_r.at[o]).wait_recv()
        for i in range(kept):
            ours, theirs = obuf[i, mine], xgot[i, mine]
            obuf[i, mine] = ours + theirs
            obuf[i + kept, mine] = pick(ratio, -ratio) * (ours - theirs)
        for where in others:
            k = chip(*beside(*where))
            remote(
                strip(obuf.at[k], lo, hi), place(bx, by, lo, hi), osem.at[0], osem.at[1], step=2 * k + core
            ).start()
        pltpu.make_async_copy(strip(obuf.at[m], lo, hi), place(bx, by, lo, hi), hsem).start()

    def receive(c):
        lo, hi = arrive[c]
        taken(raw.at[0, pl.ds(0, len(others)), pl.ds(0, hi - lo)], isem.at[c]).wait_recv()
        block = raw.at[core, :, pl.ds(rows_of(lo, hi), hi - lo)]
        remote(block, block, fsem, dsem.at[c], step=partner).start()

    def advance(c):
        a, b = arrive[c]
        taken(raw.at[0, :, pl.ds(0, b - a)], dsem.at[c]).wait_recv()
        grouped(a, b - a, spectrum, 3)
        sweeps(a, b)

    waiting = []

    def again(g):
        a, b, needs = second[g]
        for kind, e in needs:
            gather(e, kind)
        grouped(a, b - a, correct, 5)
        sweeps(a, b)
        if g in after:
            emit(after[g])
            if waiting:
                settle(waiting.pop())
            waiting.append(after[g])

    chunks, ends = len(arrive), len(final)

    def step(c):
        advance(c)
        e = c - (chunks - ends)
        if e >= 0:
            finish(e)
            if 1 <= e < ends - 1:
                change(e - 1)

    loads[2].wait()
    loads[3].wait()
    for c in range(chunks):
        receive(c)
        if c:
            step(c - 1)
    step(chunks - 1)
    late = [ends - 2, ends - 1]
    for g in range(len(second)):
        while any(kind == "own" and e in late for kind, e in second[g][2]):
            change(late.pop(0))
        again(g)
        if late:
            change(late.pop(0))
    settle(waiting.pop())

    taken(raw.at[0, pl.ds(0, len(others))], asem).wait_send()
    taken(raw.at[0], fsem).wait_send()
    taken(esend, esem_s).wait_send()
    spread_done()

    @pl.when(w < windows - 1)
    def _():
        taken(zgot, zsem_s).wait_send()

    taken(xsend, xsem_s).wait_send()
    taken(obuf.at[pl.ds(0, len(others))], osem.at[0]).wait_send()
    taken(obuf.at[pl.ds(0, len(others))], osem.at[1]).wait_recv()
    pltpu.make_async_copy(obuf.at[0], obuf.at[0], hsem).wait()


def waves(initial_state, source, absorption):
    length = lax.axis_size("step")
    windows = lax.axis_size("win")
    nx, ny, nz = initial_state.shape
    half = length // 2
    reach = SWEEPS - 1
    bs, bsy = nx // 2, ny // 2
    ext = bs + reach
    ey = bsy + TILE
    units = length // 2
    plan = spans(ext, bs, reach)
    arrive, final, _, leave, _ = (len(group) for group in plan)
    f32 = jnp.float32
    dma = pltpu.SemaphoreType.DMA
    edge = pltpu.VMEM((bs, TILE, nz), f32)
    return pl.pallas_call(
        functools.partial(wave_kernel, length, windows, nx, ny, ext, ey, plan),
        out_shape=jax.ShapeDtypeStruct((nx, ny, nz), f32),
        in_specs=[pl.BlockSpec(memory_space=pltpu.HBM)] * 3,
        out_specs=pl.BlockSpec(memory_space=pl.ANY),
        scratch_shapes=[
            pltpu.VMEM((nx, ny, nz), f32),
            pltpu.VMEM((2, half, ext, ey, nz), f32),
            pltpu.VMEM((ext, ey, nz), f32),
            pltpu.VMEM((ext, ey, nz), f32),
            pltpu.VMEM((3 * length // 4, ext, ey, nz), f32),
            [[pltpu.VMEM((2, ext + 2, ey + 2 * TILE, nz), f32)] * (units // 2)] * reach,
            [pltpu.VMEM((2, bs, bsy, nz), f32)] * (units // 2),
            pltpu.VMEM((ext, ey, nz), f32),
            edge, edge, edge,
            pltpu.VMEM((2, bs, TILE, nz), f32),
            edge,
            pltpu.VMEM((half // 2, bs, bsy, nz), f32),
            pltpu.VMEM((half // 2, bs, bsy, nz), f32),
            pltpu.VMEM((half, bs, bsy, nz), f32),
            dma((4,)),
            dma,
            dma((arrive,)),
            dma,
            dma((arrive,)),
            dma,
            dma((final,)),
            dma,
            dma((final,)),
            dma((3,)),
            dma((final,)),
            dma((final,)),
            dma,
            dma((leave,)),
            dma((2,)),
            dma,
        ],
        compiler_params=pltpu.CompilerParams(
            collective_id=0, has_side_effects=True, vmem_limit_bytes=40 * 1024 * 1024
        ),
    )(*(pltpu.with_memory_space_constraint(x, pltpu.HBM) for x in (source[0, 0], initial_state, absorption)))[None, None]


def fits(mesh, shape):
    length = mesh.shape["step"]
    if length % 8 or shape[2] != LANES or shape[1] != 4 * TILE:
        return False
    gx = length // 4
    return shape[0] % gx == 0 and shape[0] // gx >= SWEEPS - 1


def pairs_up(mesh, shape):
    return mesh.shape["step"] == 8 and shape[0] // 2 >= 2 * SWEEPS


def solution(mesh):
    def body(initial_state, source, absorption):
        plan = per_device
        if fits(mesh, initial_state.shape):
            plan = waves if pairs_up(mesh, initial_state.shape) else blocks
        return plan(initial_state, source, absorption)

    return jax.shard_map(
        body,
        mesh=mesh,
        in_specs=(P(), P("win", "step", None, None, None), P()),
        out_specs=P("win", "step", None, None, None),
        check_vma=False,
    )
```

```python
import functools
import math

import jax
import jax.numpy as jnp
from jax import lax
from jax.experimental import pallas as pl
from jax.experimental.pallas import tpu as pltpu
from jax.sharding import PartitionSpec as P

ITERS = 2
SWEEPS = 8


alpha_corner = 0.1
coupling = 0.05


def from_behind(block, axis, distance):
    devices = range(lax.axis_size(axis))
    route = [(i - distance, i) for i in devices if i - distance in devices]
    return lax.ppermute(block, axis, route)


def pad_cube(field):
    widths = [(0, 0)] * (field.ndim - 3) + [(1, 1)] * 3
    return jnp.pad(field, widths)


def neighbours(field):
    padded = pad_cube(field)
    total = padded[..., 2:, 1:-1, 1:-1] + padded[..., :-2, 1:-1, 1:-1]
    total = total + padded[..., 1:-1, 2:, 1:-1] + padded[..., 1:-1, :-2, 1:-1]
    total = total + padded[..., 1:-1, 1:-1, 2:] + padded[..., 1:-1, 1:-1, :-2]
    return total


def complex_times(first, second):
    return jnp.stack(
        [first[0] * second[0] - first[1] * second[1], first[0] * second[1] + first[1] * second[0]]
    )


def relax(spectrum, inverse):
    field = complex_times(inverse, spectrum)
    for repeat in range(SWEEPS - 1):
        field = complex_times(inverse, spectrum + coupling * neighbours(field))
    return field


def inverse_diagonal(angle, absorption, gamma):
    real_part = 1.0 - gamma * jnp.cos(angle) + absorption + 6.0 * coupling
    imag_part = jnp.broadcast_to(gamma * jnp.sin(angle), real_part.shape)
    magnitude = real_part * real_part + imag_part * imag_part
    return jnp.stack([real_part / magnitude, -imag_part / magnitude])


def dft_tables(window_len):
    index = jnp.arange(window_len, dtype=jnp.int32)
    product = index[:, None] * index[None, :] % window_len
    angle = product.astype(jnp.float32) * (2.0 * math.pi / window_len)
    return (jnp.cos(angle), jnp.sin(angle))


def transform_exchange(scaled, window_len):
    pencil = lax.all_to_all(scaled[None], "step", split_axis=1, concat_axis=0, tiled=True)
    cosine, sine = dft_tables(window_len)
    flat = pencil.reshape(window_len, -1)
    real_part = jnp.dot(cosine, flat, precision=lax.Precision.HIGHEST)
    imag_part = -jnp.dot(sine, flat, precision=lax.Precision.HIGHEST)
    shaped = pencil.shape
    spectrum = (
        lax.all_to_all(real_part.reshape(shaped), "step", split_axis=0, concat_axis=1, tiled=True),
        lax.all_to_all(imag_part.reshape(shaped), "step", split_axis=0, concat_axis=1, tiled=True),
    )
    return jnp.stack([spectrum[0][0], spectrum[1][0]])


def untransform_exchange(field, window_len):
    pencil = (
        lax.all_to_all(field[0][None], "step", split_axis=1, concat_axis=0, tiled=True),
        lax.all_to_all(field[1][None], "step", split_axis=1, concat_axis=0, tiled=True),
    )
    cosine, sine = dft_tables(window_len)
    shaped = pencil[0].shape
    values = jnp.dot(cosine, pencil[0].reshape(window_len, -1), precision=lax.Precision.HIGHEST)
    values = values - jnp.dot(
        sine, pencil[1].reshape(window_len, -1), precision=lax.Precision.HIGHEST
    )
    values = values / window_len
    result = lax.all_to_all(values.reshape(shaped), "step", split_axis=0, concat_axis=1, tiled=True)
    return result[0]


def per_device(initial_state, source, absorption):
    window_len = lax.axis_size("step")
    moment = lax.axis_index("step")
    window_index = lax.axis_index("win")
    gamma = alpha_corner ** (1.0 / window_len)
    scale = gamma ** moment.astype(jnp.float32)
    forcing_base = source[0, 0]
    is_first = moment == 0
    state = jnp.zeros_like(forcing_base)
    angle = moment.astype(jnp.float32) * (2.0 * math.pi / window_len)
    inverse = inverse_diagonal(angle, absorption, gamma)
    for repeat in range(ITERS):
        if repeat == 0:
            correction = jnp.where(window_index == 0, initial_state, 0.0)
        else:
            ends = from_behind(state, "step", 1 - window_len)
            before = from_behind(ends, "win", 1)
            before = jnp.where(window_index == 0, initial_state, before)
            correction = before - alpha_corner * ends
        forcing = forcing_base + jnp.where(is_first, correction, 0.0)
        scaled = forcing * scale
        spectrum = transform_exchange(scaled, window_len)
        field = relax(spectrum, inverse)
        values = untransform_exchange(field, window_len)
        state = values / scale
    return state[None, None]


LANES = 128
TILE = 8
GROUP = 8


def tables(length):
    gamma = alpha_corner ** (1.0 / length)
    into, back, angles = [], [], []
    for core in range(2):
        rows_in, rows_back = [], []
        for time in range(length):
            scale = gamma**time
            row_in, row_back = [], []
            for p in range(length // 4):
                j = 2 * p + core
                if j == 0:
                    pair, weight = (1.0, (-1.0) ** time), 1.0 / length
                else:
                    turn = 2.0 * math.pi * (j * time % length) / length
                    pair, weight = (math.cos(turn), -math.sin(turn)), 2.0 / length
                row_in += [value * scale / coupling for value in pair]
                row_back += [value * weight / scale for value in pair]
            rows_in.append(row_in)
            rows_back.append(row_back)
        into.append(rows_in)
        back.append(rows_back)
        angles.append([2.0 * math.pi * (2 * p + core) / length for p in range(length // 4)])
    return into, back, angles


def kernel(
    length, windows, nx, ny, ext, ey,
    source, initial, absorb, out,
    raw, first, absv, coef, base, again, fa, fb, corr,
    psend, pgot, ends, zgot, csend, qsend, qgot, obuf,
    lsem, asend, brecv, fsend, esem, zsem, csem_s, csem_r, qsem_s, qsem_r, osem_s, osem_r,
):
    half = length // 2
    gx, gy = half // 2, 2
    bs, bsy = nx // gx, ny // gy
    reach = SWEEPS - 1
    pairs = length // 4
    units = 2 * pairs
    gamma = alpha_corner ** (1.0 / length)
    into, back, angles = tables(length)
    me = lax.axis_index("step")
    w = lax.axis_index("win")
    core, m = me % 2, me // 2
    partner = m * 2 + (1 - core)
    bx, by = m % gx, m // gx

    def xlo(b):
        if gx == 2:
            return b * (nx - ext)
        return jnp.minimum(jnp.maximum(b * bs - reach, 0), nx - ext)

    def ylo(b):
        return pl.multiple_of(b * (ny - ey), TILE)

    def pick(a, b):
        return jnp.where(core == 0, jnp.float32(a), jnp.float32(b))

    def region(ref, b_x, b_y):
        return ref.at[pl.ds(xlo(b_x), ext), pl.ds(ylo(b_y), ey), :]

    ox = bx * bs - xlo(bx)
    oy = pl.multiple_of(by * bsy - ylo(by), TILE)

    loads = [
        pltpu.make_async_copy(region(absorb, bx, by), absv, lsem.at[0]),
        pltpu.make_async_copy(region(source, bx, by), raw.at[me], lsem.at[1]),
        pltpu.make_async_copy(region(initial, bx, by), first, lsem.at[2]),
    ]
    for load in loads:
        load.start()
    zero_row = jnp.zeros((ey, LANES), jnp.float32)
    for u in range(units):
        for ref in (fa, fb):
            ref[u, 0, pl.ds(TILE, ey)] = zero_row
            ref[u, ext + 1, pl.ds(TILE, ey)] = zero_row
            for r in range(1, ext + 1):
                ref[u, r, pl.ds(0, TILE)] = zero_row[:TILE]
                ref[u, r, pl.ds(TILE + ey, TILE)] = zero_row[:TILE]
    if gx > 2:
        corr[...] = jnp.zeros_like(corr)

    barrier = pltpu.get_barrier_semaphore()
    for d in range(1, length):
        pl.semaphore_signal(
            barrier, inc=1, device_id={"step": (me + d) % length}, device_id_type=pl.DeviceIdType.MESH
        )

    @pl.when(w > 0)
    def _():
        pl.semaphore_signal(barrier, inc=1, device_id={"win": w - 1}, device_id_type=pl.DeviceIdType.MESH)

    @pl.when(w < windows - 1)
    def _():
        pl.semaphore_signal(barrier, inc=1, device_id={"win": w + 1}, device_id_type=pl.DeviceIdType.MESH)

    nearby = jnp.where(w > 0, 1, 0) + jnp.where(w < windows - 1, 1, 0)
    pl.semaphore_wait(barrier, length - 1 + nearby)

    def remote(src, dst, send, recv, **where):
        return pltpu.make_async_remote_copy(
            src_ref=src, dst_ref=dst, send_sem=send, recv_sem=recv,
            device_id=where, device_id_type=pl.DeviceIdType.MESH,
        )

    outgoing = []
    for d in range(1, half):
        to = (m + d) % half
        copy = remote(
            region(source, to % gx, to // gx), raw.at[me], asend.at[d], brecv.at[me], step=to * 2 + core
        )
        copy.start()
        outgoing.append(copy)
    copy = remote(region(source, bx, by), raw.at[me], asend.at[0], brecv.at[me], step=partner)
    copy.start()
    outgoing.append(copy)

    def grouped(begin, count, work, most=GROUP):
        size = -(-count // max(1, count // most))

        def body(g, carry):
            work(begin + g * size, size)
            return carry

        lax.fori_loop(0, count // size, body, 0)
        if count % size:
            work(begin + count - size, size)

    def each(one):
        def work(start, rows):
            for n in range(rows):
                one(start + n)

        return work

    loads[0].wait()

    def coefficients(i):
        for p in range(pairs):
            rows = absv[i]
            cosine = pick(math.cos(angles[0][p]), math.cos(angles[1][p]))
            imag = pick(gamma * math.sin(angles[0][p]), gamma * math.sin(angles[1][p]))
            real = 1.0 - gamma * cosine + rows + 6.0 * coupling
            over = coupling / (real * real + imag * imag)
            coef[3 * p, i] = real * over
            coef[3 * p + 1, i] = -imag * over
            if p == 0:
                other = pick(-1.0, math.cos(angles[1][p]))
                real = 1.0 - gamma * other + rows + 6.0 * coupling
                over = coupling / (real * real + imag * imag)
                coef[3 * p + 2, i] = real * over

    grouped(0, ext, each(coefficients))

    def weights(p, i):
        straight = coef[3 * p, i]
        return straight, (coef[3 * p + 2, i] if p == 0 else straight), coef[3 * p + 1, i]

    def arrival(t):
        return remote(raw.at[t], raw.at[t], asend.at[0], brecv.at[t], step=partner)

    for d in range(1, half):
        t = ((m + half - d) % half) * 2 + core
        arrival(t).wait_recv()
        copy = remote(raw.at[t], raw.at[t], fsend.at[d], brecv.at[t], step=partner)
        copy.start()
        outgoing.append(copy)
    for d in range(half):
        arrival(((m + half - d) % half) * 2 + (1 - core)).wait_recv()
    loads[1].wait()
    loads[2].wait()
    is_first = jnp.where(w == 0, jnp.float32(1.0 / coupling), jnp.float32(0.0))

    def second_weight(p, weight):
        return weight[2] + (pick(1.0, 0.0) * weight[1] if p == 0 else 0.0)

    def transform(i):
        begin = first[i] * is_first
        fields = [raw[t, i] for t in range(length)]
        for p in range(pairs):
            weight = weights(p, i)
            s0, s1 = begin, begin * pick(1.0, 0.0) if p == 0 else None
            for t in range(length):
                s0 = s0 + pick(into[0][t][2 * p], into[1][t][2 * p]) * fields[t]
                term = pick(into[0][t][2 * p + 1], into[1][t][2 * p + 1]) * fields[t]
                s1 = term if s1 is None else s1 + term
            b0 = weight[0] * s0 - weight[2] * s1
            b1 = weight[1] * s1 + weight[2] * s0
            base[2 * p, i] = b0
            base[2 * p + 1, i] = b1
            fa[2 * p, i + 1, pl.ds(TILE, ey)] = b0
            fa[2 * p + 1, i + 1, pl.ds(TILE, ey)] = b1

    grouped(0, ext, each(transform), GROUP // 2)

    lane = lax.broadcasted_iota(jnp.int32, (ey, LANES), 1)

    def around(ref, u, r):
        v = ref[u, r, pl.ds(TILE, ey)]
        total = jnp.where(lane == 0, 0.0, pltpu.roll(v, 1, 1))
        total = total + jnp.where(lane == LANES - 1, 0.0, pltpu.roll(v, LANES - 1, 1))
        beside = ref[u, r - 1, pl.ds(TILE, ey)] + ref[u, r + 1, pl.ds(TILE, ey)]
        return total + (beside + (ref[u, r, pl.ds(TILE - 1, ey)] + ref[u, r, pl.ds(TILE + 1, ey)]))

    def sweep_rows(base, here, there, start, rows):
        for n in range(rows):
            i = start + n
            for p in range(pairs):
                weight = weights(p, i)
                n0 = around(here, 2 * p, i + 1)
                n1 = around(here, 2 * p + 1, i + 1)
                there[2 * p, i + 1, pl.ds(TILE, ey)] = base[2 * p, i] + (weight[0] * n0 - weight[2] * n1)
                there[2 * p + 1, i + 1, pl.ds(TILE, ey)] = base[2 * p + 1, i] + (
                    weight[1] * n1 + weight[2] * n0
                )

    def sweeps(base):
        here, there = fa, fb
        for k in range(1, SWEEPS):
            begin, count = (bx * k, ext - k) if gx == 2 else (0, ext)
            grouped(begin, count, functools.partial(sweep_rows, base, here, there))
            here, there = there, here
        return here

    final = sweeps(base)

    def part(t, y0, rows):
        total = None
        for u in range(units):
            factor = pick(back[0][t[0]][u], back[1][t[1]][u])
            term = factor * final[u, pl.ds(ox + 1, bs), pl.ds(y0 + TILE, rows), :]
            total = term if total is None else total + term
        return total

    last = (length - 1, length - 1)
    psend[...] = part(last, pl.multiple_of(oy + TILE * (1 - core), TILE), TILE)
    swap = remote(psend, pgot, esem.at[0], esem.at[1], step=partner)
    swap.start()
    mine = part(last, pl.multiple_of(oy + TILE * core, TILE), TILE)
    swap.wait_recv()
    mine = mine + pgot[...]
    ends[...] = mine
    outgoing.append(swap)

    onward = remote(ends, zgot, zsem.at[0], zsem.at[1], win=(w + 1) % windows)

    @pl.when(w < windows - 1)
    def _():
        onward.start()

    @pl.when(w == 0)
    def _():
        zgot[...] = jnp.zeros_like(zgot)

    @pl.when(w > 0)
    def _():
        onward.wait_recv()

    change = zgot[...] - alpha_corner * ends[...]
    csend[...] = change
    corr[pl.ds(ox, bs), pl.ds(pl.multiple_of(oy + TILE * core, TILE), TILE), :] = change

    def spread(ex, ey_, send):
        rows, skip = (bs, 0) if ex == 0 else (reach, bs - reach if ex == 1 else 0)
        tx, ty = (bx + ex, by + ey_) if send else (bx, by)
        fx, fy = (bx, by) if send else (bx - ex, by - ey_)
        ax, ay = (tx, ty) if send else (fx, fy)
        inside = (ax >= 0) & (ax < gx) & (ay >= 0) & (ay < gy)
        slot = ((ex + 1) * 3 + (ey_ + 1)) * 2
        for c in range(2):
            near = c == (1 if ey_ == 1 else 0)
            if send:
                okay = inside if ey_ == 0 else inside & (core == (1 if ey_ == 1 else 0))
                if ex == 0 and ey_ == 0:
                    okay = core != c
                fc, tc = core, c
            else:
                if ey_ != 0 and not near:
                    continue
                okay = inside
                if ex == 0 and ey_ == 0:
                    okay = core != c
                fc, tc = c, core

            @pl.when(okay)
            def _(c=c, fc=fc, tc=tc):
                copy = remote(
                    csend.at[pl.ds(skip, rows)],
                    corr.at[
                        pl.ds(fx * bs + skip - xlo(tx), rows),
                        pl.ds(pl.multiple_of(fy * bsy + TILE * fc - ylo(ty), TILE), TILE),
                        :,
                    ],
                    csem_s.at[slot + c],
                    csem_r.at[slot + fc],
                    step=(ty * gx + tx) * 2 + tc if send == 1 else partner,
                )
                if send == 1:
                    copy.start()
                elif send == 2:
                    copy.wait_send()
                else:
                    copy.wait_recv()

    offsets = [(ex, e) for ex in (-1, 0, 1) for e in (-1, 0, 1)]
    for ex, e in offsets:
        spread(ex, e, 1)
    for ex, e in offsets:
        spread(ex, e, 0)

    def correct(i):
        x = corr[i] * (1.0 / coupling)
        for p in range(pairs):
            weight = weights(p, i)
            b0 = base[2 * p, i] + weight[0] * x
            b1 = base[2 * p + 1, i] + second_weight(p, weight) * x
            again[2 * p, i] = b0
            again[2 * p + 1, i] = b1
            fa[2 * p, i + 1, pl.ds(TILE, ey)] = b0
            fa[2 * p + 1, i + 1, pl.ds(TILE, ey)] = b1

    grouped(0, ext, each(correct))
    final = sweeps(again)

    for k in range(half):
        qsend[k] = part((2 * k + 1, 2 * k), oy, bsy)
        copy = remote(qsend.at[k], qgot.at[k], qsem_s.at[k], qsem_r.at[k], step=partner)
        copy.start()
        outgoing.append(copy)
    for k in range(half):
        obuf[k] = part((2 * k, 2 * k + 1), oy, bsy)

    def place(b_x, b_y):
        return out.at[pl.ds(b_x * bs, bs), pl.ds(pl.multiple_of(b_y * bsy, TILE), bsy), :]

    for k in range(half):
        remote(qsend.at[k], qgot.at[k], qsem_s.at[k], qsem_r.at[k], step=partner).wait_recv()
        obuf[k] = obuf[k] + qgot[k]

        @pl.when(m == k)
        def _(k=k):
            pltpu.make_async_copy(obuf.at[k], place(bx, by), lsem.at[3]).start()

        @pl.when(m != k)
        def _(k=k):
            remote(obuf.at[k], place(bx, by), osem_s.at[k], osem_r.at[m], step=2 * k + core).start()

    for copy in outgoing:
        copy.wait_send()
    for ex, e in offsets:
        spread(ex, e, 2)

    @pl.when(w < windows - 1)
    def _():
        onward.wait_send()

    for k in range(half):

        @pl.when(m == k)
        def _(k=k):
            pltpu.make_async_copy(obuf.at[k], place(bx, by), lsem.at[3]).wait()

        @pl.when(m != k)
        def _(k=k):
            done = remote(obuf.at[k], place(k % gx, k // gx), osem_s.at[k], osem_r.at[k], step=partner)
            done.wait_send()
            done.wait_recv()


def blocks(initial_state, source, absorption):
    length = lax.axis_size("step")
    windows = lax.axis_size("win")
    nx, ny, nz = initial_state.shape
    half = length // 2
    gx, reach = half // 2, SWEEPS - 1
    bs, bsy = nx // gx, ny // 2
    ext = min(nx, bs + reach * (1 if gx == 2 else 2))
    ey = bsy + -(-reach // TILE) * TILE
    units = length // 2
    f32 = jnp.float32
    dma = pltpu.SemaphoreType.DMA
    return pl.pallas_call(
        functools.partial(kernel, length, windows, nx, ny, ext, ey),
        out_shape=jax.ShapeDtypeStruct((nx, ny, nz), f32),
        in_specs=[pl.BlockSpec(memory_space=pl.ANY)] * 3,
        out_specs=pl.BlockSpec(memory_space=pl.ANY),
        scratch_shapes=[
            pltpu.VMEM((length, ext, ey, nz), f32),
            pltpu.VMEM((ext, ey, nz), f32),
            pltpu.VMEM((ext, ey, nz), f32),
            pltpu.VMEM((3 * length // 4, ext, ey, nz), f32),
            pltpu.VMEM((units, ext, ey, nz), f32),
            pltpu.VMEM((units, ext, ey, nz), f32),
            pltpu.VMEM((units, ext + 2, ey + 2 * TILE, nz), f32),
            pltpu.VMEM((units, ext + 2, ey + 2 * TILE, nz), f32),
            pltpu.VMEM((ext, ey, nz), f32),
            pltpu.VMEM((bs, TILE, nz), f32),
            pltpu.VMEM((bs, TILE, nz), f32),
            pltpu.VMEM((bs, TILE, nz), f32),
            pltpu.VMEM((bs, TILE, nz), f32),
            pltpu.VMEM((bs, TILE, nz), f32),
            pltpu.VMEM((half, bs, bsy, nz), f32),
            pltpu.VMEM((half, bs, bsy, nz), f32),
            pltpu.VMEM((half, bs, bsy, nz), f32),
            dma((4,)),
            dma((half,)),
            dma((length,)),
            dma((half,)),
            dma((2,)),
            dma((2,)),
            dma((18,)),
            dma((18,)),
            dma((half,)),
            dma((half,)),
            dma((half,)),
            dma((half,)),
        ],
        compiler_params=pltpu.CompilerParams(
            collective_id=0, has_side_effects=True, vmem_limit_bytes=28 * 1024 * 1024
        ),
    )(source[0, 0], initial_state, absorption)[None, None]


ARRIVE = (8, 4, 3, 3, 3)
SECOND = (5, 3, 3, 3, 3, 3)
LEAST = 1


def cuts(sizes, extent):
    bounds = [0]
    for size in sizes:
        if bounds[-1] + size < extent:
            bounds.append(bounds[-1] + size)
    bounds.append(extent)
    return list(zip(bounds[:-1], bounds[1:]))


def spans(ext, bs, reach):
    arrive = cuts(ARRIVE, ext)
    final = [(max(0, a - reach), b - reach) for a, b in arrive if b > reach]
    sources = [(a, b, "own", e) for e, (a, b) in enumerate(final)]
    for e, (a, b) in enumerate(final):
        if b > bs - reach:
            sources.append((2 * bs - b, 2 * bs - max(a, bs - reach), "beyond", e))
    second, leave, after, sent = [], [], {}, 0
    groups = cuts(SECOND, ext)
    for g, (a, b) in enumerate(groups):
        needs = [(kind, e) for lo, hi, kind, e in sources if a <= lo < b or (lo < a and g == 0)]
        second.append((a, b, needs))
        if b - reach - sent >= LEAST or g == len(groups) - 1:
            after[g] = len(leave)
            leave.append((sent, b - reach))
            sent = b - reach
    return arrive, final, second, leave, after


def wave_kernel(
    length, windows, nx, ny, ext, ey, plan,
    source, initial, absorb, out,
    srcv, raw, first, absv, coef, levels, fin, corr,
    emine, esend, egot, zgot, csend, xsend, xgot, obuf,
    lsem, asem, isem, fsem, dsem, esem_s, esem_r, zsem_s, zsem_r, csem_s, csem_r, bsem_r, xsem_s, xsem_r, osem, hsem,
):
    arrive, final, second, leave, after = plan
    half = length // 2
    bs, bsy = nx // 2, ny // 2
    reach = SWEEPS - 1
    pairs = length // 4
    units = 2 * pairs
    kept = half // 2
    gamma = alpha_corner ** (1.0 / length)
    into, back, angles = tables(length)
    me = lax.axis_index("step")
    w = lax.axis_index("win")
    core, m = me % 2, me // 2
    partner = m * 2 + (1 - core)
    bx, by = m % 2, m // 2
    near = core == 1 - by

    def chip(b_x, b_y):
        return b_y * 2 + b_x

    def xlo(b):
        return b * (nx - ext)

    def ylo(b):
        return pl.multiple_of(b * (ny - ey), TILE)

    def rows_of(lo, hi, b=bx):
        return lo + b * (ext - lo - hi)

    def own_of(lo, hi, b=bx):
        return lo + b * (bs - lo - hi)

    def held(i):
        return i + bx * (ext - 1 - 2 * i)

    def own(i):
        return i + bx * (bs - 1 - 2 * i)

    def pick(a, b):
        if a == b:
            return jnp.float32(a)
        return jnp.where(core == 0, jnp.float32(a), jnp.float32(b))

    def region(ref, b_x, b_y, lo, hi):
        rows = pl.ds(xlo(b_x) + rows_of(lo, hi, b_x), hi - lo)
        return ref.at[rows, pl.ds(ylo(b_y), ey), :]

    ox = bx * bs - xlo(bx)
    oy = pl.multiple_of(by * bsy - ylo(by), TILE)

    loads = [
        pltpu.make_async_copy(source, srcv, lsem.at[0]),
        pltpu.make_async_copy(region(absorb, bx, by, 0, ext), absv, lsem.at[1]),
        pltpu.make_async_copy(region(source, bx, by, 0, ext), raw.at[core, m], lsem.at[2]),
        pltpu.make_async_copy(region(initial, bx, by, 0, ext), first, lsem.at[3]),
    ]
    for load in loads:
        load.start()

    barrier = pltpu.get_barrier_semaphore()

    def greet(**where):
        pl.semaphore_signal(barrier, inc=1, device_id=where, device_id_type=pl.DeviceIdType.MESH)

    for d in range(1, length):
        greet(step=(me + d) % length)

    @pl.when(w > 0)
    def _():
        greet(win=w - 1, step=me)
        greet(win=w - 1, step=partner)

    @pl.when(w < windows - 1)
    def _():
        greet(win=w + 1, step=me)
        greet(win=w + 1, step=partner)

    @pl.when(w == 0)
    def _():
        zgot[...] = jnp.zeros_like(zgot)

    nearby = jnp.where(w > 0, 2, 0) + jnp.where(w < windows - 1, 2, 0)
    loads[0].wait()
    pl.semaphore_wait(barrier, length - 1 + nearby)

    def remote(src, dst, send, recv, **where):
        return pltpu.make_async_remote_copy(
            src_ref=src, dst_ref=dst, send_sem=send, recv_sem=recv,
            device_id=where, device_id_type=pl.DeviceIdType.MESH,
        )

    def taken(block, sem):
        return remote(block, block, sem, sem, step=partner)

    others = [(1, 1), (1, 0), (0, 1)]

    def beside(ex, e_y):
        return (bx + ex) % 2, (by + e_y) % 2

    for c, (lo, hi) in enumerate(arrive):
        for where in others:
            tx, ty = beside(*where)
            remote(
                region(srcv, tx, ty, lo, hi),
                raw.at[core, m, pl.ds(rows_of(lo, hi, tx), hi - lo)],
                asem, isem.at[c], step=chip(tx, ty) * 2 + core,
            ).start()

    zero_row = jnp.zeros((ey, LANES), jnp.float32)

    def rim(r, carry):
        for refs in levels:
            for ref in refs:
                for q in range(2):
                    ref[q, r, pl.ds(0, TILE)] = zero_row[:TILE]
                    ref[q, r, pl.ds(TILE + ey, TILE)] = zero_row[:TILE]
        return carry

    for refs in levels:
        for ref in refs:
            for q in range(2):
                for r in (0, ext + 1):
                    ref[q, r, pl.ds(TILE, ey)] = zero_row
    lax.fori_loop(1, ext + 1, rim, 0)

    def grouped(begin, count, work, most):
        groups = -(-count // most)
        size = -(-count // groups)
        if groups == 1:
            work(begin, count)
            return

        def body(g, carry):
            work(begin + g * size, size)
            return carry

        lax.fori_loop(0, count // size, body, 0)
        if count % size:
            work(begin + count - count % size, count % size)

    loads[1].wait()

    def coefficients(start, rows):
        for n in range(rows):
            i = start + n
            for p in range(pairs):
                here = absv[held(i)]
                cosine = pick(math.cos(angles[0][p]), math.cos(angles[1][p]))
                imag = pick(gamma * math.sin(angles[0][p]), gamma * math.sin(angles[1][p]))
                real = 1.0 - gamma * cosine + here + 6.0 * coupling
                over = coupling / (real * real + imag * imag)
                coef[3 * p, i] = real * over
                coef[3 * p + 1, i] = -imag * over
                if p == 0:
                    other = pick(-1.0, math.cos(angles[1][p]))
                    real = 1.0 - gamma * other + here + 6.0 * coupling
                    over = coupling / (real * real + imag * imag)
                    coef[3 * p + 2, i] = real * over

    grouped(0, ext, coefficients, 4)

    def weights(p, i, y0=0, rows=ey):
        part = pl.ds(y0, rows)
        straight = coef[3 * p, i, part]
        return straight, (coef[3 * p + 2, i, part] if p == 0 else straight), coef[3 * p + 1, i, part]

    is_first = jnp.where(w == 0, jnp.float32(1.0 / coupling), jnp.float32(0.0))

    def combine(pair, values):
        total = None
        for (a, b), value in zip(pair, values):
            if a == 0 and b == 0:
                continue
            term = value if a == 1 and b == 1 else pick(a, b) * value
            total = term if total is None else total + term
        return total

    def spectrum(start, rows):
        for n in range(rows):
            i = start + n
            folded = []
            for t in range(half):
                early, late = gamma**t / coupling, gamma ** (t + half) / coupling
                now, then = raw[t % 2, t // 2, held(i)], raw[t % 2, (t + half) // 2, held(i)]
                folded.append(early * now + pick(late, -late) * then)
            folded[0] = folded[0] + first[held(i)] * is_first
            for p in range(pairs):
                weight = weights(p, i)
                turn = [
                    [
                        tuple(into[c][t][2 * p + q] * coupling / gamma**t for c in range(2))
                        for t in range(half)
                    ]
                    for q in range(2)
                ]
                turn = [[tuple(round(v, 15) for v in pair) for pair in row] for row in turn]
                s0 = combine(turn[0], folded)
                s1 = combine(turn[1], folded)
                levels[0][p][0, i + 1, pl.ds(TILE, ey)] = weight[0] * s0 - weight[2] * s1
                levels[0][p][1, i + 1, pl.ds(TILE, ey)] = weight[1] * s1 + weight[2] * s0

    def stencil(ref, q, start, rows, y0, depth):
        lane = lax.broadcasted_iota(jnp.int32, (depth, LANES), 1)
        at = pl.multiple_of(y0 + TILE, TILE)
        line = [ref[q, start + n, pl.ds(at, depth)] for n in range(rows + 2)]
        sums = []
        for n in range(1, rows + 1):
            v = line[n]
            around = ref.at[q, start + n, pl.ds(y0, depth + 2 * TILE), :]
            total = jnp.where(lane == 0, 0.0, pltpu.roll(v, 1, 1))
            total = total + jnp.where(lane == LANES - 1, 0.0, pltpu.roll(v, LANES - 1, 1))
            across = around[pl.ds(TILE - 1, depth)] + around[pl.ds(TILE + 1, depth)]
            sums.append(total + ((line[n - 1] + line[n + 1]) + across))
        return sums

    def sweep_rows(k, start, rows):
        last = k == reach
        y0, depth = (oy, bsy) if last else (0, ey)
        at = pl.multiple_of(y0 + TILE, TILE)
        for p in range(pairs):
            s0 = stencil(levels[k - 1][p], 0, start, rows, y0, depth)
            s1 = stencil(levels[k - 1][p], 1, start, rows, y0, depth)
            for n in range(rows):
                i = start + n
                weight = weights(p, i, y0, depth)
                b0 = levels[0][p][0, i + 1, pl.ds(at, depth)]
                b1 = levels[0][p][1, i + 1, pl.ds(at, depth)]
                v0 = b0 + (weight[0] * s0[n] - weight[2] * s1[n])
                v1 = b1 + (weight[1] * s1[n] + weight[2] * s0[n])
                if last:
                    fin[p][0, i] = v0
                    fin[p][1, i] = v1
                else:
                    levels[k][p][0, i + 1, pl.ds(TILE, ey)] = v0
                    levels[k][p][1, i + 1, pl.ds(TILE, ey)] = v1

    def sweeps(a, b):
        for k in range(1, SWEEPS):
            lo, hi = max(0, a - k), b - k
            if hi > lo:
                grouped(lo, hi - lo, functools.partial(sweep_rows, k), 6)

    def part(ref, t, lo, hi, y0, depth):
        factors = [pick(back[0][t[0]][u], back[1][t[1]][u]) for u in range(units)]
        for i in range(lo, hi):
            total = None
            for u, factor in enumerate(factors):
                term = factor * fin[u // 2][u % 2, i, pl.ds(y0, depth)]
                total = term if total is None else total + term
            ref[own(i)] = total

    def strip(ref, lo, hi):
        return ref.at[pl.ds(own_of(lo, hi), hi - lo)]

    def swap(e):
        lo, hi = final[e]
        return remote(strip(esend, lo, hi), strip(egot, lo, hi), esem_s, esem_r.at[e], step=partner)

    def onward(e):
        lo, hi = final[e]
        after_w = (w + 1) % windows
        return [
            remote(strip(emine, lo, hi), strip(zgot.at[0], lo, hi), zsem_s, zsem_r.at[e], win=after_w, step=me),
            remote(strip(esend, lo, hi), strip(zgot.at[1], lo, hi), zsem_s, zsem_r.at[e], win=after_w, step=partner),
        ]

    def finish(e):
        lo, hi = final[e]
        last = (length - 1, length - 1)
        part(esend, last, lo, hi, pl.multiple_of(TILE * (1 - core), TILE), TILE)
        part(emine, last, lo, hi, pl.multiple_of(TILE * core, TILE), TILE)

        @pl.when(w < windows - 1)
        def _():
            for copy in onward(e):
                copy.start()

        swap(e).start()

    def landing(f_x, f_y, f_c, t_x, t_y, lo, hi):
        rows = pl.ds(f_x * bs + own_of(lo, hi, f_x) - xlo(t_x), hi - lo)
        depth = pl.ds(pl.multiple_of(f_y * bsy + TILE * f_c - ylo(t_y), TILE), TILE)
        return corr.at[rows, depth, :]

    def edge(e):
        lo, hi = final[e]
        return max(lo, bs - reach), hi

    def spread(e):
        lo, hi = final[e]

        def one(where, to_core, lo, hi, send, recv):
            tx, ty = beside(*where)
            remote(
                strip(csend, lo, hi), landing(bx, by, core, tx, ty, lo, hi),
                send, recv, step=chip(tx, ty) * 2 + to_core,
            ).start()

        lo2, hi2 = edge(e)
        if hi2 > lo2:

            @pl.when(near)
            def _():
                for c in range(2):
                    one((1, 1), c, lo2, hi2, csem_s.at[2], bsem_r.at[e])

            for c in range(2):
                one((1, 0), c, lo2, hi2, csem_s.at[0], bsem_r.at[e])

        @pl.when(near)
        def _():
            for c in range(2):
                one((0, 1), c, lo, hi, csem_s.at[1], csem_r.at[e])

        one((0, 0), 1 - core, lo, hi, csem_s.at[0], csem_r.at[e])

    def spread_done():
        taken(srcv.at[pl.ds(0, bs + 2 * reach), pl.ds(0, TILE), :], csem_s.at[0]).wait_send()

        @pl.when(near)
        def _():
            taken(srcv.at[pl.ds(0, 2 * bs), pl.ds(0, TILE), :], csem_s.at[1]).wait_send()
            taken(srcv.at[pl.ds(0, 2 * reach), pl.ds(0, TILE), :], csem_s.at[2]).wait_send()

    def gather(e, kind):
        lo, hi = final[e]
        if kind == "own":
            taken(corr.at[pl.ds(0, hi - lo), pl.ds(0, 2 * TILE), :], csem_r.at[e]).wait_recv()
        else:
            lo, hi = edge(e)
            taken(corr.at[pl.ds(0, hi - lo)], bsem_r.at[e]).wait_recv()

    def change(e):
        lo, hi = final[e]
        swap(e).wait_recv()

        @pl.when(w > 0)
        def _():
            taken(zgot.at[:, pl.ds(0, hi - lo)], zsem_r.at[e]).wait_recv()

        mine = pl.ds(own_of(lo, hi), hi - lo)
        value = (zgot[0, mine] + zgot[1, mine]) - alpha_corner * (emine[mine] + egot[mine])
        csend[mine] = value
        corr[pl.ds(ox + own_of(lo, hi), hi - lo), pl.ds(pl.multiple_of(oy + TILE * core, TILE), TILE), :] = value
        spread(e)

    def second_weight(p, weight):
        return weight[2] + (pick(1.0, 0.0) * weight[1] if p == 0 else 0.0)

    def correct(start, rows):
        for n in range(rows):
            i = start + n
            x = corr[held(i)] * (1.0 / coupling)
            for p in range(pairs):
                weight = weights(p, i)
                spot = pl.ds(TILE, ey)
                ref = levels[0][p]
                ref[0, i + 1, spot] = ref[0, i + 1, spot] + weight[0] * x
                ref[1, i + 1, spot] = ref[1, i + 1, spot] + second_weight(p, weight) * x

    def trade(i, o):
        lo, hi = leave[o]
        mine = pl.ds(own_of(lo, hi), hi - lo)
        return remote(xsend.at[i, mine], xgot.at[i, mine], xsem_s, xsem_r.at[o], step=partner)

    def emit(o):
        lo, hi = leave[o]
        for i in range(kept):
            part(xsend.at[i], (2 * i + 1, 2 * i), lo, hi, 0, bsy)
            trade(i, o).start()
        for i in range(kept):
            part(obuf.at[i], (2 * i, 2 * i + 1), lo, hi, 0, bsy)

    def place(b_x, b_y, lo, hi):
        rows = pl.ds(b_x * bs + own_of(lo, hi, b_x), hi - lo)
        return out.at[rows, pl.ds(pl.multiple_of(b_y * bsy, TILE), bsy), :]

    def settle(o):
        lo, hi = leave[o]
        mine = pl.ds(own_of(lo, hi), hi - lo)
        ratio = gamma ** (-half)
        taken(xgot.at[:, pl.ds(0, hi - lo)], xsem_r.at[o]).wait_recv()
        for i in range(kept):
            ours, theirs = obuf[i, mine], xgot[i, mine]
            obuf[i, mine] = ours + theirs
            obuf[i + kept, mine] = pick(ratio, -ratio) * (ours - theirs)
        for where in others:
            k = chip(*beside(*where))
            remote(
                strip(obuf.at[k], lo, hi), place(bx, by, lo, hi), osem.at[0], osem.at[1], step=2 * k + core
            ).start()
        pltpu.make_async_copy(strip(obuf.at[m], lo, hi), place(bx, by, lo, hi), hsem).start()

    def receive(c):
        lo, hi = arrive[c]
        taken(raw.at[0, pl.ds(0, len(others)), pl.ds(0, hi - lo)], isem.at[c]).wait_recv()
        block = raw.at[core, :, pl.ds(rows_of(lo, hi), hi - lo)]
        remote(block, block, fsem, dsem.at[c], step=partner).start()

    waiting = []
    chunks, ends = len(arrive), len(final)
    late = list(range(ends))

    def advance(c):
        a, b = arrive[c]
        taken(raw.at[0, :, pl.ds(0, b - a)], dsem.at[c]).wait_recv()
        e = c - (chunks - ends)
        while late and late[0] <= min(e - 2, ends - 4):
            change(late.pop(0))
        grouped(a, b - a, spectrum, 3)
        sweeps(a, b)

    def again(g):
        a, b, needs = second[g]
        for kind, e in needs:
            gather(e, kind)
        grouped(a, b - a, correct, 5)
        sweeps(a, b)
        if g in after:
            emit(after[g])
            if waiting:
                settle(waiting.pop())
            waiting.append(after[g])

    def step(c):
        advance(c)
        e = c - (chunks - ends)
        if e >= 0:
            finish(e)

    loads[2].wait()
    loads[3].wait()
    for c in range(chunks):
        receive(c)
        if c:
            step(c - 1)
    step(chunks - 1)
    change(late.pop(0))
    for g in range(len(second)):
        while any(kind == "own" and e in late for kind, e in second[g][2]):
            change(late.pop(0))
        again(g)
        if late:
            change(late.pop(0))
    settle(waiting.pop())

    taken(raw.at[0, pl.ds(0, len(others))], asem).wait_send()
    taken(raw.at[0], fsem).wait_send()
    taken(esend, esem_s).wait_send()
    spread_done()

    @pl.when(w < windows - 1)
    def _():
        taken(zgot, zsem_s).wait_send()

    taken(xsend, xsem_s).wait_send()
    taken(obuf.at[pl.ds(0, len(others))], osem.at[0]).wait_send()
    taken(obuf.at[pl.ds(0, len(others))], osem.at[1]).wait_recv()
    pltpu.make_async_copy(obuf.at[0], obuf.at[0], hsem).wait()


def waves(initial_state, source, absorption):
    length = lax.axis_size("step")
    windows = lax.axis_size("win")
    nx, ny, nz = initial_state.shape
    half = length // 2
    reach = SWEEPS - 1
    bs, bsy = nx // 2, ny // 2
    ext = bs + reach
    ey = bsy + TILE
    units = length // 2
    plan = spans(ext, bs, reach)
    arrive, final, _, leave, _ = (len(group) for group in plan)
    f32 = jnp.float32
    dma = pltpu.SemaphoreType.DMA
    edge = pltpu.VMEM((bs, TILE, nz), f32)
    return pl.pallas_call(
        functools.partial(wave_kernel, length, windows, nx, ny, ext, ey, plan),
        out_shape=jax.ShapeDtypeStruct((nx, ny, nz), f32),
        in_specs=[pl.BlockSpec(memory_space=pltpu.HBM)] * 3,
        out_specs=pl.BlockSpec(memory_space=pl.ANY),
        scratch_shapes=[
            pltpu.VMEM((nx, ny, nz), f32),
            pltpu.VMEM((2, half, ext, ey, nz), f32),
            pltpu.VMEM((ext, ey, nz), f32),
            pltpu.VMEM((ext, ey, nz), f32),
            pltpu.VMEM((3 * length // 4, ext, ey, nz), f32),
            [[pltpu.VMEM((2, ext + 2, ey + 2 * TILE, nz), f32)] * (units // 2)] * reach,
            [pltpu.VMEM((2, bs, bsy, nz), f32)] * (units // 2),
            pltpu.VMEM((ext, ey, nz), f32),
            edge, edge, edge,
            pltpu.VMEM((2, bs, TILE, nz), f32),
            edge,
            pltpu.VMEM((half // 2, bs, bsy, nz), f32),
            pltpu.VMEM((half // 2, bs, bsy, nz), f32),
            pltpu.VMEM((half, bs, bsy, nz), f32),
            dma((4,)),
            dma,
            dma((arrive,)),
            dma,
            dma((arrive,)),
            dma,
            dma((final,)),
            dma,
            dma((final,)),
            dma((3,)),
            dma((final,)),
            dma((final,)),
            dma,
            dma((leave,)),
            dma((2,)),
            dma,
        ],
        compiler_params=pltpu.CompilerParams(
            collective_id=0, has_side_effects=True, vmem_limit_bytes=40 * 1024 * 1024
        ),
    )(*(pltpu.with_memory_space_constraint(x, pltpu.HBM) for x in (source[0, 0], initial_state, absorption)))[None, None]


def fits(mesh, shape):
    length = mesh.shape["step"]
    if length % 8 or shape[2] != LANES or shape[1] != 4 * TILE:
        return False
    gx = length // 4
    return shape[0] % gx == 0 and shape[0] // gx >= SWEEPS - 1


def pairs_up(mesh, shape):
    return mesh.shape["step"] == 8 and shape[0] // 2 >= 2 * SWEEPS


def solution(mesh):
    def body(initial_state, source, absorption):
        plan = per_device
        if fits(mesh, initial_state.shape):
            plan = waves if pairs_up(mesh, initial_state.shape) else blocks
        return plan(initial_state, source, absorption)

    return jax.shard_map(
        body,
        mesh=mesh,
        in_specs=(P(), P("win", "step", None, None, None), P()),
        out_specs=P("win", "step", None, None, None),
        check_vma=False,
    )
```

```python
import functools
import math

import jax
import jax.numpy as jnp
from jax import lax
from jax.experimental import pallas as pl
from jax.experimental.pallas import tpu as pltpu
from jax.sharding import PartitionSpec as P

ITERS = 2
SWEEPS = 8


alpha_corner = 0.1
coupling = 0.05


def from_behind(block, axis, distance):
    devices = range(lax.axis_size(axis))
    route = [(i - distance, i) for i in devices if i - distance in devices]
    return lax.ppermute(block, axis, route)


def pad_cube(field):
    widths = [(0, 0)] * (field.ndim - 3) + [(1, 1)] * 3
    return jnp.pad(field, widths)


def neighbours(field):
    padded = pad_cube(field)
    total = padded[..., 2:, 1:-1, 1:-1] + padded[..., :-2, 1:-1, 1:-1]
    total = total + padded[..., 1:-1, 2:, 1:-1] + padded[..., 1:-1, :-2, 1:-1]
    total = total + padded[..., 1:-1, 1:-1, 2:] + padded[..., 1:-1, 1:-1, :-2]
    return total


def complex_times(first, second):
    return jnp.stack(
        [first[0] * second[0] - first[1] * second[1], first[0] * second[1] + first[1] * second[0]]
    )


def relax(spectrum, inverse):
    field = complex_times(inverse, spectrum)
    for repeat in range(SWEEPS - 1):
        field = complex_times(inverse, spectrum + coupling * neighbours(field))
    return field


def inverse_diagonal(angle, absorption, gamma):
    real_part = 1.0 - gamma * jnp.cos(angle) + absorption + 6.0 * coupling
    imag_part = jnp.broadcast_to(gamma * jnp.sin(angle), real_part.shape)
    magnitude = real_part * real_part + imag_part * imag_part
    return jnp.stack([real_part / magnitude, -imag_part / magnitude])


def dft_tables(window_len):
    index = jnp.arange(window_len, dtype=jnp.int32)
    product = index[:, None] * index[None, :] % window_len
    angle = product.astype(jnp.float32) * (2.0 * math.pi / window_len)
    return (jnp.cos(angle), jnp.sin(angle))


def transform_exchange(scaled, window_len):
    pencil = lax.all_to_all(scaled[None], "step", split_axis=1, concat_axis=0, tiled=True)
    cosine, sine = dft_tables(window_len)
    flat = pencil.reshape(window_len, -1)
    real_part = jnp.dot(cosine, flat, precision=lax.Precision.HIGHEST)
    imag_part = -jnp.dot(sine, flat, precision=lax.Precision.HIGHEST)
    shaped = pencil.shape
    spectrum = (
        lax.all_to_all(real_part.reshape(shaped), "step", split_axis=0, concat_axis=1, tiled=True),
        lax.all_to_all(imag_part.reshape(shaped), "step", split_axis=0, concat_axis=1, tiled=True),
    )
    return jnp.stack([spectrum[0][0], spectrum[1][0]])


def untransform_exchange(field, window_len):
    pencil = (
        lax.all_to_all(field[0][None], "step", split_axis=1, concat_axis=0, tiled=True),
        lax.all_to_all(field[1][None], "step", split_axis=1, concat_axis=0, tiled=True),
    )
    cosine, sine = dft_tables(window_len)
    shaped = pencil[0].shape
    values = jnp.dot(cosine, pencil[0].reshape(window_len, -1), precision=lax.Precision.HIGHEST)
    values = values - jnp.dot(
        sine, pencil[1].reshape(window_len, -1), precision=lax.Precision.HIGHEST
    )
    values = values / window_len
    result = lax.all_to_all(values.reshape(shaped), "step", split_axis=0, concat_axis=1, tiled=True)
    return result[0]


def per_device(initial_state, source, absorption):
    window_len = lax.axis_size("step")
    moment = lax.axis_index("step")
    window_index = lax.axis_index("win")
    gamma = alpha_corner ** (1.0 / window_len)
    scale = gamma ** moment.astype(jnp.float32)
    forcing_base = source[0, 0]
    is_first = moment == 0
    state = jnp.zeros_like(forcing_base)
    angle = moment.astype(jnp.float32) * (2.0 * math.pi / window_len)
    inverse = inverse_diagonal(angle, absorption, gamma)
    for repeat in range(ITERS):
        if repeat == 0:
            correction = jnp.where(window_index == 0, initial_state, 0.0)
        else:
            ends = from_behind(state, "step", 1 - window_len)
            before = from_behind(ends, "win", 1)
            before = jnp.where(window_index == 0, initial_state, before)
            correction = before - alpha_corner * ends
        forcing = forcing_base + jnp.where(is_first, correction, 0.0)
        scaled = forcing * scale
        spectrum = transform_exchange(scaled, window_len)
        field = relax(spectrum, inverse)
        values = untransform_exchange(field, window_len)
        state = values / scale
    return state[None, None]


LANES = 128
TILE = 8
GROUP = 8


def tables(length):
    gamma = alpha_corner ** (1.0 / length)
    into, back, angles = [], [], []
    for core in range(2):
        rows_in, rows_back = [], []
        for time in range(length):
            scale = gamma**time
            row_in, row_back = [], []
            for p in range(length // 4):
                j = 2 * p + core
                if j == 0:
                    pair, weight = (1.0, (-1.0) ** time), 1.0 / length
                else:
                    turn = 2.0 * math.pi * (j * time % length) / length
                    pair, weight = (math.cos(turn), -math.sin(turn)), 2.0 / length
                row_in += [value * scale / coupling for value in pair]
                row_back += [value * weight / scale for value in pair]
            rows_in.append(row_in)
            rows_back.append(row_back)
        into.append(rows_in)
        back.append(rows_back)
        angles.append([2.0 * math.pi * (2 * p + core) / length for p in range(length // 4)])
    return into, back, angles


def kernel(
    length, windows, nx, ny, ext, ey,
    source, initial, absorb, out,
    raw, first, absv, coef, base, again, fa, fb, corr,
    psend, pgot, ends, zgot, csend, qsend, qgot, obuf,
    lsem, asend, brecv, fsend, esem, zsem, csem_s, csem_r, qsem_s, qsem_r, osem_s, osem_r,
):
    half = length // 2
    gx, gy = half // 2, 2
    bs, bsy = nx // gx, ny // gy
    reach = SWEEPS - 1
    pairs = length // 4
    units = 2 * pairs
    gamma = alpha_corner ** (1.0 / length)
    into, back, angles = tables(length)
    me = lax.axis_index("step")
    w = lax.axis_index("win")
    core, m = me % 2, me // 2
    partner = m * 2 + (1 - core)
    bx, by = m % gx, m // gx

    def xlo(b):
        if gx == 2:
            return b * (nx - ext)
        return jnp.minimum(jnp.maximum(b * bs - reach, 0), nx - ext)

    def ylo(b):
        return pl.multiple_of(b * (ny - ey), TILE)

    def pick(a, b):
        return jnp.where(core == 0, jnp.float32(a), jnp.float32(b))

    def region(ref, b_x, b_y):
        return ref.at[pl.ds(xlo(b_x), ext), pl.ds(ylo(b_y), ey), :]

    ox = bx * bs - xlo(bx)
    oy = pl.multiple_of(by * bsy - ylo(by), TILE)

    loads = [
        pltpu.make_async_copy(region(absorb, bx, by), absv, lsem.at[0]),
        pltpu.make_async_copy(region(source, bx, by), raw.at[me], lsem.at[1]),
        pltpu.make_async_copy(region(initial, bx, by), first, lsem.at[2]),
    ]
    for load in loads:
        load.start()
    zero_row = jnp.zeros((ey, LANES), jnp.float32)
    for u in range(units):
        for ref in (fa, fb):
            ref[u, 0, pl.ds(TILE, ey)] = zero_row
            ref[u, ext + 1, pl.ds(TILE, ey)] = zero_row
            for r in range(1, ext + 1):
                ref[u, r, pl.ds(0, TILE)] = zero_row[:TILE]
                ref[u, r, pl.ds(TILE + ey, TILE)] = zero_row[:TILE]
    if gx > 2:
        corr[...] = jnp.zeros_like(corr)

    barrier = pltpu.get_barrier_semaphore()
    for d in range(1, length):
        pl.semaphore_signal(
            barrier, inc=1, device_id={"step": (me + d) % length}, device_id_type=pl.DeviceIdType.MESH
        )

    @pl.when(w > 0)
    def _():
        pl.semaphore_signal(barrier, inc=1, device_id={"win": w - 1}, device_id_type=pl.DeviceIdType.MESH)

    @pl.when(w < windows - 1)
    def _():
        pl.semaphore_signal(barrier, inc=1, device_id={"win": w + 1}, device_id_type=pl.DeviceIdType.MESH)

    nearby = jnp.where(w > 0, 1, 0) + jnp.where(w < windows - 1, 1, 0)
    pl.semaphore_wait(barrier, length - 1 + nearby)

    def remote(src, dst, send, recv, **where):
        return pltpu.make_async_remote_copy(
            src_ref=src, dst_ref=dst, send_sem=send, recv_sem=recv,
            device_id=where, device_id_type=pl.DeviceIdType.MESH,
        )

    outgoing = []
    for d in range(1, half):
        to = (m + d) % half
        copy = remote(
            region(source, to % gx, to // gx), raw.at[me], asend.at[d], brecv.at[me], step=to * 2 + core
        )
        copy.start()
        outgoing.append(copy)
    copy = remote(region(source, bx, by), raw.at[me], asend.at[0], brecv.at[me], step=partner)
    copy.start()
    outgoing.append(copy)

    def grouped(begin, count, work, most=GROUP):
        size = -(-count // max(1, count // most))

        def body(g, carry):
            work(begin + g * size, size)
            return carry

        lax.fori_loop(0, count // size, body, 0)
        if count % size:
            work(begin + count - size, size)

    def each(one):
        def work(start, rows):
            for n in range(rows):
                one(start + n)

        return work

    loads[0].wait()

    def coefficients(i):
        for p in range(pairs):
            rows = absv[i]
            cosine = pick(math.cos(angles[0][p]), math.cos(angles[1][p]))
            imag = pick(gamma * math.sin(angles[0][p]), gamma * math.sin(angles[1][p]))
            real = 1.0 - gamma * cosine + rows + 6.0 * coupling
            over = coupling / (real * real + imag * imag)
            coef[3 * p, i] = real * over
            coef[3 * p + 1, i] = -imag * over
            if p == 0:
                other = pick(-1.0, math.cos(angles[1][p]))
                real = 1.0 - gamma * other + rows + 6.0 * coupling
                over = coupling / (real * real + imag * imag)
                coef[3 * p + 2, i] = real * over

    grouped(0, ext, each(coefficients))

    def weights(p, i):
        straight = coef[3 * p, i]
        return straight, (coef[3 * p + 2, i] if p == 0 else straight), coef[3 * p + 1, i]

    def arrival(t):
        return remote(raw.at[t], raw.at[t], asend.at[0], brecv.at[t], step=partner)

    for d in range(1, half):
        t = ((m + half - d) % half) * 2 + core
        arrival(t).wait_recv()
        copy = remote(raw.at[t], raw.at[t], fsend.at[d], brecv.at[t], step=partner)
        copy.start()
        outgoing.append(copy)
    for d in range(half):
        arrival(((m + half - d) % half) * 2 + (1 - core)).wait_recv()
    loads[1].wait()
    loads[2].wait()
    is_first = jnp.where(w == 0, jnp.float32(1.0 / coupling), jnp.float32(0.0))

    def second_weight(p, weight):
        return weight[2] + (pick(1.0, 0.0) * weight[1] if p == 0 else 0.0)

    def transform(i):
        begin = first[i] * is_first
        fields = [raw[t, i] for t in range(length)]
        for p in range(pairs):
            weight = weights(p, i)
            s0, s1 = begin, begin * pick(1.0, 0.0) if p == 0 else None
            for t in range(length):
                s0 = s0 + pick(into[0][t][2 * p], into[1][t][2 * p]) * fields[t]
                term = pick(into[0][t][2 * p + 1], into[1][t][2 * p + 1]) * fields[t]
                s1 = term if s1 is None else s1 + term
            b0 = weight[0] * s0 - weight[2] * s1
            b1 = weight[1] * s1 + weight[2] * s0
            base[2 * p, i] = b0
            base[2 * p + 1, i] = b1
            fa[2 * p, i + 1, pl.ds(TILE, ey)] = b0
            fa[2 * p + 1, i + 1, pl.ds(TILE, ey)] = b1

    grouped(0, ext, each(transform), GROUP // 2)

    lane = lax.broadcasted_iota(jnp.int32, (ey, LANES), 1)

    def around(ref, u, r):
        v = ref[u, r, pl.ds(TILE, ey)]
        total = jnp.where(lane == 0, 0.0, pltpu.roll(v, 1, 1))
        total = total + jnp.where(lane == LANES - 1, 0.0, pltpu.roll(v, LANES - 1, 1))
        beside = ref[u, r - 1, pl.ds(TILE, ey)] + ref[u, r + 1, pl.ds(TILE, ey)]
        return total + (beside + (ref[u, r, pl.ds(TILE - 1, ey)] + ref[u, r, pl.ds(TILE + 1, ey)]))

    def sweep_rows(base, here, there, start, rows):
        for n in range(rows):
            i = start + n
            for p in range(pairs):
                weight = weights(p, i)
                n0 = around(here, 2 * p, i + 1)
                n1 = around(here, 2 * p + 1, i + 1)
                there[2 * p, i + 1, pl.ds(TILE, ey)] = base[2 * p, i] + (weight[0] * n0 - weight[2] * n1)
                there[2 * p + 1, i + 1, pl.ds(TILE, ey)] = base[2 * p + 1, i] + (
                    weight[1] * n1 + weight[2] * n0
                )

    def sweeps(base):
        here, there = fa, fb
        for k in range(1, SWEEPS):
            begin, count = (bx * k, ext - k) if gx == 2 else (0, ext)
            grouped(begin, count, functools.partial(sweep_rows, base, here, there))
            here, there = there, here
        return here

    final = sweeps(base)

    def part(t, y0, rows):
        total = None
        for u in range(units):
            factor = pick(back[0][t[0]][u], back[1][t[1]][u])
            term = factor * final[u, pl.ds(ox + 1, bs), pl.ds(y0 + TILE, rows), :]
            total = term if total is None else total + term
        return total

    last = (length - 1, length - 1)
    psend[...] = part(last, pl.multiple_of(oy + TILE * (1 - core), TILE), TILE)
    swap = remote(psend, pgot, esem.at[0], esem.at[1], step=partner)
    swap.start()
    mine = part(last, pl.multiple_of(oy + TILE * core, TILE), TILE)
    swap.wait_recv()
    mine = mine + pgot[...]
    ends[...] = mine
    outgoing.append(swap)

    onward = remote(ends, zgot, zsem.at[0], zsem.at[1], win=(w + 1) % windows)

    @pl.when(w < windows - 1)
    def _():
        onward.start()

    @pl.when(w == 0)
    def _():
        zgot[...] = jnp.zeros_like(zgot)

    @pl.when(w > 0)
    def _():
        onward.wait_recv()

    change = zgot[...] - alpha_corner * ends[...]
    csend[...] = change
    corr[pl.ds(ox, bs), pl.ds(pl.multiple_of(oy + TILE * core, TILE), TILE), :] = change

    def spread(ex, ey_, send):
        rows, skip = (bs, 0) if ex == 0 else (reach, bs - reach if ex == 1 else 0)
        tx, ty = (bx + ex, by + ey_) if send else (bx, by)
        fx, fy = (bx, by) if send else (bx - ex, by - ey_)
        ax, ay = (tx, ty) if send else (fx, fy)
        inside = (ax >= 0) & (ax < gx) & (ay >= 0) & (ay < gy)
        slot = ((ex + 1) * 3 + (ey_ + 1)) * 2
        for c in range(2):
            near = c == (1 if ey_ == 1 else 0)
            if send:
                okay = inside if ey_ == 0 else inside & (core == (1 if ey_ == 1 else 0))
                if ex == 0 and ey_ == 0:
                    okay = core != c
                fc, tc = core, c
            else:
                if ey_ != 0 and not near:
                    continue
                okay = inside
                if ex == 0 and ey_ == 0:
                    okay = core != c
                fc, tc = c, core

            @pl.when(okay)
            def _(c=c, fc=fc, tc=tc):
                copy = remote(
                    csend.at[pl.ds(skip, rows)],
                    corr.at[
                        pl.ds(fx * bs + skip - xlo(tx), rows),
                        pl.ds(pl.multiple_of(fy * bsy + TILE * fc - ylo(ty), TILE), TILE),
                        :,
                    ],
                    csem_s.at[slot + c],
                    csem_r.at[slot + fc],
                    step=(ty * gx + tx) * 2 + tc if send == 1 else partner,
                )
                if send == 1:
                    copy.start()
                elif send == 2:
                    copy.wait_send()
                else:
                    copy.wait_recv()

    offsets = [(ex, e) for ex in (-1, 0, 1) for e in (-1, 0, 1)]
    for ex, e in offsets:
        spread(ex, e, 1)
    for ex, e in offsets:
        spread(ex, e, 0)

    def correct(i):
        x = corr[i] * (1.0 / coupling)
        for p in range(pairs):
            weight = weights(p, i)
            b0 = base[2 * p, i] + weight[0] * x
            b1 = base[2 * p + 1, i] + second_weight(p, weight) * x
            again[2 * p, i] = b0
            again[2 * p + 1, i] = b1
            fa[2 * p, i + 1, pl.ds(TILE, ey)] = b0
            fa[2 * p + 1, i + 1, pl.ds(TILE, ey)] = b1

    grouped(0, ext, each(correct))
    final = sweeps(again)

    for k in range(half):
        qsend[k] = part((2 * k + 1, 2 * k), oy, bsy)
        copy = remote(qsend.at[k], qgot.at[k], qsem_s.at[k], qsem_r.at[k], step=partner)
        copy.start()
        outgoing.append(copy)
    for k in range(half):
        obuf[k] = part((2 * k, 2 * k + 1), oy, bsy)

    def place(b_x, b_y):
        return out.at[pl.ds(b_x * bs, bs), pl.ds(pl.multiple_of(b_y * bsy, TILE), bsy), :]

    for k in range(half):
        remote(qsend.at[k], qgot.at[k], qsem_s.at[k], qsem_r.at[k], step=partner).wait_recv()
        obuf[k] = obuf[k] + qgot[k]

        @pl.when(m == k)
        def _(k=k):
            pltpu.make_async_copy(obuf.at[k], place(bx, by), lsem.at[3]).start()

        @pl.when(m != k)
        def _(k=k):
            remote(obuf.at[k], place(bx, by), osem_s.at[k], osem_r.at[m], step=2 * k + core).start()

    for copy in outgoing:
        copy.wait_send()
    for ex, e in offsets:
        spread(ex, e, 2)

    @pl.when(w < windows - 1)
    def _():
        onward.wait_send()

    for k in range(half):

        @pl.when(m == k)
        def _(k=k):
            pltpu.make_async_copy(obuf.at[k], place(bx, by), lsem.at[3]).wait()

        @pl.when(m != k)
        def _(k=k):
            done = remote(obuf.at[k], place(k % gx, k // gx), osem_s.at[k], osem_r.at[k], step=partner)
            done.wait_send()
            done.wait_recv()


def blocks(initial_state, source, absorption):
    length = lax.axis_size("step")
    windows = lax.axis_size("win")
    nx, ny, nz = initial_state.shape
    half = length // 2
    gx, reach = half // 2, SWEEPS - 1
    bs, bsy = nx // gx, ny // 2
    ext = min(nx, bs + reach * (1 if gx == 2 else 2))
    ey = bsy + -(-reach // TILE) * TILE
    units = length // 2
    f32 = jnp.float32
    dma = pltpu.SemaphoreType.DMA
    return pl.pallas_call(
        functools.partial(kernel, length, windows, nx, ny, ext, ey),
        out_shape=jax.ShapeDtypeStruct((nx, ny, nz), f32),
        in_specs=[pl.BlockSpec(memory_space=pl.ANY)] * 3,
        out_specs=pl.BlockSpec(memory_space=pl.ANY),
        scratch_shapes=[
            pltpu.VMEM((length, ext, ey, nz), f32),
            pltpu.VMEM((ext, ey, nz), f32),
            pltpu.VMEM((ext, ey, nz), f32),
            pltpu.VMEM((3 * length // 4, ext, ey, nz), f32),
            pltpu.VMEM((units, ext, ey, nz), f32),
            pltpu.VMEM((units, ext, ey, nz), f32),
            pltpu.VMEM((units, ext + 2, ey + 2 * TILE, nz), f32),
            pltpu.VMEM((units, ext + 2, ey + 2 * TILE, nz), f32),
            pltpu.VMEM((ext, ey, nz), f32),
            pltpu.VMEM((bs, TILE, nz), f32),
            pltpu.VMEM((bs, TILE, nz), f32),
            pltpu.VMEM((bs, TILE, nz), f32),
            pltpu.VMEM((bs, TILE, nz), f32),
            pltpu.VMEM((bs, TILE, nz), f32),
            pltpu.VMEM((half, bs, bsy, nz), f32),
            pltpu.VMEM((half, bs, bsy, nz), f32),
            pltpu.VMEM((half, bs, bsy, nz), f32),
            dma((4,)),
            dma((half,)),
            dma((length,)),
            dma((half,)),
            dma((2,)),
            dma((2,)),
            dma((18,)),
            dma((18,)),
            dma((half,)),
            dma((half,)),
            dma((half,)),
            dma((half,)),
        ],
        compiler_params=pltpu.CompilerParams(
            collective_id=0, has_side_effects=True, vmem_limit_bytes=28 * 1024 * 1024
        ),
    )(source[0, 0], initial_state, absorption)[None, None]


ARRIVE = (7, 5, 3, 3, 3)
SECOND = (5, 3, 3, 3, 3, 3)
LEAST = 1


def cuts(sizes, extent):
    bounds = [0]
    for size in sizes:
        if bounds[-1] + size < extent:
            bounds.append(bounds[-1] + size)
    bounds.append(extent)
    return list(zip(bounds[:-1], bounds[1:]))


def spans(ext, bs, reach):
    arrive = cuts(ARRIVE, ext)
    final = [(max(0, a - reach), b - reach) for a, b in arrive if b > reach]
    sources = [(a, b, "own", e) for e, (a, b) in enumerate(final)]
    for e, (a, b) in enumerate(final):
        if b > bs - reach:
            sources.append((2 * bs - b, 2 * bs - max(a, bs - reach), "beyond", e))
    second, leave, after, sent = [], [], {}, 0
    groups = cuts(SECOND, ext)
    for g, (a, b) in enumerate(groups):
        needs = [(kind, e) for lo, hi, kind, e in sources if a <= lo < b or (lo < a and g == 0)]
        second.append((a, b, needs))
        if b - reach - sent >= LEAST or g == len(groups) - 1:
            after[g] = len(leave)
            leave.append((sent, b - reach))
            sent = b - reach
    return arrive, final, second, leave, after


def wave_kernel(
    length, windows, nx, ny, ext, ey, plan,
    source, initial, absorb, out,
    srcv, raw, first, absv, coef, levels, fin, corr,
    emine, esend, egot, zgot, csend, xsend, xgot, obuf,
    lsem, asem, isem, fsem, dsem, esem_s, esem_r, zsem_s, zsem_r, csem_s, csem_r, bsem_r, xsem_s, osem, hsem,
):
    arrive, final, second, leave, after = plan
    half = length // 2
    bs, bsy = nx // 2, ny // 2
    reach = SWEEPS - 1
    pairs = length // 4
    units = 2 * pairs
    kept = half // 2
    gamma = alpha_corner ** (1.0 / length)
    into, back, angles = tables(length)
    me = lax.axis_index("step")
    w = lax.axis_index("win")
    core, m = me % 2, me // 2
    partner = m * 2 + (1 - core)
    bx, by = m % 2, m // 2
    near = core == 1 - by

    def chip(b_x, b_y):
        return b_y * 2 + b_x

    def xlo(b):
        return b * (nx - ext)

    def ylo(b):
        return pl.multiple_of(b * (ny - ey), TILE)

    def rows_of(lo, hi, b=bx):
        return lo + b * (ext - lo - hi)

    def own_of(lo, hi, b=bx):
        return lo + b * (bs - lo - hi)

    def held(i):
        return i + bx * (ext - 1 - 2 * i)

    def own(i):
        return i + bx * (bs - 1 - 2 * i)

    def pick(a, b):
        if a == b:
            return jnp.float32(a)
        return jnp.where(core == 0, jnp.float32(a), jnp.float32(b))

    def region(ref, b_x, b_y, lo, hi):
        rows = pl.ds(xlo(b_x) + rows_of(lo, hi, b_x), hi - lo)
        return ref.at[rows, pl.ds(ylo(b_y), ey), :]

    ox = bx * bs - xlo(bx)
    oy = pl.multiple_of(by * bsy - ylo(by), TILE)

    loads = [
        pltpu.make_async_copy(source, srcv, lsem.at[0]),
        pltpu.make_async_copy(region(absorb, bx, by, 0, ext), absv, lsem.at[1]),
        pltpu.make_async_copy(region(source, bx, by, 0, ext), raw.at[core, m], lsem.at[2]),
        pltpu.make_async_copy(region(initial, bx, by, 0, ext), first, lsem.at[3]),
    ]
    for load in loads:
        load.start()

    barrier = pltpu.get_barrier_semaphore()

    def greet(**where):
        pl.semaphore_signal(barrier, inc=1, device_id=where, device_id_type=pl.DeviceIdType.MESH)

    for d in range(1, length):
        greet(step=(me + d) % length)

    @pl.when(w > 0)
    def _():
        greet(win=w - 1, step=me)
        greet(win=w - 1, step=partner)

    @pl.when(w < windows - 1)
    def _():
        greet(win=w + 1, step=me)
        greet(win=w + 1, step=partner)

    @pl.when(w == 0)
    def _():
        zgot[...] = jnp.zeros_like(zgot)

    nearby = jnp.where(w > 0, 2, 0) + jnp.where(w < windows - 1, 2, 0)
    loads[0].wait()
    pl.semaphore_wait(barrier, length - 1 + nearby)

    def remote(src, dst, send, recv, **where):
        return pltpu.make_async_remote_copy(
            src_ref=src, dst_ref=dst, send_sem=send, recv_sem=recv,
            device_id=where, device_id_type=pl.DeviceIdType.MESH,
        )

    def taken(block, sem):
        return remote(block, block, sem, sem, step=partner)

    others = [(1, 1), (1, 0), (0, 1)]

    def beside(ex, e_y):
        return (bx + ex) % 2, (by + e_y) % 2

    for c, (lo, hi) in enumerate(arrive):
        for where in others:
            tx, ty = beside(*where)
            remote(
                region(srcv, tx, ty, lo, hi),
                raw.at[core, m, pl.ds(rows_of(lo, hi, tx), hi - lo)],
                asem, isem.at[c], step=chip(tx, ty) * 2 + core,
            ).start()

    zero_row = jnp.zeros((ey, LANES), jnp.float32)

    def rim(r, carry):
        for refs in levels:
            for ref in refs:
                for q in range(2):
                    ref[q, r, pl.ds(0, TILE)] = zero_row[:TILE]
                    ref[q, r, pl.ds(TILE + ey, TILE)] = zero_row[:TILE]
        return carry

    for refs in levels:
        for ref in refs:
            for q in range(2):
                for r in (0, ext + 1):
                    ref[q, r, pl.ds(TILE, ey)] = zero_row
    lax.fori_loop(1, ext + 1, rim, 0)

    def grouped(begin, count, work, most):
        groups = -(-count // most)
        size = -(-count // groups)
        if groups == 1:
            work(begin, count)
            return

        def body(g, carry):
            work(begin + g * size, size)
            return carry

        lax.fori_loop(0, count // size, body, 0)
        if count % size:
            work(begin + count - count % size, count % size)

    loads[1].wait()

    def coefficients(start, rows):
        for n in range(rows):
            i = start + n
            for p in range(pairs):
                here = absv[held(i)]
                cosine = pick(math.cos(angles[0][p]), math.cos(angles[1][p]))
                imag = pick(gamma * math.sin(angles[0][p]), gamma * math.sin(angles[1][p]))
                real = 1.0 - gamma * cosine + here + 6.0 * coupling
                over = coupling / (real * real + imag * imag)
                coef[3 * p, i] = real * over
                coef[3 * p + 1, i] = -imag * over
                if p == 0:
                    other = pick(-1.0, math.cos(angles[1][p]))
                    real = 1.0 - gamma * other + here + 6.0 * coupling
                    over = coupling / (real * real + imag * imag)
                    coef[3 * p + 2, i] = real * over

    grouped(0, ext, coefficients, 4)

    def weights(p, i, y0=0, rows=ey):
        part = pl.ds(y0, rows)
        straight = coef[3 * p, i, part]
        return straight, (coef[3 * p + 2, i, part] if p == 0 else straight), coef[3 * p + 1, i, part]

    is_first = jnp.where(w == 0, jnp.float32(1.0 / coupling), jnp.float32(0.0))

    def combine(pair, values):
        total = None
        for (a, b), value in zip(pair, values):
            if a == 0 and b == 0:
                continue
            term = value if a == 1 and b == 1 else pick(a, b) * value
            total = term if total is None else total + term
        return total

    def spectrum(start, rows):
        for n in range(rows):
            i = start + n
            folded = []
            for t in range(half):
                early, late = gamma**t / coupling, gamma ** (t + half) / coupling
                now, then = raw[t % 2, t // 2, held(i)], raw[t % 2, (t + half) // 2, held(i)]
                folded.append(early * now + pick(late, -late) * then)
            folded[0] = folded[0] + first[held(i)] * is_first
            for p in range(pairs):
                weight = weights(p, i)
                turn = [
                    [
                        tuple(into[c][t][2 * p + q] * coupling / gamma**t for c in range(2))
                        for t in range(half)
                    ]
                    for q in range(2)
                ]
                turn = [[tuple(round(v, 15) for v in pair) for pair in row] for row in turn]
                s0 = combine(turn[0], folded)
                s1 = combine(turn[1], folded)
                levels[0][p][0, i + 1, pl.ds(TILE, ey)] = weight[0] * s0 - weight[2] * s1
                levels[0][p][1, i + 1, pl.ds(TILE, ey)] = weight[1] * s1 + weight[2] * s0

    def stencil(ref, q, start, rows, y0, depth):
        lane = lax.broadcasted_iota(jnp.int32, (depth, LANES), 1)
        at = pl.multiple_of(y0 + TILE, TILE)
        line = [ref[q, start + n, pl.ds(at, depth)] for n in range(rows + 2)]
        sums = []
        for n in range(1, rows + 1):
            v = line[n]
            around = ref.at[q, start + n, pl.ds(y0, depth + 2 * TILE), :]
            total = jnp.where(lane == 0, 0.0, pltpu.roll(v, 1, 1))
            total = total + jnp.where(lane == LANES - 1, 0.0, pltpu.roll(v, LANES - 1, 1))
            across = around[pl.ds(TILE - 1, depth)] + around[pl.ds(TILE + 1, depth)]
            sums.append(total + ((line[n - 1] + line[n + 1]) + across))
        return sums

    def sweep_rows(k, start, rows):
        last = k == reach
        y0, depth = (oy, bsy) if last else (0, ey)
        at = pl.multiple_of(y0 + TILE, TILE)
        for p in range(pairs):
            s0 = stencil(levels[k - 1][p], 0, start, rows, y0, depth)
            s1 = stencil(levels[k - 1][p], 1, start, rows, y0, depth)
            for n in range(rows):
                i = start + n
                weight = weights(p, i, y0, depth)
                b0 = levels[0][p][0, i + 1, pl.ds(at, depth)]
                b1 = levels[0][p][1, i + 1, pl.ds(at, depth)]
                v0 = b0 + (weight[0] * s0[n] - weight[2] * s1[n])
                v1 = b1 + (weight[1] * s1[n] + weight[2] * s0[n])
                if last:
                    fin[p][0, i] = v0
                    fin[p][1, i] = v1
                else:
                    levels[k][p][0, i + 1, pl.ds(TILE, ey)] = v0
                    levels[k][p][1, i + 1, pl.ds(TILE, ey)] = v1

    def sweeps(a, b):
        for k in range(1, SWEEPS):
            lo, hi = max(0, a - k), b - k
            if hi > lo:
                grouped(lo, hi - lo, functools.partial(sweep_rows, k), 6)

    def part(ref, t, lo, hi, y0, depth):
        factors = [pick(back[0][t[0]][u], back[1][t[1]][u]) for u in range(units)]
        for i in range(lo, hi):
            total = None
            for u, factor in enumerate(factors):
                term = factor * fin[u // 2][u % 2, i, pl.ds(y0, depth)]
                total = term if total is None else total + term
            ref[own(i)] = total

    def strip(ref, lo, hi):
        return ref.at[pl.ds(own_of(lo, hi), hi - lo)]

    def swap(e):
        lo, hi = final[e]
        return remote(strip(esend, lo, hi), strip(egot, lo, hi), esem_s, esem_r.at[e], step=partner)

    def onward(e):
        lo, hi = final[e]
        after_w = (w + 1) % windows
        return [
            remote(strip(emine, lo, hi), strip(zgot.at[0], lo, hi), zsem_s, zsem_r.at[e], win=after_w, step=me),
            remote(strip(esend, lo, hi), strip(zgot.at[1], lo, hi), zsem_s, zsem_r.at[e], win=after_w, step=partner),
        ]

    def finish(e):
        lo, hi = final[e]
        last = (length - 1, length - 1)
        part(esend, last, lo, hi, pl.multiple_of(TILE * (1 - core), TILE), TILE)
        part(emine, last, lo, hi, pl.multiple_of(TILE * core, TILE), TILE)

        @pl.when(w < windows - 1)
        def _():
            for copy in onward(e):
                copy.start()

        swap(e).start()

    def landing(f_x, f_y, f_c, t_x, t_y, lo, hi):
        rows = pl.ds(f_x * bs + own_of(lo, hi, f_x) - xlo(t_x), hi - lo)
        depth = pl.ds(pl.multiple_of(f_y * bsy + TILE * f_c - ylo(t_y), TILE), TILE)
        return corr.at[rows, depth, :]

    def edge(e):
        lo, hi = final[e]
        return max(lo, bs - reach), hi

    def spread(e):
        lo, hi = final[e]

        def one(where, to_core, lo, hi, send, recv):
            tx, ty = beside(*where)
            remote(
                strip(csend, lo, hi), landing(bx, by, core, tx, ty, lo, hi),
                send, recv, step=chip(tx, ty) * 2 + to_core,
            ).start()

        lo2, hi2 = edge(e)
        if hi2 > lo2:

            @pl.when(near)
            def _():
                for c in range(2):
                    one((1, 1), c, lo2, hi2, csem_s.at[2], bsem_r.at[e])

            for c in range(2):
                one((1, 0), c, lo2, hi2, csem_s.at[0], bsem_r.at[e])

        @pl.when(near)
        def _():
            for c in range(2):
                one((0, 1), c, lo, hi, csem_s.at[1], csem_r.at[e])

        one((0, 0), 1 - core, lo, hi, csem_s.at[0], csem_r.at[e])

    def spread_done():
        taken(srcv.at[pl.ds(0, bs + 2 * reach), pl.ds(0, TILE), :], csem_s.at[0]).wait_send()

        @pl.when(near)
        def _():
            taken(srcv.at[pl.ds(0, 2 * bs), pl.ds(0, TILE), :], csem_s.at[1]).wait_send()
            taken(srcv.at[pl.ds(0, 2 * reach), pl.ds(0, TILE), :], csem_s.at[2]).wait_send()

    def gather(e, kind):
        lo, hi = final[e]
        if kind == "own":
            taken(corr.at[pl.ds(0, hi - lo), pl.ds(0, 2 * TILE), :], csem_r.at[e]).wait_recv()
        else:
            lo, hi = edge(e)
            taken(corr.at[pl.ds(0, hi - lo)], bsem_r.at[e]).wait_recv()

    def change(e):
        lo, hi = final[e]
        swap(e).wait_recv()

        @pl.when(w > 0)
        def _():
            taken(zgot.at[:, pl.ds(0, hi - lo)], zsem_r.at[e]).wait_recv()

        mine = pl.ds(own_of(lo, hi), hi - lo)
        value = (zgot[0, mine] + zgot[1, mine]) - alpha_corner * (emine[mine] + egot[mine])
        csend[mine] = value
        corr[pl.ds(ox + own_of(lo, hi), hi - lo), pl.ds(pl.multiple_of(oy + TILE * core, TILE), TILE), :] = value
        spread(e)

    def second_weight(p, weight):
        return weight[2] + (pick(1.0, 0.0) * weight[1] if p == 0 else 0.0)

    def correct(start, rows):
        for n in range(rows):
            i = start + n
            x = corr[held(i)] * (1.0 / coupling)
            for p in range(pairs):
                weight = weights(p, i)
                spot = pl.ds(TILE, ey)
                ref = levels[0][p]
                ref[0, i + 1, spot] = ref[0, i + 1, spot] + weight[0] * x
                ref[1, i + 1, spot] = ref[1, i + 1, spot] + second_weight(p, weight) * x

    def trade(i, o):
        lo, hi = leave[o]
        mine = pl.ds(own_of(lo, hi), hi - lo)
        return remote(xsend.at[i, mine], xgot.at[i, mine], xsem_s, isem.at[o], step=partner)

    def emit(o):
        lo, hi = leave[o]
        for i in range(kept):
            part(xsend.at[i], (2 * i + 1, 2 * i), lo, hi, 0, bsy)
            trade(i, o).start()
        for i in range(kept):
            part(obuf.at[i], (2 * i, 2 * i + 1), lo, hi, 0, bsy)

    def place(b_x, b_y, lo, hi):
        rows = pl.ds(b_x * bs + own_of(lo, hi, b_x), hi - lo)
        return out.at[rows, pl.ds(pl.multiple_of(b_y * bsy, TILE), bsy), :]

    def settle(o):
        lo, hi = leave[o]
        mine = pl.ds(own_of(lo, hi), hi - lo)
        ratio = gamma ** (-half)
        taken(xgot.at[:, pl.ds(0, hi - lo)], isem.at[o]).wait_recv()
        for i in range(kept):
            ours, theirs = obuf[i, mine], xgot[i, mine]
            obuf[i, mine] = ours + theirs
            obuf[i + kept, mine] = pick(ratio, -ratio) * (ours - theirs)
        for where in others:
            k = chip(*beside(*where))
            remote(
                strip(obuf.at[k], lo, hi), place(bx, by, lo, hi), osem.at[0], osem.at[1], step=2 * k + core
            ).start()
        pltpu.make_async_copy(strip(obuf.at[m], lo, hi), place(bx, by, lo, hi), hsem).start()

    def receive(c):
        lo, hi = arrive[c]
        taken(raw.at[0, pl.ds(0, len(others)), pl.ds(0, hi - lo)], isem.at[c]).wait_recv()
        block = raw.at[core, :, pl.ds(rows_of(lo, hi), hi - lo)]
        remote(block, block, fsem, dsem.at[c], step=partner).start()

    waiting = []
    chunks, ends = len(arrive), len(final)
    late = list(range(ends))

    def advance(c):
        a, b = arrive[c]
        taken(raw.at[0, :, pl.ds(0, b - a)], dsem.at[c]).wait_recv()
        e = c - (chunks - ends)
        while late and late[0] <= min(e - 2, ends - 4):
            change(late.pop(0))
        grouped(a, b - a, spectrum, 3)
        sweeps(a, b)

    def again(g):
        a, b, needs = second[g]
        for kind, e in needs:
            gather(e, kind)
        grouped(a, b - a, correct, 5)
        sweeps(a, b)
        if g in after:
            emit(after[g])
            if waiting:
                settle(waiting.pop())
            waiting.append(after[g])

    def step(c):
        advance(c)
        e = c - (chunks - ends)
        if e >= 0:
            finish(e)

    loads[2].wait()
    loads[3].wait()
    for c in range(chunks):
        receive(c)
        if c:
            step(c - 1)
    step(chunks - 1)
    change(late.pop(0))
    for g in range(len(second)):
        while any(kind == "own" and e in late for kind, e in second[g][2]):
            change(late.pop(0))
        again(g)
        if late:
            change(late.pop(0))
    settle(waiting.pop())

    taken(raw.at[0, pl.ds(0, len(others))], asem).wait_send()
    taken(raw.at[0], fsem).wait_send()
    taken(esend, esem_s).wait_send()
    spread_done()

    @pl.when(w < windows - 1)
    def _():
        taken(zgot, zsem_s).wait_send()

    taken(xsend, xsem_s).wait_send()
    taken(obuf.at[pl.ds(0, len(others))], osem.at[0]).wait_send()
    taken(obuf.at[pl.ds(0, len(others))], osem.at[1]).wait_recv()
    pltpu.make_async_copy(obuf.at[0], obuf.at[0], hsem).wait()


def waves(initial_state, source, absorption):
    length = lax.axis_size("step")
    windows = lax.axis_size("win")
    nx, ny, nz = initial_state.shape
    half = length // 2
    reach = SWEEPS - 1
    bs, bsy = nx // 2, ny // 2
    ext = bs + reach
    ey = bsy + TILE
    units = length // 2
    plan = spans(ext, bs, reach)
    arrive, final, _, leave, _ = (len(group) for group in plan)
    f32 = jnp.float32
    dma = pltpu.SemaphoreType.DMA
    edge = pltpu.VMEM((bs, TILE, nz), f32)
    return pl.pallas_call(
        functools.partial(wave_kernel, length, windows, nx, ny, ext, ey, plan),
        out_shape=jax.ShapeDtypeStruct((nx, ny, nz), f32),
        in_specs=[pl.BlockSpec(memory_space=pltpu.HBM)] * 3,
        out_specs=pl.BlockSpec(memory_space=pl.ANY),
        scratch_shapes=[
            pltpu.VMEM((nx, ny, nz), f32),
            pltpu.VMEM((2, half, ext, ey, nz), f32),
            pltpu.VMEM((ext, ey, nz), f32),
            pltpu.VMEM((ext, ey, nz), f32),
            pltpu.VMEM((3 * length // 4, ext, ey, nz), f32),
            [[pltpu.VMEM((2, ext + 2, ey + 2 * TILE, nz), f32)] * (units // 2)] * reach,
            [pltpu.VMEM((2, bs, bsy, nz), f32)] * (units // 2),
            pltpu.VMEM((ext, ey, nz), f32),
            edge, edge, edge,
            pltpu.VMEM((2, bs, TILE, nz), f32),
            edge,
            pltpu.VMEM((half // 2, bs, bsy, nz), f32),
            pltpu.VMEM((half // 2, bs, bsy, nz), f32),
            pltpu.VMEM((half, bs, bsy, nz), f32),
            dma((4,)),
            dma,
            dma((max(arrive, leave),)),
            dma,
            dma((arrive,)),
            dma,
            dma((final,)),
            dma,
            dma((final,)),
            dma((3,)),
            dma((final,)),
            dma((final,)),
            dma,
            dma((2,)),
            dma,
        ],
        compiler_params=pltpu.CompilerParams(
            collective_id=0, has_side_effects=True, vmem_limit_bytes=40 * 1024 * 1024
        ),
    )(*(pltpu.with_memory_space_constraint(x, pltpu.HBM) for x in (source[0, 0], initial_state, absorption)))[None, None]


def fits(mesh, shape):
    length = mesh.shape["step"]
    if length % 8 or shape[2] != LANES or shape[1] != 4 * TILE:
        return False
    gx = length // 4
    return shape[0] % gx == 0 and shape[0] // gx >= SWEEPS - 1


def pairs_up(mesh, shape):
    return mesh.shape["step"] == 8 and shape[0] // 2 >= 2 * SWEEPS


def solution(mesh):
    def body(initial_state, source, absorption):
        plan = per_device
        if fits(mesh, initial_state.shape):
            plan = waves if pairs_up(mesh, initial_state.shape) else blocks
        return plan(initial_state, source, absorption)

    return jax.shard_map(
        body,
        mesh=mesh,
        in_specs=(P(), P("win", "step", None, None, None), P()),
        out_specs=P("win", "step", None, None, None),
        check_vma=False,
    )
```
